128 devices in a mesh: gx: 16 (over z_lo, x, core), gy: 8 (over y, z_hi).
Axes of the slice: x: 4, y: 4, z: 4 (z_hi: 2, z_lo: 2; z = z_hi * 2 + z_lo), core: 2. Of those that a mesh axis runs over, the one named last changes fastest.
Arguments:
- pair_in: bfloat16 [1024, 1024, 128], P(('gx', 'gy')), may hold values from -6 to 6
- residue_mask: int32 [1024], P(('gx', 'gy')), may hold values 0 or 1
- norm_start: float32 [128], replicated, may hold values from 0.25 to 1.75
- proj_start: bfloat16 [128, 512], replicated, may hold values from -0.5 to 0.5
- gate_bias_start: float32 [128], replicated, may hold values from -4 to 4
- bias_w_start: bfloat16 [128, 4], replicated, may hold values from -1.5 to 1.5
- out_w_start: bfloat16 [128, 128], replicated, may hold values from -1 to 1
- norm_end: float32 [128], replicated, may hold values from 0.25 to 1.75
- proj_end: bfloat16 [128, 512], replicated, may hold values from -0.5 to 0.5
- gate_bias_end: float32 [128], replicated, may hold values from -4 to 4
- bias_w_end: bfloat16 [128, 4], replicated, may hold values from -1.5 to 1.5
- out_w_end: bfloat16 [128, 128], replicated, may hold values from -1 to 1
- norm_trans: float32 [128], replicated, may hold values from 0.25 to 1.75
- trans_in: bfloat16 [128, 512], replicated, may hold values from -0.5 to 0.5
- trans_bias: float32 [512], replicated, may hold values from -4 to 4
- trans_out: bfloat16 [512, 128], replicated, may hold values from -0.375 to 0.375
Outputs:
- pair_out: bfloat16 [1024, 1024, 128], P(('gx', 'gy'))
The draws below stay inside these ranges and needn't reach their ends.
Inputs may be any that keep to these rules, and one draw needn't show every extreme that they name: residue_mask holds only 0 and 1.
All inputs are finite; a program needn't handle non-finite values.
Results may differ from the reference program's by a relative error of at most 0.02.
Values may be sent and summed in bfloat16 or wider, within the bound.
A program may use at most 192 MiB of HBM per device.

```python
import jax
import jax.numpy as jnp
from jax import lax

C = 128
HEADS = 4
HEAD_DIM = 32
FFN = 512
RES = 1024


def with_ends(array, key, smallest, top_value):
    place = [jax.random.randint(jax.random.fold_in(key, axis), (), 0, length) for axis, length in enumerate(array.shape)]
    longest = array.shape.index(max(array.shape))
    next_to = place[:longest] + [(place[longest] + 1) % array.shape[longest]] + place[longest + 1:]
    return array.at[tuple(place)].set(smallest).at[tuple(next_to)].set(top_value)


def block_scale(own_key, shape, split, least, high):
    loudness = 1.0
    for position, shards_of in split:
        steps = jax.random.uniform(jax.random.fold_in(jax.random.fold_in(own_key, 6), position), (shards_of,), jnp.float32, least / len(split), high / len(split))
        loudness = loudness * jnp.repeat(jnp.exp(steps), shape[position] // shards_of).reshape((-1,) + (1,) * (len(shape) - 1 - position))
    return loudness


def scatter_about(own_key, extent, deviation, bound, pieces=(), held_as=jnp.bfloat16):
    values = jax.random.normal(own_key, extent, jnp.float32) * deviation
    if len(pieces) > 0:
        values = block_scale(own_key, extent, pieces, -0.22, 0.18) * values
    return jnp.clip(values, min=-bound, max=bound).astype(held_as)


def setup_inputs(seed: int = 0) -> dict:
    streams_of = jax.random.split(jax.random.key(seed), 17)
    return {
        "pair_in": scatter_about(streams_of[0], (RES, RES, C), 1.0, 6.0, ((0, 128),)),
        "residue_mask": with_ends((jax.random.randint(streams_of[1], (RES,), 0, 8) < 7).astype(jnp.int32), jax.random.fold_in(streams_of[1], 1), 0, 1),
        "norm_start": jnp.clip(1.0 + 0.15 * jax.random.normal(streams_of[2], (C,), jnp.float32), 0.25, 1.75),
        "proj_start": scatter_about(streams_of[3], (C, 4 * C), C ** -0.5, 0.5),
        "gate_bias_start": scatter_about(streams_of[4], (C,), 1.0, 4.0, (), jnp.float32),
        "bias_w_start": scatter_about(streams_of[5], (C, HEADS), (C // 8) ** -0.5, 1.5),
        "out_w_start": scatter_about(streams_of[6], (C, C), (C // 4) ** -0.5, 1.0),
        "norm_end": jnp.clip(1.0 + 0.15 * jax.random.normal(streams_of[7], (C,), jnp.float32), 0.25, 1.75),
        "proj_end": scatter_about(streams_of[8], (C, 4 * C), C ** -0.5, 0.5),
        "gate_bias_end": scatter_about(streams_of[9], (C,), 1.0, 4.0, (), jnp.float32),
        "bias_w_end": scatter_about(streams_of[10], (C, HEADS), (C // 8) ** -0.5, 1.5),
        "out_w_end": scatter_about(streams_of[11], (C, C), (C // 4) ** -0.5, 1.0),
        "norm_trans": jnp.clip(1.0 + 0.15 * jax.random.normal(streams_of[12], (C,), jnp.float32), 0.25, 1.75),
        "trans_in": scatter_about(streams_of[13], (C, FFN), C ** -0.5, 0.5),
        "trans_bias": scatter_about(streams_of[14], (FFN,), 1.0, 4.0, (), jnp.float32),
        "trans_out": scatter_about(streams_of[15], (FFN, C), (FFN // 2) ** -0.5, 0.375),
    }


big_negative = 1000000000.0

def layer_norm(values, norm_gain):
    widened = values.astype(jnp.float32)
    row_mean = lax.optimization_barrier(jnp.mean(widened, axis=-1, keepdims=True))
    row_var = lax.optimization_barrier(jnp.mean(jnp.square(widened - row_mean), axis=-1, keepdims=True))
    return ((widened - row_mean) * lax.rsqrt(row_var + 1e-05) * norm_gain).astype(jnp.bfloat16)

def project(normed, weight):
    flat = normed.reshape(-1, normed.shape[-1])
    result = jnp.dot(flat, weight, preferred_element_type=jnp.float32)
    return result.reshape(normed.shape[:-1] + (weight.shape[1],))

def split_heads(merged):
    return merged.astype(jnp.bfloat16).reshape(merged.shape[:-1] + (HEADS, HEAD_DIM))

def attend_block(query, keys, values, pair_bias, key_bias):
    score_scale = HEAD_DIM ** (-0.5)
    scores = jnp.einsum('jhd,khd->hjk', query.astype(jnp.float32), keys.astype(jnp.float32), precision=lax.Precision.HIGHEST)
    scores = scores * score_scale + pair_bias + key_bias
    attn_weights = jax.nn.softmax(scores, axis=-1)
    mixed = jnp.einsum('hjk,khd->jhd', attn_weights, values.astype(jnp.float32), precision=lax.Precision.HIGHEST)
    return mixed.reshape(query.shape[0], HEADS * HEAD_DIM)

def gated_residual(residual, mixed, gate_logit, gate_bias, out_weight):
    gated = (mixed * jax.nn.sigmoid(gate_logit + gate_bias)).astype(jnp.bfloat16)
    return (residual.astype(jnp.float32) + project(gated, out_weight)).astype(jnp.bfloat16)

def projections(normed, weight, channels):
    projected = project(normed, weight)
    query = split_heads(projected[..., :channels])
    keys = split_heads(projected[..., channels:2 * channels])
    values = split_heads(projected[..., 2 * channels:3 * channels])
    return (query, keys, values, projected[..., 3 * channels:])

def reference(pair_in, residue_mask, norm_start, proj_start, gate_bias_start, bias_w_start, out_w_start, norm_end, proj_end, gate_bias_end, bias_w_end, out_w_end, norm_trans, trans_in, trans_bias, trans_out):
    channels = pair_in.shape[-1]
    key_bias = (residue_mask.astype(jnp.float32) - 1.0) * big_negative
    normed = layer_norm(pair_in, norm_start)
    query, keys, values, gate_logit = projections(normed, proj_start, channels)
    pair_bias = project(normed, bias_w_start).astype(jnp.bfloat16)
    start_bias = jnp.transpose(pair_bias, (2, 0, 1)).astype(jnp.float32)

    def per_row(operands):
        query_row, key_row, value_row = operands
        return attend_block(query_row, key_row, value_row, start_bias, key_bias)
    mixed = lax.map(per_row, (query, keys, values))
    after_start = gated_residual(pair_in, mixed, gate_logit, gate_bias_start, out_w_start)
    normed = layer_norm(after_start, norm_end)
    query, keys, values, gate_logit = projections(normed, proj_end, channels)
    pair_bias = project(normed, bias_w_end).astype(jnp.bfloat16)
    end_bias = jnp.transpose(pair_bias, (2, 1, 0)).astype(jnp.float32)

    def per_column(operands):
        query_col, key_col, value_col = operands
        return attend_block(query_col, key_col, value_col, end_bias, key_bias)
    mixed = lax.map(per_column, (jnp.swapaxes(query, 0, 1), jnp.swapaxes(keys, 0, 1), jnp.swapaxes(values, 0, 1)))
    mixed = jnp.swapaxes(mixed, 0, 1)
    after_end = gated_residual(after_start, mixed, gate_logit, gate_bias_end, out_w_end)
    normed = layer_norm(after_end, norm_trans)
    hidden = jax.nn.relu(project(normed, trans_in) + trans_bias).astype(jnp.bfloat16)
    return (after_end.astype(jnp.float32) + project(hidden, trans_out)).astype(jnp.bfloat16)
```

```python
import jax
import jax.numpy as jnp
from jax import lax
from jax.experimental import pallas as pl
from jax.experimental.pallas import tpu as pltpu
from jax.sharding import PartitionSpec as P

F32 = jnp.float32
BF = jnp.bfloat16
AX = ("gx", "gy")
HEADS = 4
HEAD_DIM = 32
LOG2E = 1.4426950408889634
LN2 = 0.6931471805599453
big_negative = 1000000000.0


def attn_body(q_ref, k_ref, vt_ref, b_ref, mask_ref, o_ref, den_ref, qs, eye, ps, *accs):
    h = pl.program_id(1)
    NS = 6
    sacc = [accs[m * (NS + 4): m * (NS + 4) + NS] for m in range(2)]
    oacc = [accs[m * (NS + 4) + NS: (m + 1) * (NS + 4)] for m in range(2)]
    qp = pl.program_id(0)
    lane = lax.broadcasted_iota(jnp.int32, (16, 128), 1) // 32
    masks = [jnp.where(lane == lax.rem(h + r, 4), 1.0, 0.0).astype(BF)[0:1] for r in range(4)]
    rowi = lax.broadcasted_iota(jnp.int32, (128, 128), 0)
    coli = lax.broadcasted_iota(jnp.int32, (128, 128), 1)
    eye[...] = jnp.where(rowi == coli, 1.0, 0.0).astype(BF)
    qrow = pl.multiple_of(qp * 512, 512)
    G = 2
    for g in range(G):
        for m in range(2):
            s = None
            for r in range(4):
                t = q_ref[4 * g + r, pl.ds(qrow + m * 256, 256), :] * masks[r]
                s = t if s is None else s + t
            qs[g, m * 256:(m + 1) * 256, :] = s

    pend = []
    LAG = 4
    unit = [0]
    def pop_one():
        (g, kt, r, sl) = pend.pop(0)
        for m in range(2):
            s = pltpu.matmul_pop(sacc[m][sl])
            p = jnp.exp2(s.astype(BF))
            ps[m, r, (g * 4 + kt // 2) % 2, (kt % 2) * 128:(kt % 2) * 128 + 128, :] = p
    def push_qb(g, kt):
        for m in range(2):
            rhs = jnp.concatenate([qs[g, m * 256:(m + 1) * 256, :], b_ref[0, kt, m * 256:(m + 1) * 256, :]], axis=1)
            pltpu.matmul_push_rhs(rhs, 0, m, transpose=True)
    def push_p(g, kp, r):
        for m in range(2):
            pltpu.matmul_push_rhs(ps[m, r, (g * 4 + kp) % 2], 1, m)
    def pv(g, kp, r):
        i = 4 * g + r
        lhs = vt_ref[i, 0, :, kp * 256:(kp + 1) * 256] * mask_ref[0:1, kp * 256:(kp + 1) * 256]
        for m in range(2):
            pltpu.matmul_acc_lhs(oacc[m][r], lhs, 1)
    def out(g, r):
        i = 4 * g + r
        for m in range(2):
            o = pltpu.matmul_pop(oacc[m][r])
            d = o[32:33, :]
            o_ref[i, :, m * 256:(m + 1) * 256] = o[0:32, :] * (1.0 / d)
            den_ref[0, i:i + 1, m * 256:(m + 1) * 256] = d
    pvq = []
    push_qb(0, 0)
    steps = [(g, kt) for g in range(G) for kt in range(8)]
    staged = None
    for n, (g, kt) in enumerate(steps):
        for r in range(4):
            i = 4 * g + r
            lhs = jnp.concatenate([k_ref[i, kt * 128:(kt + 1) * 128, :] * masks[r], eye[...]], axis=1)
            sl = unit[0] % NS
            unit[0] += 1
            for m in range(2):
                pltpu.matmul_acc_lhs(sacc[m][sl], lhs, 0 if r == 0 else None)
            if r == 0 and n + 1 < len(steps):
                push_qb(*steps[n + 1])
            pend.append((g, kt, r, sl))
            if len(pend) > LAG:
                pop_one()
            if r == 1 and pvq and staged is None:
                staged = pvq.pop(0)
                push_p(*staged)
        if staged is not None:
            done = staged
            pv(*staged); staged = None
            if pvq:
                staged = pvq.pop(0); push_p(*staged); pv(*staged); last = staged; staged = None
            else:
                last = done
            for (gg, kp, r) in ([done] if last is done else [done, last]):
                if kp == 3:
                    out(gg, r)
        if kt % 2 == 1:
            pvq += [(g, kt // 2, r) for r in range(4)]
    while pend:
        pop_one()
    while pvq:
        w = pvq.pop(0); push_p(*w); pv(*w)
        if w[1] == 3: out(w[0], w[2])

def attn_kernel(q_ref, k_ref, vt_ref, b_ref, mask_ref, o_ref, den_ref, qs, eye, ps):
    specs = []
    for m in range(2):
        specs += [pltpu.ACC(m)((128, 256), F32)] * 6 + [pltpu.ACC(m)((48, 256), F32)] * 4
    pl.run_scoped(lambda *accs: attn_body(q_ref, k_ref, vt_ref, b_ref, mask_ref, o_ref, den_ref, qs, eye, ps, *accs), *specs)

def attention(q, k, vt, b, mask16):
    return pl.pallas_call(
        attn_kernel,
        grid=(2, 4),
        in_specs=[
            pl.BlockSpec((8, 1024, 128), lambda a, h: (0, 0, 0)),
            pl.BlockSpec((8, 1024, 128), lambda a, h: (0, 0, 0)),
            pl.BlockSpec((8, 1, 48, 1024), lambda a, h: (0, h, 0, 0)),
            pl.BlockSpec((1, 8, 512, 128), lambda a, h: (h, 0, a, 0)),
            pl.BlockSpec((16, 1024), lambda a, h: (0, 0)),
        ],
        out_specs=[
            pl.BlockSpec((8, 32, 512), lambda a, h: (0, h, a)),
            pl.BlockSpec((1, 8, 512), lambda a, h: (h, 0, a)),
        ],
        out_shape=[jax.ShapeDtypeStruct((8, 128, 1024), F32), jax.ShapeDtypeStruct((4, 8, 1024), F32)],
        scratch_shapes=[pltpu.VMEM((2, 512, 128), BF), pltpu.VMEM((128, 128), BF), pltpu.VMEM((2, 4, 2, 256, 256), BF)],
        compiler_params=pltpu.CompilerParams(vmem_limit_bytes=60 * 2**20),
        name="tri_attn",
    )(q, k, vt, b, mask16)


def layer_norm(x, gain):
    mean = jnp.mean(x, axis=-1, keepdims=True)
    c = x - mean
    var = jnp.mean(c * c, axis=-1, keepdims=True)
    return (c * lax.rsqrt(var + 1e-05) * gain).astype(BF)


def pre_kernel(z_ref, gain_ref, wqk_ref, wvg_ref, bw_ref, gb_ref, q_ref, k_ref, vt_ref, gate_ref, b_ref, m_ref, scr):
    i = pl.program_id(0)
    a = layer_norm(z_ref[0].astype(F32), gain_ref[...])
    qk = jnp.dot(a, wqk_ref[0], preferred_element_type=F32)
    q_ref[0] = (qk[:, :128] * (HEAD_DIM ** -0.5 * LOG2E)).astype(BF)
    k_ref[0] = qk[:, 128:].astype(BF)
    vg = jnp.dot(a, wvg_ref[...], preferred_element_type=F32)
    vt = jnp.transpose(vg[:, :128].astype(BF))
    tail = jnp.where(lax.broadcasted_iota(jnp.int32, (16, 1024), 0) == 0, 1.0, 0.0).astype(BF)
    for h in range(4):
        vt_ref[0, h, 0:32, :] = vt[32 * h:32 * h + 32, :]
        vt_ref[0, h, 32:48, :] = tail
    gate_ref[0] = jax.nn.sigmoid(vg[:, 128:] + gb_ref[...]).astype(BF)
    b = lax.dot_general(bw_ref[...], a, (((1,), (1,)), ((), ())), preferred_element_type=F32)
    b = b.astype(BF).astype(F32)
    m = jnp.max(b, axis=-1, keepdims=True)
    b = (b - m) * LOG2E
    for h in range(4):
        for kt in range(8):
            scr[h, kt, pl.ds(i, 1), :] = b[h:h + 1, kt * 128:(kt + 1) * 128]
    m_ref[0] = jnp.broadcast_to(m, (16, 128))

    @pl.when(i == 7)
    def _():
        b_ref[...] = scr[...].astype(BF)


def pre(z, gain, proj, bias_w, gate_bias):
    wq, wk, wv, wg = [proj[:, 128 * n:128 * n + 128] for n in range(4)]

    def slots(w, i):
        return jnp.concatenate([w[:, 32 * ((s - i) % 4):32 * ((s - i) % 4) + 32] for s in range(4)], axis=1)

    wqk = jnp.stack([jnp.concatenate([slots(wq, i), slots(wk, i)], axis=1) for i in range(4)])
    wvg = jnp.concatenate([wv, wg], axis=1)
    bwt = jnp.pad(jnp.transpose(bias_w), ((0, 12), (0, 0)))
    row = lambda i: (i, 0, 0)
    return pl.pallas_call(
        pre_kernel,
        grid=(8,),
        in_specs=[
            pl.BlockSpec((1, 1024, 128), row),
            pl.BlockSpec((1, 128), lambda i: (0, 0)),
            pl.BlockSpec((1, 128, 256), lambda i: (lax.rem(i, 4), 0, 0)),
            pl.BlockSpec((128, 256), lambda i: (0, 0)),
            pl.BlockSpec((16, 128), lambda i: (0, 0)),
            pl.BlockSpec((1, 128), lambda i: (0, 0)),
        ],
        out_specs=[
            pl.BlockSpec((1, 1024, 128), row),
            pl.BlockSpec((1, 1024, 128), row),
            pl.BlockSpec((1, 4, 48, 1024), lambda i: (i, 0, 0, 0)),
            pl.BlockSpec((1, 1024, 128), row),
            pl.BlockSpec((4, 8, 8, 128), lambda i: (0, 0, 0, 0)),
            pl.BlockSpec((1, 16, 128), row),
        ],
        out_shape=[
            jax.ShapeDtypeStruct((8, 1024, 128), BF),
            jax.ShapeDtypeStruct((8, 1024, 128), BF),
            jax.ShapeDtypeStruct((8, 4, 48, 1024), BF),
            jax.ShapeDtypeStruct((8, 1024, 128), BF),
            jax.ShapeDtypeStruct((4, 8, 8, 128), BF),
            jax.ShapeDtypeStruct((8, 16, 128), F32),
        ],
        scratch_shapes=[pltpu.VMEM((4, 8, 8, 128), F32)],
        compiler_params=pltpu.CompilerParams(vmem_limit_bytes=48 * 2**20),
        name="tri_pre",
    )(z, gain.reshape(1, 128), wqk, wvg, bwt, gate_bias.reshape(1, 128))


def post_kernel(o_ref, gate_ref, z_ref, w_ref, out_ref, scr):
    parts = []
    for i in range(8):
        o = jnp.transpose(o_ref[i])
        parts.append((o * gate_ref[i].astype(F32)).astype(BF))
    y = jnp.dot(jnp.concatenate(parts, axis=0), w_ref[...], preferred_element_type=F32)
    for i in range(8):
        scr[pl.ds(i, 128, stride=8), :] = z_ref[i].astype(F32) + y[128 * i:128 * i + 128]
    out_ref[...] = scr[...].astype(BF)


def post(o, gate, z, w):
    tile = lambda t: (0, t, 0)
    return pl.pallas_call(
        post_kernel,
        grid=(8,),
        in_specs=[
            pl.BlockSpec((8, 128, 128), lambda t: (0, 0, t)),
            pl.BlockSpec((8, 128, 128), tile),
            pl.BlockSpec((8, 128, 128), tile),
            pl.BlockSpec((128, 128), lambda t: (0, 0)),
        ],
        out_specs=pl.BlockSpec((1024, 128), lambda t: (t, 0)),
        out_shape=jax.ShapeDtypeStruct((8192, 128), BF),
        scratch_shapes=[pltpu.VMEM((1024, 128), F32)],
        compiler_params=pltpu.CompilerParams(vmem_limit_bytes=48 * 2**20),
        name="tri_post",
    )(o, gate, z, w)


def trans_kernel(z_ref, gain_ref, w1_ref, b1_ref, w2_ref, out_ref):
    z = z_ref[0].astype(F32)
    a = layer_norm(z, gain_ref[...])
    hid = jax.nn.relu(jnp.dot(a, w1_ref[...], preferred_element_type=F32) + b1_ref[...]).astype(BF)
    out_ref[0] = (z + jnp.dot(hid, w2_ref[...], preferred_element_type=F32)).astype(BF)


def trans(z, gain, w1, b1, w2):
    row = lambda i: (i, 0, 0)
    whole = lambda i: (0, 0)
    return pl.pallas_call(
        trans_kernel,
        grid=(8,),
        in_specs=[
            pl.BlockSpec((1, 1024, 128), row),
            pl.BlockSpec((1, 128), whole),
            pl.BlockSpec((128, 512), whole),
            pl.BlockSpec((1, 512), whole),
            pl.BlockSpec((512, 128), whole),
        ],
        out_specs=pl.BlockSpec((1, 1024, 128), row),
        out_shape=jax.ShapeDtypeStruct((8, 1024, 128), BF),
        compiler_params=pltpu.CompilerParams(vmem_limit_bytes=48 * 2**20),
        name="tri_trans",
    )(z, gain.reshape(1, 128), w1, b1.reshape(1, 512), w2)


def exact_attention(q, k, vt, b, maxima, mask):
    key_bias = (mask - 1.0) * big_negative
    heads = [jnp.array([(h + i) % 4 for h in range(4)]) for i in range(4)]

    def per_row(operands):
        i, q_row, k_row, vt_row = operands
        order = jnp.stack(heads)[lax.rem(i, 4)]
        qh = q_row.reshape(1024, 4, 32)[:, order]
        kh = k_row.reshape(1024, 4, 32)[:, order]

        def per_head(ops):
            qx, kx, vx, bx, mx = ops
            s = jnp.dot(qx, kx.T, preferred_element_type=F32)
            bias = jnp.swapaxes(bx, 0, 1).reshape(1024, 1024).astype(F32)
            s = (s + bias) * LN2 + mx[:, None] + key_bias
            w = jax.nn.softmax(s, axis=-1)
            return jnp.dot(vx[:32].astype(F32), w.T, preferred_element_type=F32)

        o = lax.map(per_head, (jnp.moveaxis(qh, 1, 0), jnp.moveaxis(kh, 1, 0), vt_row, b, maxima))
        return o.reshape(128, 1024)

    return lax.map(per_row, (jnp.arange(8), q, k, vt))


def gather_bias(piece, extra):
    block = jnp.concatenate([piece.reshape(256, 128), extra], axis=0)[None]
    full = lax.all_gather(lax.all_gather(block, "gy", axis=0, tiled=True), "gx", axis=0, tiled=True)
    b = full[:, :256].reshape(128, 4, 8, 8, 128)
    b = jnp.transpose(b, (1, 2, 0, 3, 4)).reshape(4, 8, 1024, 128)
    return b, full[:, 256:]


def swap(z):
    z = z.reshape(128, 8, 8, 128)
    z = lax.all_to_all(z, AX, split_axis=0, concat_axis=0, tiled=True)
    return jnp.swapaxes(z, 0, 1).reshape(8, 1024, 128)


def phase(z, mask_local, gain, proj, gate_bias, bias_w, out_w):
    q, k, vt, gate, piece, m = pre(z, gain, proj, bias_w, gate_bias)
    maxima = jnp.transpose(m[:, :4, 0]).reshape(1, 32)
    extra = jnp.zeros((8, 128), F32)
    extra = extra.at[0:1, 0:8].set(mask_local.astype(F32).reshape(1, 8)).at[1:2, 0:32].set(maxima).astype(BF)
    b, extras = gather_bias(piece, extra)
    mask = extras[:, 0, :8].reshape(1, 1024)
    o, den = attention(q, k, vt, b, jnp.broadcast_to(mask, (16, 1024)))
    fine = jnp.all((den > 2.0 ** -60) & (den < 2.0 ** 100))
    maxima = jnp.transpose(extras[:, 1, :32].reshape(128, 4, 8), (1, 0, 2)).reshape(4, 1024).astype(F32)
    o = lax.cond(
        fine,
        lambda: o,
        lambda: exact_attention(q, k, vt, b, maxima, mask.reshape(1024).astype(F32)),
    )
    return post(o, gate, z, out_w)


def local(
    pair_in,
    residue_mask,
    norm_start,
    proj_start,
    gate_bias_start,
    bias_w_start,
    out_w_start,
    norm_end,
    proj_end,
    gate_bias_end,
    bias_w_end,
    out_w_end,
    norm_trans,
    trans_in,
    trans_bias,
    trans_out,
):
    z = phase(pair_in, residue_mask, norm_start, proj_start, gate_bias_start, bias_w_start, out_w_start)
    z = swap(z)
    z = phase(z, residue_mask, norm_end, proj_end, gate_bias_end, bias_w_end, out_w_end)
    z = swap(z)
    return trans(z, norm_trans, trans_in, trans_bias, trans_out)


def solution(mesh):
    rows = P(AX, None, None)
    placed = (rows, P(AX)) + (P(),) * 14

    def whole(*args):
        with jax.sharding.use_abstract_mesh(mesh.abstract_mesh):
            return jax.shard_map(local, mesh=mesh, in_specs=placed, out_specs=rows, check_vma=False)(*args)

    return whole
```

```python
import jax
import jax.numpy as jnp
from jax import lax
from jax.experimental import pallas as pl
from jax.experimental.pallas import tpu as pltpu
from jax.sharding import PartitionSpec as P

F32 = jnp.float32
BF = jnp.bfloat16
AX = ("gx", "gy")
HEADS = 4
HEAD_DIM = 32
LOG2E = 1.4426950408889634
LN2 = 0.6931471805599453
big_negative = 1000000000.0


def attn_body(q_ref, k_ref, vt_ref, b_ref, extra_ref, o_ref, den_ref, qs, eye, ps, mask_ref, *accs):
    h = pl.program_id(1)

    @pl.when((pl.program_id(0) == 0) & (h == 0))
    def _():
        placed = jnp.sum(extra_ref[0].astype(F32).reshape(8, 16, 8, 128), axis=1)
        for t in range(8):
            mask_ref[:, t * 128:(t + 1) * 128] = jnp.broadcast_to(placed[t, 0:1, :], (16, 128)).astype(BF)

    NS = 6
    sacc = [accs[m * (NS + 4): m * (NS + 4) + NS] for m in range(2)]
    oacc = [accs[m * (NS + 4) + NS: (m + 1) * (NS + 4)] for m in range(2)]
    qp = pl.program_id(0)
    lane = lax.broadcasted_iota(jnp.int32, (16, 128), 1) // 32
    masks = [jnp.where(lane == lax.rem(h + r, 4), 1.0, 0.0).astype(BF)[0:1] for r in range(4)]
    rowi = lax.broadcasted_iota(jnp.int32, (128, 128), 0)
    coli = lax.broadcasted_iota(jnp.int32, (128, 128), 1)
    eye[...] = jnp.where(rowi == coli, 1.0, 0.0).astype(BF)
    qrow = pl.multiple_of(qp * 512, 512)
    G = 2
    for g in range(G):
        for m in range(2):
            s = None
            for r in range(4):
                t = q_ref[4 * g + r, pl.ds(qrow + m * 256, 256), :] * masks[r]
                s = t if s is None else s + t
            qs[g, m * 256:(m + 1) * 256, :] = s

    pend = []
    LAG = 4
    unit = [0]
    def pop_one():
        (g, kt, r, sl) = pend.pop(0)
        for m in range(2):
            s = pltpu.matmul_pop(sacc[m][sl])
            p = jnp.exp2(s.astype(BF))
            ps[m, r, (g * 4 + kt // 2) % 2, (kt % 2) * 128:(kt % 2) * 128 + 128, :] = p
    def push_qb(g, kt):
        for m in range(2):
            rhs = jnp.concatenate([qs[g, m * 256:(m + 1) * 256, :], b_ref[kt, m * 256:(m + 1) * 256, :]], axis=1)
            pltpu.matmul_push_rhs(rhs, 0, m, transpose=True)
    def push_p(g, kp, r):
        for m in range(2):
            pltpu.matmul_push_rhs(ps[m, r, (g * 4 + kp) % 2], 1, m)
    def pv(g, kp, r):
        i = 4 * g + r
        keep = mask_ref[:, kp * 256:(kp + 1) * 256]
        lhs = vt_ref[i, 0, :, kp * 256:(kp + 1) * 256] * jnp.concatenate([keep] * 3, axis=0)
        for m in range(2):
            pltpu.matmul_acc_lhs(oacc[m][r], lhs, 1)
    def out(g, r):
        i = 4 * g + r
        for m in range(2):
            o = pltpu.matmul_pop(oacc[m][r])
            d = o[32:33, :]
            o_ref[i, :, m * 256:(m + 1) * 256] = o[0:32, :] * (1.0 / d)
            den_ref[0, i:i + 1, m * 256:(m + 1) * 256] = d
    pvq = []
    push_qb(0, 0)
    steps = [(g, kt) for g in range(G) for kt in range(8)]
    staged = None
    for n, (g, kt) in enumerate(steps):
        for r in range(4):
            i = 4 * g + r
            lhs = jnp.concatenate([k_ref[i, kt * 128:(kt + 1) * 128, :] * masks[r], eye[...]], axis=1)
            sl = unit[0] % NS
            unit[0] += 1
            for m in range(2):
                pltpu.matmul_acc_lhs(sacc[m][sl], lhs, 0 if r == 0 else None)
            if r == 0 and n + 1 < len(steps):
                push_qb(*steps[n + 1])
            pend.append((g, kt, r, sl))
            if len(pend) > LAG:
                pop_one()
            if r == 1 and pvq and staged is None:
                staged = pvq.pop(0)
                push_p(*staged)
        if staged is not None:
            done = staged
            pv(*staged); staged = None
            if pvq:
                staged = pvq.pop(0); push_p(*staged); pv(*staged); last = staged; staged = None
            else:
                last = done
            for (gg, kp, r) in ([done] if last is done else [done, last]):
                if kp == 3:
                    out(gg, r)
        if kt % 2 == 1:
            pvq += [(g, kt // 2, r) for r in range(4)]
    while pend:
        pop_one()
    while pvq:
        w = pvq.pop(0); push_p(*w); pv(*w)
        if w[1] == 3: out(w[0], w[2])

def attn_kernel(q_ref, k_ref, vt_ref, b_ref, extra_ref, o_ref, den_ref, qs, eye, ps, mask_ref):
    specs = []
    for m in range(2):
        specs += [pltpu.ACC(m)((128, 256), F32)] * 6 + [pltpu.ACC(m)((48, 256), F32)] * 4
    pl.run_scoped(lambda *accs: attn_body(q_ref, k_ref, vt_ref, b_ref, extra_ref, o_ref, den_ref, qs, eye, ps, mask_ref, *accs), *specs)

def attention(q, k, vt, b):
    return pl.pallas_call(
        attn_kernel,
        grid=(2, 4),
        in_specs=[
            pl.BlockSpec((8, 1024, 128), lambda a, h: (0, 0, 0)),
            pl.BlockSpec((8, 1024, 128), lambda a, h: (0, 0, 0)),
            pl.BlockSpec((8, 1, 48, 1024), lambda a, h: (0, h, 0, 0)),
            pl.BlockSpec((8, 512, 128), lambda a, h: (h, a, 0)),
            pl.BlockSpec((1, 1024, 128), lambda a, h: (32, 0, 0)),
        ],
        out_specs=[
            pl.BlockSpec((8, 32, 512), lambda a, h: (0, h, a)),
            pl.BlockSpec((1, 8, 512), lambda a, h: (h, 0, a)),
        ],
        out_shape=[jax.ShapeDtypeStruct((8, 128, 1024), F32), jax.ShapeDtypeStruct((4, 8, 1024), F32)],
        scratch_shapes=[pltpu.VMEM((2, 512, 128), BF), pltpu.VMEM((128, 128), BF), pltpu.VMEM((2, 4, 2, 256, 256), BF), pltpu.VMEM((16, 1024), BF)],
        compiler_params=pltpu.CompilerParams(vmem_limit_bytes=60 * 2**20),
        name="tri_attn",
    )(q, k, vt, b, b)


MESH_ID = pl.DeviceIdType.MESH
ORDERS = ((0, 1, 2), (1, 2, 0), (2, 0, 1))


def gather_kernel(piece_ref, out_ref, full, send_sem, recv_sem, out_sem):
    gx, gy = lax.axis_index("gx"), lax.axis_index("gy")
    core = lax.rem(gx, 2)
    x = lax.rem(gx // 2, 4)
    y = gy // 2
    z = lax.rem(gy, 2) * 2 + gx // 8
    here = (x, y, z)

    def device(pos, c):
        px, py, pz = pos
        return ((lax.rem(pz, 2) * 4 + px) * 2 + c, py * 2 + pz // 2)

    def moved(dim, step):
        pos = list(here)
        pos[dim] = lax.rem(pos[dim] + step + 4, 4)
        return tuple(pos)

    def region(lo, hi, pos, done):
        px, py, pz = pos
        zl = slice(None) if 2 in done else lax.rem(pz, 2)
        zh = slice(None) if 2 in done else pz // 2
        xi = slice(None) if 0 in done else px
        yi = slice(None) if 1 in done else py
        return full.at[lo:hi, zl, xi, core, yi, zh]

    barrier = pltpu.get_barrier_semaphore()
    partner = device(here, 1 - core)
    peers = [device(moved(d, s), core) for d in range(3) for s in (1, 3)] + [partner]
    for peer in peers:
        pl.semaphore_signal(barrier, inc=1, device_id=peer, device_id_type=MESH_ID)
    full[:, lax.rem(z, 2), x, core, y, z // 2] = piece_ref[...]
    pl.semaphore_wait(barrier, 7)

    slots = [0]
    started = []

    def copy(src, dst, dev):
        n = slots[0]
        slots[0] += 1
        return pltpu.make_async_remote_copy(
            src_ref=src, dst_ref=dst, send_sem=send_sem.at[n], recv_sem=recv_sem.at[n],
            device_id=dev, device_id_type=MESH_ID)

    def send(lo, hi, pos, done, dev, first=False):
        spot = region(lo, hi, pos, done)
        c = copy(piece_ref.at[lo:hi] if first else spot, spot, dev)
        c.start()
        started.append(c)
        return c

    def arrival(n, lo, hi, pos, done):
        spot = region(lo, hi, pos, done)
        pltpu.make_async_remote_copy(
            src_ref=spot, dst_ref=spot, send_sem=send_sem.at[n], recv_sem=recv_sem.at[n],
            device_id=partner, device_id_type=MESH_ID).wait_recv()

    partner_waits = []

    def share(lo, hi, pos, done, first=False):
        n = slots[0]
        send(lo, hi, pos, done, partner, first)
        partner_waits.append((n, lo, hi, pos, done))

    for stage in range(3):
        tags = []
        for part in range(3):
            order = ORDERS[part]
            dim, done = order[stage], order[:stage]
            lo, hi = 11 * part, 11 * part + 11
            right, left = device(moved(dim, 1), core), device(moved(dim, 3), core)
            n = slots[0]
            send(lo, hi, here, done, right, stage == 0)
            send(lo, hi, here, done, left, stage == 0)
            tags.append((n, lo, hi, dim, done, right, left))
        if stage == 0:
            share(0, 33, here, (), True)
        halves = []
        for n, lo, hi, dim, done, right, left in tags:
            mid = lo + 6
            h = slots[0]
            arrival(n, lo, hi, moved(dim, 3), done)
            send(lo, mid, moved(dim, 3), done, right)
            arrival(n + 1, lo, hi, moved(dim, 1), done)
            send(mid, hi, moved(dim, 1), done, left)
            share(lo, hi, moved(dim, 3), done)
            share(lo, hi, moved(dim, 1), done)
            halves.append((h, lo, mid, hi, dim, done))
        for h, lo, mid, hi, dim, done in halves:
            arrival(h, lo, mid, moved(dim, 2), done)
            arrival(h + 1, mid, hi, moved(dim, 2), done)
            share(lo, hi, moved(dim, 2), done)

    def partner_region(lo, hi, pos, done):
        px, py, pz = pos
        zl = slice(None) if 2 in done else lax.rem(pz, 2)
        zh = slice(None) if 2 in done else pz // 2
        xi = slice(None) if 0 in done else px
        yi = slice(None) if 1 in done else py
        return full.at[lo:hi, zl, xi, 1 - core, yi, zh]

    for n, lo, hi, pos, done in partner_waits:
        spot = partner_region(lo, hi, pos, done)
        pltpu.make_async_remote_copy(
            src_ref=spot, dst_ref=spot, send_sem=send_sem.at[n], recv_sem=recv_sem.at[n],
            device_id=partner, device_id_type=MESH_ID).wait_recv()
    outs = [pltpu.make_async_copy(full.at[11 * p:11 * p + 11], out_ref.at[11 * p:11 * p + 11], out_sem.at[p]) for p in range(3)]
    for c in outs:
        c.start()
    for c in started:
        c.wait_send()
    for c in outs:
        c.wait()


def gather(piece, collective_id):
    shape = (33, 2, 4, 2, 4, 2, 8, 128)
    n = 64
    out = pl.pallas_call(
        gather_kernel,
        in_specs=[pl.BlockSpec(memory_space=pltpu.VMEM)],
        out_specs=pl.BlockSpec(memory_space=pl.ANY),
        out_shape=jax.ShapeDtypeStruct(shape, BF),
        scratch_shapes=[
            pltpu.VMEM(shape, BF),
            pltpu.SemaphoreType.DMA((n,)),
            pltpu.SemaphoreType.DMA((n,)),
            pltpu.SemaphoreType.DMA((3,)),
        ],
        compiler_params=pltpu.CompilerParams(collective_id=collective_id, has_side_effects=True, vmem_limit_bytes=24 * 2**20),
        name="tri_gather",
    )(piece)
    return out.reshape(33, 1024, 128)


def layer_norm(x, gain):
    mean = jnp.mean(x, axis=-1, keepdims=True)
    c = x - mean
    var = jnp.mean(c * c, axis=-1, keepdims=True)
    return (c * lax.rsqrt(var + 1e-05) * gain).astype(BF)


def pre_kernel(z_ref, gain_ref, wqk_ref, wvg_ref, bw_ref, gb_ref, mask_ref, q_ref, k_ref, vt_ref, gate_ref, b_ref, scr):
    i = pl.program_id(0)

    @pl.when(i == 0)
    def _():
        scr[32] = mask_ref[...]

    a = layer_norm(z_ref[0].astype(F32), gain_ref[...])
    qk = jnp.dot(a, wqk_ref[0], preferred_element_type=F32)
    q_ref[0] = (qk[:, :128] * (HEAD_DIM ** -0.5 * LOG2E)).astype(BF)
    k_ref[0] = qk[:, 128:].astype(BF)
    vg = jnp.dot(a, wvg_ref[...], preferred_element_type=F32)
    vt = jnp.transpose(vg[:, :128].astype(BF))
    tail = jnp.where(lax.broadcasted_iota(jnp.int32, (16, 1024), 0) == 0, 1.0, 0.0).astype(BF)
    for h in range(4):
        vt_ref[0, h, 0:32, :] = vt[32 * h:32 * h + 32, :]
        vt_ref[0, h, 32:48, :] = tail
    gate_ref[0] = jax.nn.sigmoid(vg[:, 128:] + gb_ref[...]).astype(BF)
    b = lax.dot_general(bw_ref[...], a, (((1,), (1,)), ((), ())), preferred_element_type=F32)
    b = b.astype(BF).astype(F32)
    m = jnp.max(b, axis=-1, keepdims=True)
    b = (b - m) * LOG2E
    for h in range(4):
        for kt in range(8):
            scr[8 * h + kt, pl.ds(i, 1), :] = b[h:h + 1, kt * 128:(kt + 1) * 128]
    lane = lax.broadcasted_iota(jnp.int32, (4, 128), 1)
    scr[32, 1:5, :] = jnp.where(lane == i, m[0:4], scr[32, 1:5, :])

    @pl.when(i == 7)
    def _():
        b_ref[...] = scr[...].astype(BF)


def pre(z, gain, proj, bias_w, gate_bias, mask_tile):
    wq, wk, wv, wg = [proj[:, 128 * n:128 * n + 128] for n in range(4)]

    def slots(w, i):
        return jnp.concatenate([w[:, 32 * ((s - i) % 4):32 * ((s - i) % 4) + 32] for s in range(4)], axis=1)

    wqk = jnp.stack([jnp.concatenate([slots(wq, i), slots(wk, i)], axis=1) for i in range(4)])
    wvg = jnp.concatenate([wv, wg], axis=1)
    bwt = jnp.pad(jnp.transpose(bias_w), ((0, 12), (0, 0)))
    row = lambda i: (i, 0, 0)
    return pl.pallas_call(
        pre_kernel,
        grid=(8,),
        in_specs=[
            pl.BlockSpec((1, 1024, 128), row),
            pl.BlockSpec((1, 128), lambda i: (0, 0)),
            pl.BlockSpec((1, 128, 256), lambda i: (lax.rem(i, 4), 0, 0)),
            pl.BlockSpec((128, 256), lambda i: (0, 0)),
            pl.BlockSpec((16, 128), lambda i: (0, 0)),
            pl.BlockSpec((1, 128), lambda i: (0, 0)),
            pl.BlockSpec((8, 128), lambda i: (0, 0)),
        ],
        out_specs=[
            pl.BlockSpec((1, 1024, 128), row),
            pl.BlockSpec((1, 1024, 128), row),
            pl.BlockSpec((1, 4, 48, 1024), lambda i: (i, 0, 0, 0)),
            pl.BlockSpec((1, 1024, 128), row),
            pl.BlockSpec((33, 8, 128), lambda i: (0, 0, 0)),
        ],
        out_shape=[
            jax.ShapeDtypeStruct((8, 1024, 128), BF),
            jax.ShapeDtypeStruct((8, 1024, 128), BF),
            jax.ShapeDtypeStruct((8, 4, 48, 1024), BF),
            jax.ShapeDtypeStruct((8, 1024, 128), BF),
            jax.ShapeDtypeStruct((33, 8, 128), BF),
        ],
        scratch_shapes=[pltpu.VMEM((33, 8, 128), F32)],
        compiler_params=pltpu.CompilerParams(vmem_limit_bytes=48 * 2**20),
        name="tri_pre",
    )(z, gain.reshape(1, 128), wqk, wvg, bwt, gate_bias.reshape(1, 128), mask_tile)


def post_kernel(o_ref, gate_ref, z_ref, w_ref, out_ref, scr):
    parts = []
    for i in range(8):
        o = jnp.transpose(o_ref[i])
        parts.append((o * gate_ref[i].astype(F32)).astype(BF))
    y = jnp.dot(jnp.concatenate(parts, axis=0), w_ref[...], preferred_element_type=F32)
    for i in range(8):
        scr[pl.ds(i, 128, stride=8), :] = z_ref[i].astype(F32) + y[128 * i:128 * i + 128]
    out_ref[...] = scr[...].astype(BF)


def post(o, gate, z, w):
    tile = lambda t: (0, t, 0)
    return pl.pallas_call(
        post_kernel,
        grid=(8,),
        in_specs=[
            pl.BlockSpec((8, 128, 128), lambda t: (0, 0, t)),
            pl.BlockSpec((8, 128, 128), tile),
            pl.BlockSpec((8, 128, 128), tile),
            pl.BlockSpec((128, 128), lambda t: (0, 0)),
        ],
        out_specs=pl.BlockSpec((1024, 128), lambda t: (t, 0)),
        out_shape=jax.ShapeDtypeStruct((8192, 128), BF),
        scratch_shapes=[pltpu.VMEM((1024, 128), F32)],
        compiler_params=pltpu.CompilerParams(vmem_limit_bytes=48 * 2**20),
        name="tri_post",
    )(o, gate, z, w)


def trans_kernel(z_ref, gain_ref, w1_ref, b1_ref, w2_ref, out_ref):
    z = z_ref[0].astype(F32)
    a = layer_norm(z, gain_ref[...])
    hid = jax.nn.relu(jnp.dot(a, w1_ref[...], preferred_element_type=F32) + b1_ref[...]).astype(BF)
    out_ref[0] = (z + jnp.dot(hid, w2_ref[...], preferred_element_type=F32)).astype(BF)


def trans(z, gain, w1, b1, w2):
    row = lambda i: (i, 0, 0)
    whole = lambda i: (0, 0)
    return pl.pallas_call(
        trans_kernel,
        grid=(8,),
        in_specs=[
            pl.BlockSpec((1, 1024, 128), row),
            pl.BlockSpec((1, 128), whole),
            pl.BlockSpec((128, 512), whole),
            pl.BlockSpec((1, 512), whole),
            pl.BlockSpec((512, 128), whole),
        ],
        out_specs=pl.BlockSpec((1, 1024, 128), row),
        out_shape=jax.ShapeDtypeStruct((8, 1024, 128), BF),
        compiler_params=pltpu.CompilerParams(vmem_limit_bytes=48 * 2**20),
        name="tri_trans",
    )(z, gain.reshape(1, 128), w1, b1.reshape(1, 512), w2)


def exact_attention(q, k, vt, full):
    extra = full[32].reshape(128, 8, 128)
    mask = jnp.sum(extra[:, 0].reshape(8, 16, 128).astype(F32), axis=1).reshape(1024)
    maxima = jnp.transpose(extra[:, 1:5, :8], (1, 0, 2)).reshape(4, 1024).astype(F32)
    key_bias = (mask - 1.0) * big_negative
    b = full[:32].reshape(4, 8, 1024, 128)
    orders = jnp.array([[(h + i) % 4 for h in range(4)] for i in range(4)])

    def per_row(operands):
        i, q_row, k_row, vt_row = operands
        order = orders[lax.rem(i, 4)]
        qh = q_row.reshape(1024, 4, 32)[:, order]
        kh = k_row.reshape(1024, 4, 32)[:, order]

        def per_head(ops):
            qx, kx, vx, bx, mx = ops
            s = jnp.dot(qx, kx.T, preferred_element_type=F32)
            bias = jnp.swapaxes(bx, 0, 1).reshape(1024, 1024).astype(F32)
            s = (s + bias) * LN2 + mx[:, None] + key_bias
            w = jax.nn.softmax(s, axis=-1)
            return jnp.dot(vx[:32].astype(F32), w.T, preferred_element_type=F32)

        o = lax.map(per_head, (jnp.moveaxis(qh, 1, 0), jnp.moveaxis(kh, 1, 0), vt_row, b, maxima))
        return o.reshape(128, 1024)

    return lax.map(per_row, (jnp.arange(8), q, k, vt))


def swap(z):
    z = z.reshape(128, 8, 8, 128)
    z = lax.all_to_all(z, AX, split_axis=0, concat_axis=0, tiled=True)
    return jnp.swapaxes(z, 0, 1).reshape(8, 1024, 128)


def phase(z, mask_tile, gain, proj, gate_bias, bias_w, out_w, collective_id):
    q, k, vt, gate, piece = pre(z, gain, proj, bias_w, gate_bias, mask_tile)
    full = gather(piece, collective_id)
    o, den = attention(q, k, vt, full)
    fine = jnp.all((den > 2.0 ** -60) & (den < 2.0 ** 100))
    o = lax.cond(fine, lambda: o, lambda: exact_attention(q, k, vt, full))
    return post(o, gate, z, out_w)


def local(
    pair_in,
    residue_mask,
    norm_start,
    proj_start,
    gate_bias_start,
    bias_w_start,
    out_w_start,
    norm_end,
    proj_end,
    gate_bias_end,
    bias_w_end,
    out_w_end,
    norm_trans,
    trans_in,
    trans_bias,
    trans_out,
):
    device = lax.axis_index("gx") * 8 + lax.axis_index("gy")
    lane = lax.broadcasted_iota(jnp.int32, (8, 128), 1)
    row = lax.broadcasted_iota(jnp.int32, (8, 128), 0)
    spread = jnp.tile(residue_mask.astype(F32), 16).reshape(1, 128)
    mask_tile = jnp.where((lane // 8 == lax.rem(device, 16)) & (row == 0), spread, 0.0)
    z = phase(pair_in, mask_tile, norm_start, proj_start, gate_bias_start, bias_w_start, out_w_start, 0)
    z = swap(z)
    z = phase(z, mask_tile, norm_end, proj_end, gate_bias_end, bias_w_end, out_w_end, 1)
    z = swap(z)
    return trans(z, norm_trans, trans_in, trans_bias, trans_out)


def solution(mesh):
    rows = P(AX, None, None)
    placed = (rows, P(AX)) + (P(),) * 14

    def whole(*args):
        with jax.sharding.use_abstract_mesh(mesh.abstract_mesh):
            return jax.shard_map(local, mesh=mesh, in_specs=placed, out_specs=rows, check_vma=False)(*args)

    return whole
```

```python
import jax
import jax.numpy as jnp
from jax import lax
from jax.experimental import pallas as pl
from jax.experimental.pallas import tpu as pltpu
from jax.sharding import PartitionSpec as P

F32 = jnp.float32
BF = jnp.bfloat16
AX = ("gx", "gy")
HEADS = 4
HEAD_DIM = 32
LOG2E = 1.4426950408889634
LN2 = 0.6931471805599453
big_negative = 1000000000.0


def attn_body(q_ref, k_ref, vt_ref, b_ref, extra_ref, o_ref, den_ref, qs, eye, ps, mask_ref, *accs):
    h = pl.program_id(1)

    @pl.when((pl.program_id(0) == 0) & (h == 0))
    def _():
        placed = jnp.sum(extra_ref[0].astype(F32).reshape(8, 16, 8, 128), axis=1)
        for t in range(8):
            mask_ref[:, t * 128:(t + 1) * 128] = jnp.broadcast_to(placed[t, 0:1, :], (16, 128)).astype(BF)

    NS = 6
    sacc = [accs[m * (NS + 4): m * (NS + 4) + NS] for m in range(2)]
    oacc = [accs[m * (NS + 4) + NS: (m + 1) * (NS + 4)] for m in range(2)]
    qp = pl.program_id(0)
    lane = lax.broadcasted_iota(jnp.int32, (16, 128), 1) // 32
    masks = [jnp.where(lane == lax.rem(h + r, 4), 1.0, 0.0).astype(BF)[0:1] for r in range(4)]
    rowi = lax.broadcasted_iota(jnp.int32, (128, 128), 0)
    coli = lax.broadcasted_iota(jnp.int32, (128, 128), 1)
    eye[...] = jnp.where(rowi == coli, 1.0, 0.0).astype(BF)
    qrow = pl.multiple_of(qp * 512, 512)
    G = 2
    for g in range(G):
        for m in range(2):
            s = None
            for r in range(4):
                t = q_ref[4 * g + r, pl.ds(qrow + m * 256, 256), :] * masks[r]
                s = t if s is None else s + t
            qs[g, m * 256:(m + 1) * 256, :] = s

    pend = []
    LAG = 4
    unit = [0]
    def pop_one():
        (g, kt, r, sl) = pend.pop(0)
        for m in range(2):
            s = pltpu.matmul_pop(sacc[m][sl])
            p = jnp.exp2(s.astype(BF))
            ps[m, r, (g * 4 + kt // 2) % 2, (kt % 2) * 128:(kt % 2) * 128 + 128, :] = p
    def push_qb(g, kt):
        for m in range(2):
            rhs = jnp.concatenate([qs[g, m * 256:(m + 1) * 256, :], b_ref[kt, m * 256:(m + 1) * 256, :]], axis=1)
            pltpu.matmul_push_rhs(rhs, 0, m, transpose=True)
    def push_p(g, kp, r):
        for m in range(2):
            pltpu.matmul_push_rhs(ps[m, r, (g * 4 + kp) % 2], 1, m)
    def pv(g, kp, r):
        i = 4 * g + r
        keep = mask_ref[:, kp * 256:(kp + 1) * 256]
        lhs = vt_ref[i, 0, :, kp * 256:(kp + 1) * 256] * jnp.concatenate([keep] * 3, axis=0)
        for m in range(2):
            pltpu.matmul_acc_lhs(oacc[m][r], lhs, 1)
    def out(g, r):
        i = 4 * g + r
        for m in range(2):
            o = pltpu.matmul_pop(oacc[m][r])
            d = o[32:33, :]
            o_ref[i, :, m * 256:(m + 1) * 256] = o[0:32, :] * (1.0 / d)
            den_ref[0, i:i + 1, m * 256:(m + 1) * 256] = d
    pvq = []
    push_qb(0, 0)
    steps = [(g, kt) for g in range(G) for kt in range(8)]
    staged = None
    for n, (g, kt) in enumerate(steps):
        for r in range(4):
            i = 4 * g + r
            lhs = jnp.concatenate([k_ref[i, kt * 128:(kt + 1) * 128, :] * masks[r], eye[...]], axis=1)
            sl = unit[0] % NS
            unit[0] += 1
            for m in range(2):
                pltpu.matmul_acc_lhs(sacc[m][sl], lhs, 0 if r == 0 else None)
            if r == 0 and n + 1 < len(steps):
                push_qb(*steps[n + 1])
            pend.append((g, kt, r, sl))
            if len(pend) > LAG:
                pop_one()
            if r == 1 and pvq and staged is None:
                staged = pvq.pop(0)
                push_p(*staged)
        if staged is not None:
            done = staged
            pv(*staged); staged = None
            if pvq:
                staged = pvq.pop(0); push_p(*staged); pv(*staged); last = staged; staged = None
            else:
                last = done
            for (gg, kp, r) in ([done] if last is done else [done, last]):
                if kp == 3:
                    out(gg, r)
        if kt % 2 == 1:
            pvq += [(g, kt // 2, r) for r in range(4)]
    while pend:
        pop_one()
    while pvq:
        w = pvq.pop(0); push_p(*w); pv(*w)
        if w[1] == 3: out(w[0], w[2])

def attn_kernel(q_ref, k_ref, vt_ref, b_ref, extra_ref, o_ref, den_ref, qs, eye, ps, mask_ref):
    specs = []
    for m in range(2):
        specs += [pltpu.ACC(m)((128, 256), F32)] * 6 + [pltpu.ACC(m)((48, 256), F32)] * 4
    pl.run_scoped(lambda *accs: attn_body(q_ref, k_ref, vt_ref, b_ref, extra_ref, o_ref, den_ref, qs, eye, ps, mask_ref, *accs), *specs)

def attention(q, k, vt, b):
    return pl.pallas_call(
        attn_kernel,
        grid=(2, 4),
        in_specs=[
            pl.BlockSpec((8, 1024, 128), lambda a, h: (0, 0, 0)),
            pl.BlockSpec((8, 1024, 128), lambda a, h: (0, 0, 0)),
            pl.BlockSpec((8, 1, 48, 1024), lambda a, h: (0, h, 0, 0)),
            pl.BlockSpec((8, 512, 128), lambda a, h: (h, a, 0)),
            pl.BlockSpec((1, 1024, 128), lambda a, h: (32, 0, 0)),
        ],
        out_specs=[
            pl.BlockSpec((8, 32, 512), lambda a, h: (0, h, a)),
            pl.BlockSpec((1, 8, 512), lambda a, h: (h, 0, a)),
        ],
        out_shape=[jax.ShapeDtypeStruct((8, 128, 1024), F32), jax.ShapeDtypeStruct((4, 8, 1024), F32)],
        scratch_shapes=[pltpu.VMEM((2, 512, 128), BF), pltpu.VMEM((128, 128), BF), pltpu.VMEM((2, 4, 2, 256, 256), BF), pltpu.VMEM((16, 1024), BF)],
        compiler_params=pltpu.CompilerParams(vmem_limit_bytes=60 * 2**20),
        name="tri_attn",
    )(q, k, vt, b, b)


MESH_ID = pl.DeviceIdType.MESH
ORDERS = ((0, 1, 2), (1, 2, 0), (2, 0, 1))


def gather_kernel(piece_ref, out_ref, full, send_sem, recv_sem, out_sem):
    gx, gy = lax.axis_index("gx"), lax.axis_index("gy")
    core = lax.rem(gx, 2)
    x = lax.rem(gx // 2, 4)
    y = gy // 2
    z = lax.rem(gy, 2) * 2 + gx // 8
    here = (x, y, z)

    def device(pos, c):
        px, py, pz = pos
        return ((lax.rem(pz, 2) * 4 + px) * 2 + c, py * 2 + pz // 2)

    def moved(dim, step):
        pos = list(here)
        pos[dim] = lax.rem(pos[dim] + step + 4, 4)
        return tuple(pos)

    def region(lo, hi, pos, done):
        px, py, pz = pos
        zl = slice(None) if 2 in done else lax.rem(pz, 2)
        zh = slice(None) if 2 in done else pz // 2
        xi = slice(None) if 0 in done else px
        yi = slice(None) if 1 in done else py
        return full.at[lo:hi, zl, xi, core, yi, zh]

    barrier = pltpu.get_barrier_semaphore()
    partner = device(here, 1 - core)
    peers = [device(moved(d, s), core) for d in range(3) for s in (1, 3)] + [partner]
    for peer in peers:
        pl.semaphore_signal(barrier, inc=1, device_id=peer, device_id_type=MESH_ID)
    full[:, lax.rem(z, 2), x, core, y, z // 2] = piece_ref[...]
    pl.semaphore_wait(barrier, 7)

    slots = [0]
    started = []

    def copy(src, dst, dev):
        n = slots[0]
        slots[0] += 1
        return pltpu.make_async_remote_copy(
            src_ref=src, dst_ref=dst, send_sem=send_sem.at[n], recv_sem=recv_sem.at[n],
            device_id=dev, device_id_type=MESH_ID)

    def send(lo, hi, pos, done, dev, first=False):
        spot = region(lo, hi, pos, done)
        c = copy(piece_ref.at[lo:hi] if first else spot, spot, dev)
        c.start()
        started.append(c)
        return c

    def arrival(n, lo, hi, pos, done):
        spot = region(lo, hi, pos, done)
        pltpu.make_async_remote_copy(
            src_ref=spot, dst_ref=spot, send_sem=send_sem.at[n], recv_sem=recv_sem.at[n],
            device_id=partner, device_id_type=MESH_ID).wait_recv()

    partner_waits = []

    def share(lo, hi, pos, done, first=False):
        n = slots[0]
        send(lo, hi, pos, done, partner, first)
        partner_waits.append((n, lo, hi, pos, done))

    for stage in range(3):
        tags = []
        for part in range(3):
            order = ORDERS[part]
            dim, done = order[stage], order[:stage]
            lo, hi = 11 * part, 11 * part + 11
            right, left = device(moved(dim, 1), core), device(moved(dim, 3), core)
            n = slots[0]
            send(lo, hi, here, done, right, stage == 0)
            send(lo, hi, here, done, left, stage == 0)
            tags.append((n, lo, hi, dim, done, right, left))
        if stage == 0:
            share(0, 33, here, (), True)
        halves = []
        for n, lo, hi, dim, done, right, left in tags:
            mid = lo + 6
            h = slots[0]
            arrival(n, lo, hi, moved(dim, 3), done)
            send(lo, mid, moved(dim, 3), done, right)
            arrival(n + 1, lo, hi, moved(dim, 1), done)
            send(mid, hi, moved(dim, 1), done, left)
            share(lo, hi, moved(dim, 3), done)
            share(lo, hi, moved(dim, 1), done)
            halves.append((h, lo, mid, hi, dim, done))
        for h, lo, mid, hi, dim, done in halves:
            arrival(h, lo, mid, moved(dim, 2), done)
            arrival(h + 1, mid, hi, moved(dim, 2), done)
            share(lo, hi, moved(dim, 2), done)

    def partner_region(lo, hi, pos, done):
        px, py, pz = pos
        zl = slice(None) if 2 in done else lax.rem(pz, 2)
        zh = slice(None) if 2 in done else pz // 2
        xi = slice(None) if 0 in done else px
        yi = slice(None) if 1 in done else py
        return full.at[lo:hi, zl, xi, 1 - core, yi, zh]

    for n, lo, hi, pos, done in partner_waits:
        spot = partner_region(lo, hi, pos, done)
        pltpu.make_async_remote_copy(
            src_ref=spot, dst_ref=spot, send_sem=send_sem.at[n], recv_sem=recv_sem.at[n],
            device_id=partner, device_id_type=MESH_ID).wait_recv()
    outs = [pltpu.make_async_copy(full.at[11 * p:11 * p + 11], out_ref.at[11 * p:11 * p + 11], out_sem.at[p]) for p in range(3)]
    for c in outs:
        c.start()
    for c in started:
        c.wait_send()
    for c in outs:
        c.wait()


def gather(piece, collective_id):
    shape = (33, 2, 4, 2, 4, 2, 8, 128)
    n = 64
    out = pl.pallas_call(
        gather_kernel,
        in_specs=[pl.BlockSpec(memory_space=pltpu.VMEM)],
        out_specs=pl.BlockSpec(memory_space=pl.ANY),
        out_shape=jax.ShapeDtypeStruct(shape, BF),
        scratch_shapes=[
            pltpu.VMEM(shape, BF),
            pltpu.SemaphoreType.DMA((n,)),
            pltpu.SemaphoreType.DMA((n,)),
            pltpu.SemaphoreType.DMA((3,)),
        ],
        compiler_params=pltpu.CompilerParams(collective_id=collective_id, has_side_effects=True, vmem_limit_bytes=24 * 2**20),
        name="tri_gather",
    )(piece)
    return out.reshape(33, 1024, 128)


def layer_norm(x, gain):
    mean = jnp.mean(x, axis=-1, keepdims=True)
    c = x - mean
    var = jnp.mean(c * c, axis=-1, keepdims=True)
    return (c * lax.rsqrt(var + 1e-05) * gain).astype(BF)


def pre_kernel(z_ref, gain_ref, wqk_ref, wvg_ref, bw_ref, gb_ref, mask_ref, q_ref, k_ref, vt_ref, gate_ref, b_ref, scr):
    i = pl.program_id(0)

    @pl.when(i == 0)
    def _():
        scr[32] = mask_ref[...]

    a = layer_norm(z_ref[0].astype(F32), gain_ref[...])
    qk = jnp.dot(a, wqk_ref[0], preferred_element_type=F32)
    q_ref[0] = (qk[:, :128] * (HEAD_DIM ** -0.5 * LOG2E)).astype(BF)
    k_ref[0] = qk[:, 128:].astype(BF)
    vg = jnp.dot(a, wvg_ref[...], preferred_element_type=F32)
    vt = jnp.transpose(vg[:, :128].astype(BF))
    tail = jnp.where(lax.broadcasted_iota(jnp.int32, (16, 1024), 0) == 0, 1.0, 0.0).astype(BF)
    for h in range(4):
        vt_ref[0, h, 0:32, :] = vt[32 * h:32 * h + 32, :]
        vt_ref[0, h, 32:48, :] = tail
    gate_ref[0] = jax.nn.sigmoid(vg[:, 128:] + gb_ref[...]).astype(BF)
    b = lax.dot_general(bw_ref[...], a, (((1,), (1,)), ((), ())), preferred_element_type=F32)
    b = b.astype(BF).astype(F32)
    m = jnp.max(b, axis=-1, keepdims=True)
    b = (b - m) * LOG2E
    for h in range(4):
        for kt in range(8):
            scr[8 * h + kt, pl.ds(i, 1), :] = b[h:h + 1, kt * 128:(kt + 1) * 128]
    lane = lax.broadcasted_iota(jnp.int32, (4, 128), 1)
    scr[32, 1:5, :] = jnp.where(lane == i, m[0:4], scr[32, 1:5, :])

    @pl.when(i == 7)
    def _():
        b_ref[...] = scr[...].astype(BF)


def pre(z, gain, proj, bias_w, gate_bias, mask_tile):
    wq, wk, wv, wg = [proj[:, 128 * n:128 * n + 128] for n in range(4)]

    def slots(w, i):
        return jnp.concatenate([w[:, 32 * ((s - i) % 4):32 * ((s - i) % 4) + 32] for s in range(4)], axis=1)

    wqk = jnp.stack([jnp.concatenate([slots(wq, i), slots(wk, i)], axis=1) for i in range(4)])
    wvg = jnp.concatenate([wv, wg], axis=1)
    bwt = jnp.pad(jnp.transpose(bias_w), ((0, 12), (0, 0)))
    row = lambda i: (i, 0, 0)
    return pl.pallas_call(
        pre_kernel,
        grid=(8,),
        in_specs=[
            pl.BlockSpec((1, 1024, 128), row),
            pl.BlockSpec((1, 128), lambda i: (0, 0)),
            pl.BlockSpec((1, 128, 256), lambda i: (lax.rem(i, 4), 0, 0)),
            pl.BlockSpec((128, 256), lambda i: (0, 0)),
            pl.BlockSpec((16, 128), lambda i: (0, 0)),
            pl.BlockSpec((1, 128), lambda i: (0, 0)),
            pl.BlockSpec((8, 128), lambda i: (0, 0)),
        ],
        out_specs=[
            pl.BlockSpec((1, 1024, 128), row),
            pl.BlockSpec((1, 1024, 128), row),
            pl.BlockSpec((1, 4, 48, 1024), lambda i: (i, 0, 0, 0)),
            pl.BlockSpec((1, 1024, 128), row),
            pl.BlockSpec((33, 8, 128), lambda i: (0, 0, 0)),
        ],
        out_shape=[
            jax.ShapeDtypeStruct((8, 1024, 128), BF),
            jax.ShapeDtypeStruct((8, 1024, 128), BF),
            jax.ShapeDtypeStruct((8, 4, 48, 1024), BF),
            jax.ShapeDtypeStruct((8, 1024, 128), BF),
            jax.ShapeDtypeStruct((33, 8, 128), BF),
        ],
        scratch_shapes=[pltpu.VMEM((33, 8, 128), F32)],
        compiler_params=pltpu.CompilerParams(vmem_limit_bytes=48 * 2**20),
        name="tri_pre",
    )(z, gain.reshape(1, 128), wqk, wvg, bwt, gate_bias.reshape(1, 128), mask_tile)


def post_kernel(o_ref, gate_ref, z_ref, w_ref, out_ref, scr, outgoing, landed, send_sem, recv_sem, out_sem):
    gx, gy = lax.axis_index("gx"), lax.axis_index("gy")
    me = gx * 8 + gy
    barrier = pltpu.get_barrier_semaphore()

    def greet(n, _):
        peer = lax.rem(me + n, 128)
        pl.semaphore_signal(barrier, inc=1, device_id=(peer // 8, lax.rem(peer, 8)), device_id_type=MESH_ID)
        return 0

    lax.fori_loop(1, 128, greet, 0)

    def tile(s, _):
        t = lax.rem(s + gx // 2, 8)
        at = pl.ds(pl.multiple_of(t * 128, 128), 128)
        parts = []
        for i in range(8):
            o = jnp.transpose(o_ref[i, :, at])
            parts.append((o * gate_ref[i, at].astype(F32)).astype(BF))
        y = jnp.dot(jnp.concatenate(parts, axis=0), w_ref[...], preferred_element_type=F32)
        for i in range(8):
            scr[pl.ds(i, 128, stride=8), :] = z_ref[i, at].astype(F32) + y[128 * i:128 * i + 128]
        outgoing[pl.ds(pl.multiple_of(t * 16, 16), 16)] = scr[...].astype(BF).reshape(16, 8, 8, 128)

        @pl.when(s == 0)
        def _():
            pl.semaphore_wait(barrier, 127)

        def push(n, _):
            dest = t * 16 + lax.rem(me + n, 16)

            @pl.when(dest != me)
            def _():
                pltpu.make_async_remote_copy(
                    src_ref=outgoing.at[dest], dst_ref=landed.at[:, me], send_sem=send_sem, recv_sem=recv_sem,
                    device_id=(dest // 8, lax.rem(dest, 8)), device_id_type=MESH_ID).start()

            return 0

        lax.fori_loop(0, 16, push, 0)
        return 0

    lax.fori_loop(0, 8, tile, 0)
    landed[:, me] = outgoing[me]
    everything = landed.at[:, 0:127]
    arrived = pltpu.make_async_remote_copy(
        src_ref=outgoing.at[0:127], dst_ref=everything, send_sem=send_sem, recv_sem=recv_sem,
        device_id=(lax.rem(gx + 1, 16), gy), device_id_type=MESH_ID)
    arrived.wait_recv()
    out = pltpu.make_async_copy(landed, out_ref, out_sem)
    out.start()
    arrived.wait_send()
    out.wait()


def post(o, gate, z, w, collective_id):
    vmem = pl.BlockSpec(memory_space=pltpu.VMEM)
    out = pl.pallas_call(
        post_kernel,
        in_specs=[vmem] * 4,
        out_specs=pl.BlockSpec(memory_space=pl.ANY),
        out_shape=jax.ShapeDtypeStruct((8, 128, 8, 128), BF),
        scratch_shapes=[
            pltpu.VMEM((1024, 128), F32),
            pltpu.VMEM((128, 8, 8, 128), BF),
            pltpu.VMEM((8, 128, 8, 128), BF),
            pltpu.SemaphoreType.DMA,
            pltpu.SemaphoreType.DMA,
            pltpu.SemaphoreType.DMA,
        ],
        compiler_params=pltpu.CompilerParams(collective_id=collective_id, has_side_effects=True, vmem_limit_bytes=40 * 2**20),
        name="tri_post",
    )(o, gate, z, w)
    return out.reshape(8, 1024, 128)


def trans_kernel(z_ref, gain_ref, w1_ref, b1_ref, w2_ref, out_ref):
    z = z_ref[0].astype(F32)
    a = layer_norm(z, gain_ref[...])
    hid = jax.nn.relu(jnp.dot(a, w1_ref[...], preferred_element_type=F32) + b1_ref[...]).astype(BF)
    out_ref[0] = (z + jnp.dot(hid, w2_ref[...], preferred_element_type=F32)).astype(BF)


def trans(z, gain, w1, b1, w2):
    row = lambda i: (i, 0, 0)
    whole = lambda i: (0, 0)
    return pl.pallas_call(
        trans_kernel,
        grid=(8,),
        in_specs=[
            pl.BlockSpec((1, 1024, 128), row),
            pl.BlockSpec((1, 128), whole),
            pl.BlockSpec((128, 512), whole),
            pl.BlockSpec((1, 512), whole),
            pl.BlockSpec((512, 128), whole),
        ],
        out_specs=pl.BlockSpec((1, 1024, 128), row),
        out_shape=jax.ShapeDtypeStruct((8, 1024, 128), BF),
        compiler_params=pltpu.CompilerParams(vmem_limit_bytes=48 * 2**20),
        name="tri_trans",
    )(z, gain.reshape(1, 128), w1, b1.reshape(1, 512), w2)


def exact_attention(q, k, vt, full):
    extra = full[32].reshape(128, 8, 128)
    mask = jnp.sum(extra[:, 0].reshape(8, 16, 128).astype(F32), axis=1).reshape(1024)
    maxima = jnp.transpose(extra[:, 1:5, :8], (1, 0, 2)).reshape(4, 1024).astype(F32)
    key_bias = (mask - 1.0) * big_negative
    b = full[:32].reshape(4, 8, 1024, 128)
    orders = jnp.array([[(h + i) % 4 for h in range(4)] for i in range(4)])

    def per_row(operands):
        i, q_row, k_row, vt_row = operands
        order = orders[lax.rem(i, 4)]
        qh = q_row.reshape(1024, 4, 32)[:, order]
        kh = k_row.reshape(1024, 4, 32)[:, order]

        def per_head(ops):
            qx, kx, vx, bx, mx = ops
            s = jnp.dot(qx, kx.T, preferred_element_type=F32)
            bias = jnp.swapaxes(bx, 0, 1).reshape(1024, 1024).astype(F32)
            s = (s + bias) * LN2 + mx[:, None] + key_bias
            w = jax.nn.softmax(s, axis=-1)
            return jnp.dot(vx[:32].astype(F32), w.T, preferred_element_type=F32)

        o = lax.map(per_head, (jnp.moveaxis(qh, 1, 0), jnp.moveaxis(kh, 1, 0), vt_row, b, maxima))
        return o.reshape(128, 1024)

    return lax.map(per_row, (jnp.arange(8), q, k, vt))


def phase(z, mask_tile, gain, proj, gate_bias, bias_w, out_w, collective_id):
    q, k, vt, gate, piece = pre(z, gain, proj, bias_w, gate_bias, mask_tile)
    full = gather(piece, collective_id)
    o, den = attention(q, k, vt, full)
    fine = jnp.all((den > 2.0 ** -60) & (den < 2.0 ** 100))
    o = lax.cond(fine, lambda: o, lambda: exact_attention(q, k, vt, full))
    return post(o, gate, z, out_w, 2 + collective_id)


def local(
    pair_in,
    residue_mask,
    norm_start,
    proj_start,
    gate_bias_start,
    bias_w_start,
    out_w_start,
    norm_end,
    proj_end,
    gate_bias_end,
    bias_w_end,
    out_w_end,
    norm_trans,
    trans_in,
    trans_bias,
    trans_out,
):
    device = lax.axis_index("gx") * 8 + lax.axis_index("gy")
    lane = lax.broadcasted_iota(jnp.int32, (8, 128), 1)
    row = lax.broadcasted_iota(jnp.int32, (8, 128), 0)
    spread = jnp.tile(residue_mask.astype(F32), 16).reshape(1, 128)
    mask_tile = jnp.where((lane // 8 == lax.rem(device, 16)) & (row == 0), spread, 0.0)
    z = phase(pair_in, mask_tile, norm_start, proj_start, gate_bias_start, bias_w_start, out_w_start, 0)
    z = phase(z, mask_tile, norm_end, proj_end, gate_bias_end, bias_w_end, out_w_end, 1)
    return trans(z, norm_trans, trans_in, trans_bias, trans_out)


def solution(mesh):
    rows = P(AX, None, None)
    placed = (rows, P(AX)) + (P(),) * 14

    def whole(*args):
        with jax.sharding.use_abstract_mesh(mesh.abstract_mesh):
            return jax.shard_map(local, mesh=mesh, in_specs=placed, out_specs=rows, check_vma=False)(*args)

    return whole
```

```python
import jax
import jax.numpy as jnp
from jax import lax
from jax.experimental import pallas as pl
from jax.experimental.pallas import tpu as pltpu
from jax.sharding import PartitionSpec as P

F32 = jnp.float32
BF = jnp.bfloat16
AX = ("gx", "gy")
HEADS = 4
HEAD_DIM = 32
LOG2E = 1.4426950408889634
LN2 = 0.6931471805599453
big_negative = 1000000000.0


def attn_setup(q_ref, qs, eye, slot):
    lane = lax.broadcasted_iota(jnp.int32, (16, 128), 1) // 32
    for s in range(4):
        slot[s] = jnp.where(lane == s, 1.0, 0.0).astype(BF)
    rowi = lax.broadcasted_iota(jnp.int32, (128, 128), 0)
    coli = lax.broadcasted_iota(jnp.int32, (128, 128), 1)
    eye[...] = jnp.where(rowi == coli, 1.0, 0.0).astype(BF)

    def stack(n, _):
        at = pl.ds(pl.multiple_of(n * 128, 128), 128)
        for g in range(2):
            rows = [q_ref[4 * g + r, at, :] for r in range(4)]
            for h in range(4):
                s = None
                for r in range(4):
                    t = rows[r] * jnp.concatenate([slot[(h + r) % 4]] * 8, axis=0)
                    s = t if s is None else s + t
                qs[2 * h + g, at, :] = s
        return 0

    lax.fori_loop(0, 8, stack, 0)


def attn_mask(extra, mask_ref):
    placed = jnp.sum(extra.astype(F32).reshape(8, 16, 8, 128), axis=1)
    for t in range(8):
        mask_ref[:, t * 128:(t + 1) * 128] = jnp.broadcast_to(placed[t, 0:1, :], (16, 128)).astype(BF)


def attn_split(it):
    group = it // 4
    return lax.rem(group, 2), lax.rem(group // 2, 4), group // 8, lax.rem(it, 4)


def attn_loop(first, last, k_ref, vt_ref, b_ref, o_ref, den_ref, qs, eye, slot, ps, mask_ref, sacc, oacc):
    def push_qb(it, odd):
        g, h, qp, kp = attn_split(it)
        at = [pl.ds(pl.multiple_of(qp * 512 + m * 256, 256), 256) for m in range(2)]
        for m in range(2):
            rhs = jnp.concatenate([qs[2 * h + g, at[m], :], b_ref[8 * h + 2 * kp + odd, at[m], :]], axis=1)
            pltpu.matmul_push_rhs(rhs, 0, m, transpose=True)

    def pop_scores(par, odd, r, n):
        for m in range(2):
            ps[2 * par + m][r, odd * 128:odd * 128 + 128, :] = jnp.exp2(pltpu.matmul_pop(sacc[m][n]).astype(BF))

    def push_p(par, r):
        for m in range(2):
            pltpu.matmul_push_rhs(ps[2 * par + m][r], 1, m)

    def pv(it, r):
        g, h, _, kp = attn_split(it)
        at = pl.ds(pl.multiple_of(kp * 256, 256), 256)
        lhs = vt_ref[4 * g + r, h, :, at] * jnp.concatenate([mask_ref[:, at]] * 3, axis=0)
        for m in range(2):
            pltpu.matmul_acc_lhs(oacc[m][r], lhs, 1)

    def result(it):
        g, h, qp, _ = attn_split(it)
        for r in range(4):
            for m in range(2):
                o = pltpu.matmul_pop(oacc[m][r])
                d = o[32:33, :]
                at = pl.ds(pl.multiple_of(qp * 512 + m * 256, 256), 256)
                o_ref[4 * g + r, pl.ds(pl.multiple_of(h * 32, 32), 32), at] = o[0:32, :] * (1.0 / d)
                den_ref[h, r, pl.ds(g, 1), at] = d

    def step(it, par):
        g, h, qp, kp = attn_split(it)
        before = lax.max(it - 1, 0)
        for odd in range(2):
            for r in range(4):
                at = pl.ds(pl.multiple_of((2 * kp + odd) * 128, 128), 128)
                keep = jnp.concatenate([slot[lax.rem(h + r, 4)]] * 8, axis=0)
                lhs = jnp.concatenate([k_ref[4 * g + r, at, :] * keep, eye[...]], axis=1)
                if r >= 2:
                    pop_scores(1 - par if odd == 0 else par, 1 - odd, r, r)
                for m in range(2):
                    pltpu.matmul_acc_lhs(sacc[m][r], lhs, 0 if r == 0 else None)
                if r == 0:
                    if odd == 0:
                        push_qb(it, 1)
                    else:
                        push_qb(lax.min(it + 1, 63), 0)
                    push_p(1 - par, 2 * odd)
            pv(before, 2 * odd)
            push_p(1 - par, 2 * odd + 1)
            pv(before, 2 * odd + 1)
            for r in range(2):
                pop_scores(par, odd, r, r)

    def body(pair, _):
        step(2 * pair, 0)

        @pl.when(lax.rem(pair, 2) == 0)
        def _():
            result(lax.max(2 * pair - 4, 0))

        step(2 * pair + 1, 1)
        return 0

    if first == 0:
        push_qb(0, 0)
    lax.fori_loop(first // 2, last // 2, body, 0)
    if last < 64:
        return
    par = (last - 1) % 2
    zero = jnp.zeros((128, 256), BF)
    for r in (2, 3):
        pop_scores(par, 1, r, r)
    for m in range(2):
        pltpu.matmul_acc_lhs(sacc[m][0], zero, 0)
        pltpu.matmul_pop(sacc[m][0])
    for r in range(4):
        push_p(par, r)
        pv(last - 1, r)
    result(last - 1)


def attn_kernel(q_ref, k_ref, vt_ref, b_ref, o_ref, den_ref, qs, eye, slot, ps0, ps1, ps2, ps3, mask_ref):
    ps = (ps0, ps1, ps2, ps3)
    attn_setup(q_ref, qs, eye, slot)
    attn_mask(b_ref[32], mask_ref)
    specs = []
    for m in range(2):
        specs += [pltpu.ACC(m)((128, 256), F32)] * 4 + [pltpu.ACC(m)((48, 256), F32)] * 4

    def run(*accs):
        sacc = [accs[8 * m:8 * m + 4] for m in range(2)]
        oacc = [accs[8 * m + 4:8 * m + 8] for m in range(2)]
        attn_loop(0, 64, k_ref, vt_ref, b_ref, o_ref, den_ref, qs, eye, slot, ps, mask_ref, sacc, oacc)

    pl.run_scoped(run, *specs)


def attention(q, k, vt, b):
    vmem = pl.BlockSpec(memory_space=pltpu.VMEM)
    return pl.pallas_call(
        attn_kernel,
        in_specs=[vmem] * 4,
        out_specs=[vmem] * 2,
        out_shape=[jax.ShapeDtypeStruct((8, 128, 1024), F32), jax.ShapeDtypeStruct((4, 4, 2, 1024), F32)],
        scratch_shapes=[
            pltpu.VMEM((8, 1024, 128), BF), pltpu.VMEM((128, 128), BF), pltpu.VMEM((4, 16, 128), BF),
            *[pltpu.VMEM((4, 256, 256), BF)] * 4, pltpu.VMEM((16, 1024), BF)],
        compiler_params=pltpu.CompilerParams(vmem_limit_bytes=40 * 2**20),
        name="tri_attn",
    )(q, k, vt, b)


MESH_ID = pl.DeviceIdType.MESH
ORDERS = ((0, 1, 2), (1, 2, 0), (2, 0, 1))


def gather_kernel(piece_ref, out_ref, full, send_sem, recv_sem, out_sem):
    gx, gy = lax.axis_index("gx"), lax.axis_index("gy")
    core = lax.rem(gx, 2)
    x = lax.rem(gx // 2, 4)
    y = gy // 2
    z = lax.rem(gy, 2) * 2 + gx // 8
    here = (x, y, z)

    def device(pos, c):
        px, py, pz = pos
        return ((lax.rem(pz, 2) * 4 + px) * 2 + c, py * 2 + pz // 2)

    def moved(dim, step):
        pos = list(here)
        pos[dim] = lax.rem(pos[dim] + step + 4, 4)
        return tuple(pos)

    def region(lo, hi, pos, done):
        px, py, pz = pos
        zl = slice(None) if 2 in done else lax.rem(pz, 2)
        zh = slice(None) if 2 in done else pz // 2
        xi = slice(None) if 0 in done else px
        yi = slice(None) if 1 in done else py
        return full.at[lo:hi, zl, xi, core, yi, zh]

    barrier = pltpu.get_barrier_semaphore()
    partner = device(here, 1 - core)
    peers = [device(moved(d, s), core) for d in range(3) for s in (1, 3)] + [partner]
    for peer in peers:
        pl.semaphore_signal(barrier, inc=1, device_id=peer, device_id_type=MESH_ID)
    full[:, lax.rem(z, 2), x, core, y, z // 2] = piece_ref[...]
    pl.semaphore_wait(barrier, 7)

    slots = [0]
    started = []

    def copy(src, dst, dev):
        n = slots[0]
        slots[0] += 1
        return pltpu.make_async_remote_copy(
            src_ref=src, dst_ref=dst, send_sem=send_sem.at[n], recv_sem=recv_sem.at[n],
            device_id=dev, device_id_type=MESH_ID)

    def send(lo, hi, pos, done, dev, first=False):
        spot = region(lo, hi, pos, done)
        c = copy(piece_ref.at[lo:hi] if first else spot, spot, dev)
        c.start()
        started.append(c)
        return c

    def arrival(n, lo, hi, pos, done):
        spot = region(lo, hi, pos, done)
        pltpu.make_async_remote_copy(
            src_ref=spot, dst_ref=spot, send_sem=send_sem.at[n], recv_sem=recv_sem.at[n],
            device_id=partner, device_id_type=MESH_ID).wait_recv()

    partner_waits = []

    def share(lo, hi, pos, done, first=False):
        n = slots[0]
        send(lo, hi, pos, done, partner, first)
        partner_waits.append((n, lo, hi, pos, done))

    for stage in range(3):
        tags = []
        for part in range(3):
            order = ORDERS[part]
            dim, done = order[stage], order[:stage]
            lo, hi = 11 * part, 11 * part + 11
            right, left = device(moved(dim, 1), core), device(moved(dim, 3), core)
            n = slots[0]
            send(lo, hi, here, done, right, stage == 0)
            send(lo, hi, here, done, left, stage == 0)
            tags.append((n, lo, hi, dim, done, right, left))
        if stage == 0:
            share(0, 33, here, (), True)
        halves = []
        for n, lo, hi, dim, done, right, left in tags:
            mid = lo + 6
            h = slots[0]
            arrival(n, lo, hi, moved(dim, 3), done)
            send(lo, mid, moved(dim, 3), done, right)
            arrival(n + 1, lo, hi, moved(dim, 1), done)
            send(mid, hi, moved(dim, 1), done, left)
            share(lo, hi, moved(dim, 3), done)
            share(lo, hi, moved(dim, 1), done)
            halves.append((h, lo, mid, hi, dim, done))
        for h, lo, mid, hi, dim, done in halves:
            arrival(h, lo, mid, moved(dim, 2), done)
            arrival(h + 1, mid, hi, moved(dim, 2), done)
            share(lo, hi, moved(dim, 2), done)

    def partner_region(lo, hi, pos, done):
        px, py, pz = pos
        zl = slice(None) if 2 in done else lax.rem(pz, 2)
        zh = slice(None) if 2 in done else pz // 2
        xi = slice(None) if 0 in done else px
        yi = slice(None) if 1 in done else py
        return full.at[lo:hi, zl, xi, 1 - core, yi, zh]

    for n, lo, hi, pos, done in partner_waits:
        spot = partner_region(lo, hi, pos, done)
        pltpu.make_async_remote_copy(
            src_ref=spot, dst_ref=spot, send_sem=send_sem.at[n], recv_sem=recv_sem.at[n],
            device_id=partner, device_id_type=MESH_ID).wait_recv()
    outs = [pltpu.make_async_copy(full.at[11 * p:11 * p + 11], out_ref.at[11 * p:11 * p + 11], out_sem.at[p]) for p in range(3)]
    for c in outs:
        c.start()
    for c in started:
        c.wait_send()
    for c in outs:
        c.wait()


def gather(piece, collective_id):
    shape = (33, 2, 4, 2, 4, 2, 8, 128)
    n = 64
    out = pl.pallas_call(
        gather_kernel,
        in_specs=[pl.BlockSpec(memory_space=pltpu.VMEM)],
        out_specs=pl.BlockSpec(memory_space=pl.ANY),
        out_shape=jax.ShapeDtypeStruct(shape, BF),
        scratch_shapes=[
            pltpu.VMEM(shape, BF),
            pltpu.SemaphoreType.DMA((n,)),
            pltpu.SemaphoreType.DMA((n,)),
            pltpu.SemaphoreType.DMA((3,)),
        ],
        compiler_params=pltpu.CompilerParams(collective_id=collective_id, has_side_effects=True, vmem_limit_bytes=24 * 2**20),
        name="tri_gather",
    )(piece)
    return out.reshape(33, 1024, 128)


def layer_norm(x, gain):
    mean = jnp.mean(x, axis=-1, keepdims=True)
    c = x - mean
    var = jnp.mean(c * c, axis=-1, keepdims=True)
    return (c * lax.rsqrt(var + 1e-05) * gain).astype(BF)


def pre_kernel(z_ref, gain_ref, wqk_ref, wvg_ref, bw_ref, gb_ref, mask_ref, q_ref, k_ref, vt_ref, gate_ref, b_ref, scr):
    i = pl.program_id(0)

    @pl.when(i == 0)
    def _():
        scr[32] = mask_ref[...]

    a = layer_norm(z_ref[0].astype(F32), gain_ref[...])
    qk = jnp.dot(a, wqk_ref[0], preferred_element_type=F32)
    q_ref[0] = (qk[:, :128] * (HEAD_DIM ** -0.5 * LOG2E)).astype(BF)
    k_ref[0] = qk[:, 128:].astype(BF)
    vg = jnp.dot(a, wvg_ref[...], preferred_element_type=F32)
    vt = jnp.transpose(vg[:, :128].astype(BF))
    tail = jnp.where(lax.broadcasted_iota(jnp.int32, (16, 1024), 0) == 0, 1.0, 0.0).astype(BF)
    for h in range(4):
        vt_ref[0, h, 0:32, :] = vt[32 * h:32 * h + 32, :]
        vt_ref[0, h, 32:48, :] = tail
    gate_ref[0] = jax.nn.sigmoid(vg[:, 128:] + gb_ref[...]).astype(BF)
    b = lax.dot_general(bw_ref[...], a, (((1,), (1,)), ((), ())), preferred_element_type=F32)
    b = b.astype(BF).astype(F32)
    m = jnp.max(b, axis=-1, keepdims=True)
    b = (b - m) * LOG2E
    for h in range(4):
        for kt in range(8):
            scr[8 * h + kt, pl.ds(i, 1), :] = b[h:h + 1, kt * 128:(kt + 1) * 128]
    lane = lax.broadcasted_iota(jnp.int32, (4, 128), 1)
    scr[32, 1:5, :] = jnp.where(lane == i, m[0:4], scr[32, 1:5, :])

    @pl.when(i == 7)
    def _():
        b_ref[...] = scr[...].astype(BF)


def pre(z, gain, proj, bias_w, gate_bias, mask_tile):
    wq, wk, wv, wg = [proj[:, 128 * n:128 * n + 128] for n in range(4)]

    def slots(w, i):
        return jnp.concatenate([w[:, 32 * ((s - i) % 4):32 * ((s - i) % 4) + 32] for s in range(4)], axis=1)

    wqk = jnp.stack([jnp.concatenate([slots(wq, i), slots(wk, i)], axis=1) for i in range(4)])
    wvg = jnp.concatenate([wv, wg], axis=1)
    bwt = jnp.pad(jnp.transpose(bias_w), ((0, 12), (0, 0)))
    row = lambda i: (i, 0, 0)
    return pl.pallas_call(
        pre_kernel,
        grid=(8,),
        in_specs=[
            pl.BlockSpec((1, 1024, 128), row),
            pl.BlockSpec((1, 128), lambda i: (0, 0)),
            pl.BlockSpec((1, 128, 256), lambda i: (lax.rem(i, 4), 0, 0)),
            pl.BlockSpec((128, 256), lambda i: (0, 0)),
            pl.BlockSpec((16, 128), lambda i: (0, 0)),
            pl.BlockSpec((1, 128), lambda i: (0, 0)),
            pl.BlockSpec((8, 128), lambda i: (0, 0)),
        ],
        out_specs=[
            pl.BlockSpec((1, 1024, 128), row),
            pl.BlockSpec((1, 1024, 128), row),
            pl.BlockSpec((1, 4, 48, 1024), lambda i: (i, 0, 0, 0)),
            pl.BlockSpec((1, 1024, 128), row),
            pl.BlockSpec((33, 8, 128), lambda i: (0, 0, 0)),
        ],
        out_shape=[
            jax.ShapeDtypeStruct((8, 1024, 128), BF),
            jax.ShapeDtypeStruct((8, 1024, 128), BF),
            jax.ShapeDtypeStruct((8, 4, 48, 1024), BF),
            jax.ShapeDtypeStruct((8, 1024, 128), BF),
            jax.ShapeDtypeStruct((33, 8, 128), BF),
        ],
        scratch_shapes=[pltpu.VMEM((33, 8, 128), F32)],
        compiler_params=pltpu.CompilerParams(vmem_limit_bytes=48 * 2**20),
        name="tri_pre",
    )(z, gain.reshape(1, 128), wqk, wvg, bwt, gate_bias.reshape(1, 128), mask_tile)


def post_kernel(o_ref, gate_ref, z_ref, w_ref, out_ref, scr, outgoing, landed, send_sem, recv_sem, out_sem):
    gx, gy = lax.axis_index("gx"), lax.axis_index("gy")
    me = gx * 8 + gy
    barrier = pltpu.get_barrier_semaphore()

    def greet(n, _):
        peer = lax.rem(me + n, 128)
        pl.semaphore_signal(barrier, inc=1, device_id=(peer // 8, lax.rem(peer, 8)), device_id_type=MESH_ID)
        return 0

    lax.fori_loop(1, 128, greet, 0)

    def tile(s, _):
        t = lax.rem(s + gx // 2, 8)
        at = pl.ds(pl.multiple_of(t * 128, 128), 128)
        parts = []
        for i in range(8):
            o = jnp.transpose(o_ref[i, :, at])
            parts.append((o * gate_ref[i, at].astype(F32)).astype(BF))
        y = jnp.dot(jnp.concatenate(parts, axis=0), w_ref[...], preferred_element_type=F32)
        for i in range(8):
            scr[pl.ds(i, 128, stride=8), :] = z_ref[i, at].astype(F32) + y[128 * i:128 * i + 128]
        outgoing[pl.ds(pl.multiple_of(t * 16, 16), 16)] = scr[...].astype(BF).reshape(16, 8, 8, 128)

        @pl.when(s == 0)
        def _():
            pl.semaphore_wait(barrier, 127)

        def push(n, _):
            dest = t * 16 + lax.rem(me + n, 16)

            @pl.when(dest != me)
            def _():
                pltpu.make_async_remote_copy(
                    src_ref=outgoing.at[dest], dst_ref=landed.at[:, me], send_sem=send_sem, recv_sem=recv_sem,
                    device_id=(dest // 8, lax.rem(dest, 8)), device_id_type=MESH_ID).start()

            return 0

        lax.fori_loop(0, 16, push, 0)
        return 0

    lax.fori_loop(0, 8, tile, 0)
    landed[:, me] = outgoing[me]
    everything = landed.at[:, 0:127]
    arrived = pltpu.make_async_remote_copy(
        src_ref=outgoing.at[0:127], dst_ref=everything, send_sem=send_sem, recv_sem=recv_sem,
        device_id=(lax.rem(gx + 1, 16), gy), device_id_type=MESH_ID)
    arrived.wait_recv()
    out = pltpu.make_async_copy(landed, out_ref, out_sem)
    out.start()
    arrived.wait_send()
    out.wait()


def post(o, gate, z, w, collective_id):
    vmem = pl.BlockSpec(memory_space=pltpu.VMEM)
    out = pl.pallas_call(
        post_kernel,
        in_specs=[vmem] * 4,
        out_specs=pl.BlockSpec(memory_space=pl.ANY),
        out_shape=jax.ShapeDtypeStruct((8, 128, 8, 128), BF),
        scratch_shapes=[
            pltpu.VMEM((1024, 128), F32),
            pltpu.VMEM((128, 8, 8, 128), BF),
            pltpu.VMEM((8, 128, 8, 128), BF),
            pltpu.SemaphoreType.DMA,
            pltpu.SemaphoreType.DMA,
            pltpu.SemaphoreType.DMA,
        ],
        compiler_params=pltpu.CompilerParams(collective_id=collective_id, has_side_effects=True, vmem_limit_bytes=40 * 2**20),
        name="tri_post",
    )(o, gate, z, w)
    return out.reshape(8, 1024, 128)


def trans_kernel(z_ref, gain_ref, w1_ref, b1_ref, w2_ref, out_ref):
    z = z_ref[0].astype(F32)
    a = layer_norm(z, gain_ref[...])
    hid = jax.nn.relu(jnp.dot(a, w1_ref[...], preferred_element_type=F32) + b1_ref[...]).astype(BF)
    out_ref[0] = (z + jnp.dot(hid, w2_ref[...], preferred_element_type=F32)).astype(BF)


def trans(z, gain, w1, b1, w2):
    row = lambda i: (i, 0, 0)
    whole = lambda i: (0, 0)
    return pl.pallas_call(
        trans_kernel,
        grid=(8,),
        in_specs=[
            pl.BlockSpec((1, 1024, 128), row),
            pl.BlockSpec((1, 128), whole),
            pl.BlockSpec((128, 512), whole),
            pl.BlockSpec((1, 512), whole),
            pl.BlockSpec((512, 128), whole),
        ],
        out_specs=pl.BlockSpec((1, 1024, 128), row),
        out_shape=jax.ShapeDtypeStruct((8, 1024, 128), BF),
        compiler_params=pltpu.CompilerParams(vmem_limit_bytes=48 * 2**20),
        name="tri_trans",
    )(z, gain.reshape(1, 128), w1, b1.reshape(1, 512), w2)


def exact_attention(q, k, vt, full):
    extra = full[32].reshape(128, 8, 128)
    mask = jnp.sum(extra[:, 0].reshape(8, 16, 128).astype(F32), axis=1).reshape(1024)
    maxima = jnp.transpose(extra[:, 1:5, :8], (1, 0, 2)).reshape(4, 1024).astype(F32)
    key_bias = (mask - 1.0) * big_negative
    b = full[:32].reshape(4, 8, 1024, 128)
    orders = jnp.array([[(h + i) % 4 for h in range(4)] for i in range(4)])

    def per_row(operands):
        i, q_row, k_row, vt_row = operands
        order = orders[lax.rem(i, 4)]
        qh = q_row.reshape(1024, 4, 32)[:, order]
        kh = k_row.reshape(1024, 4, 32)[:, order]

        def per_head(ops):
            qx, kx, vx, bx, mx = ops
            s = jnp.dot(qx, kx.T, preferred_element_type=F32)
            bias = jnp.swapaxes(bx, 0, 1).reshape(1024, 1024).astype(F32)
            s = (s + bias) * LN2 + mx[:, None] + key_bias
            w = jax.nn.softmax(s, axis=-1)
            return jnp.dot(vx[:32].astype(F32), w.T, preferred_element_type=F32)

        o = lax.map(per_head, (jnp.moveaxis(qh, 1, 0), jnp.moveaxis(kh, 1, 0), vt_row, b, maxima))
        return o.reshape(128, 1024)

    return lax.map(per_row, (jnp.arange(8), q, k, vt))


def phase(z, mask_tile, gain, proj, gate_bias, bias_w, out_w, collective_id):
    q, k, vt, gate, piece = pre(z, gain, proj, bias_w, gate_bias, mask_tile)
    full = gather(piece, collective_id)
    o, den = attention(q, k, vt, full)
    fine = jnp.all((den > 2.0 ** -60) & (den < 2.0 ** 100))
    o = lax.cond(fine, lambda: o, lambda: exact_attention(q, k, vt, full))
    return post(o, gate, z, out_w, 2 + collective_id)


def local(
    pair_in,
    residue_mask,
    norm_start,
    proj_start,
    gate_bias_start,
    bias_w_start,
    out_w_start,
    norm_end,
    proj_end,
    gate_bias_end,
    bias_w_end,
    out_w_end,
    norm_trans,
    trans_in,
    trans_bias,
    trans_out,
):
    device = lax.axis_index("gx") * 8 + lax.axis_index("gy")
    lane = lax.broadcasted_iota(jnp.int32, (8, 128), 1)
    row = lax.broadcasted_iota(jnp.int32, (8, 128), 0)
    spread = jnp.tile(residue_mask.astype(F32), 16).reshape(1, 128)
    mask_tile = jnp.where((lane // 8 == lax.rem(device, 16)) & (row == 0), spread, 0.0)
    z = phase(pair_in, mask_tile, norm_start, proj_start, gate_bias_start, bias_w_start, out_w_start, 0)
    z = phase(z, mask_tile, norm_end, proj_end, gate_bias_end, bias_w_end, out_w_end, 1)
    return trans(z, norm_trans, trans_in, trans_bias, trans_out)


def solution(mesh):
    rows = P(AX, None, None)
    placed = (rows, P(AX)) + (P(),) * 14

    def whole(*args):
        with jax.sharding.use_abstract_mesh(mesh.abstract_mesh):
            return jax.shard_map(local, mesh=mesh, in_specs=placed, out_specs=rows, check_vma=False)(*args)

    return whole
```

```python
import jax
import jax.numpy as jnp
from jax import lax
from jax.experimental import pallas as pl
from jax.experimental.pallas import tpu as pltpu
from jax.sharding import PartitionSpec as P

F32 = jnp.float32
BF = jnp.bfloat16
AX = ("gx", "gy")
HEADS = 4
HEAD_DIM = 32
LOG2E = 1.4426950408889634
LN2 = 0.6931471805599453
big_negative = 1000000000.0


MESH_ID = pl.DeviceIdType.MESH
ORDERS = ((0, 1, 2), (1, 2, 0), (2, 0, 1))
EXTRA = 26
PLANES = 36
EARLY = 43


def plane(h, t):
    if isinstance(t, int):
        return 12 * (t // 3) + 3 * h + t % 3
    return 12 * (t // 3) + 3 * h + lax.rem(t, 3)


class Torus:
    def __init__(self, piece_ref, full, send_sem, recv_sem):
        gx, gy = lax.axis_index("gx"), lax.axis_index("gy")
        self.core = lax.rem(gx, 2)
        self.here = (lax.rem(gx // 2, 4), gy // 2, lax.rem(gy, 2) * 2 + gx // 8)
        self.piece, self.full, self.send_sem, self.recv_sem = piece_ref, full, send_sem, recv_sem
        self.partner = self.device(self.here, 1 - self.core)
        self.sent = []

    def device(self, pos, c):
        px, py, pz = pos
        return ((lax.rem(pz, 2) * 4 + px) * 2 + c, py * 2 + pz // 2)

    def moved(self, dim, step):
        pos = list(self.here)
        pos[dim] = lax.rem(pos[dim] + step, 4)
        return tuple(pos)

    def region(self, lo, n, pos, done, other=False):
        px, py, pz = pos
        zl = slice(None) if 2 in done else lax.rem(pz, 2)
        zh = slice(None) if 2 in done else pz // 2
        xi = slice(None) if 0 in done else px
        yi = slice(None) if 1 in done else py
        return self.full.at[pl.ds(lo, n), zl, xi, 1 - self.core if other else self.core, yi, zh]

    def send(self, slot, lo, n, pos, done, dev, first=False):
        spot = self.region(lo, n, pos, done)
        pltpu.make_async_remote_copy(
            src_ref=self.piece.at[pl.ds(lo, n)] if first else spot, dst_ref=spot, send_sem=self.send_sem.at[slot],
            recv_sem=self.recv_sem.at[slot], device_id=dev, device_id_type=MESH_ID).start()

    def wait(self, slot, lo, n, pos, done, other=False, sent=False):
        spot = self.region(lo, n, pos, done, other)
        c = pltpu.make_async_remote_copy(
            src_ref=spot, dst_ref=spot, send_sem=self.send_sem.at[slot], recv_sem=self.recv_sem.at[slot],
            device_id=self.partner, device_id_type=MESH_ID)
        c.wait_send() if sent else c.wait_recv()

    def barrier(self):
        barrier = pltpu.get_barrier_semaphore()
        peers = [self.device(self.moved(d, s), self.core) for d in range(3) for s in (1, 3)] + [self.partner]
        for peer in peers:
            pl.semaphore_signal(barrier, inc=1, device_id=peer, device_id_type=MESH_ID)
        px, py, pz = self.here
        self.full[:, lax.rem(pz, 2), px, self.core, py, pz // 2] = self.piece[...]
        pl.semaphore_wait(barrier, 7)

    def outward(self, base, o, stage, lo, n):
        dim, done = ORDERS[o][stage], ORDERS[o][:stage]
        self.send(base, lo, n, self.here, done, self.device(self.moved(dim, 1), self.core), stage == 0)
        self.send(base + 1, lo, n, self.here, done, self.device(self.moved(dim, 3), self.core), stage == 0)

    def onward(self, base, o, stage, lo, n, n1):
        dim, done = ORDERS[o][stage], ORDERS[o][:stage]
        left, right = self.moved(dim, 3), self.moved(dim, 1)
        self.wait(base, lo, n, left, done)
        self.send(base + 2, lo, n1, left, done, self.device(right, self.core))
        self.wait(base + 1, lo, n, right, done)
        self.send(base + 3, lo + n1, n - n1, right, done, self.device(left, self.core))
        self.send(base + 4, lo, n, left, done, self.partner)
        self.send(base + 5, lo, n, right, done, self.partner)

    def closing(self, base, o, stage, lo, n, n1):
        dim, done = ORDERS[o][stage], ORDERS[o][:stage]
        far = self.moved(dim, 2)
        self.wait(base + 2, lo, n1, far, done)
        self.wait(base + 3, lo + n1, n - n1, far, done)
        self.send(base + 6, lo, n, far, done, self.partner)

    def shared(self, base, o, stage, lo, n):
        dim, done = ORDERS[o][stage], ORDERS[o][:stage]
        for k, step in ((4, 3), (5, 1), (6, 2)):
            self.wait(base + k, lo, n, self.moved(dim, step), done, True)

    def settled(self, base, o, stage, lo, n, n1):
        done = ORDERS[o][:stage]
        for k, size in ((0, n), (1, n), (2, n1), (3, n - n1), (4, n), (5, n), (6, n)):
            self.wait(base + k, lo, size, self.here, done, False, True)

    def early(self):
        for stage in range(2):
            bases = [21 * stage + 7 * o for o in range(3)]
            for o in range(3):
                self.outward(bases[o], o, stage, 12 * o, 12)
            if stage == 0:
                self.send(42, 0, PLANES, self.here, (), self.partner, True)
            for o in range(3):
                self.onward(bases[o], o, stage, 12 * o, 12, 6)
            for o in range(3):
                self.closing(bases[o], o, stage, 12 * o, 12, 6)

    def sizes(self, first):
        return ((3, 2), (3, 1), (3, 1) if first else (2, 1))

    def late(self, action, h, first=False):
        for o, (n, n1) in enumerate(self.sizes(first)):
            base, lo = EARLY + 21 * h + 7 * o, 12 * o + 3 * h
            if action in ("outward", "shared"):
                getattr(self, action)(base, o, 2, lo, n)
            else:
                getattr(self, action)(base, o, 2, lo, n, n1)

    def early_shared(self):
        self.wait(42, 0, PLANES, self.here, (), True)
        for stage in range(2):
            for o in range(3):
                self.shared(21 * stage + 7 * o, o, stage, 12 * o, 12)

    def finish(self):
        self.wait(42, 0, PLANES, self.here, (), False, True)
        for stage in range(2):
            for o in range(3):
                self.settled(21 * stage + 7 * o, o, stage, 12 * o, 12, 6)
        for h in range(4):
            self.late("settled", h, h == 0)


def attn_setup(q_ref, qs, eye, slot):
    lane = lax.broadcasted_iota(jnp.int32, (16, 128), 1) // 32
    for s in range(4):
        slot[s] = jnp.where(lane == s, 1.0, 0.0).astype(BF)
    rowi = lax.broadcasted_iota(jnp.int32, (128, 128), 0)
    coli = lax.broadcasted_iota(jnp.int32, (128, 128), 1)
    eye[...] = jnp.where(rowi == coli, 1.0, 0.0).astype(BF)

    def stack(n, _):
        at = pl.ds(pl.multiple_of(n * 128, 128), 128)
        for g in range(2):
            rows = [q_ref[4 * g + r, at, :] for r in range(4)]
            for h in range(4):
                s = None
                for r in range(4):
                    t = rows[r] * jnp.concatenate([slot[(h + r) % 4]] * 8, axis=0)
                    s = t if s is None else s + t
                qs[2 * h + g, at, :] = s
        return 0

    lax.fori_loop(0, 8, stack, 0)


def attn_mask(extra, mask_ref):
    placed = jnp.sum(extra.astype(F32).reshape(8, 16, 8, 128), axis=1)
    for t in range(8):
        mask_ref[:, t * 128:(t + 1) * 128] = jnp.broadcast_to(placed[t, 0:1, :], (16, 128)).astype(BF)


def attn_split(it):
    group = it // 4
    return lax.rem(group, 2), lax.rem(group // 2, 4), group // 8, lax.rem(it, 4)


def attn_loop(first, last, comm, k_ref, vt_ref, b_ref, o_ref, den_ref, qs, eye, slot, ps, mask_ref, sacc, oacc):
    def push_qb(it, odd):
        g, h, qp, kp = attn_split(it)
        at = [pl.ds(pl.multiple_of(qp * 512 + m * 256, 256), 256) for m in range(2)]
        for m in range(2):
            rhs = jnp.concatenate([qs[2 * h + g, at[m], :], b_ref[plane(h, 2 * kp + odd), at[m], :]], axis=1)
            pltpu.matmul_push_rhs(rhs, 0, m, transpose=True)

    def pop_scores(par, odd, r, n):
        for m in range(2):
            ps[2 * par + m][r, odd * 128:odd * 128 + 128, :] = jnp.exp2(pltpu.matmul_pop(sacc[m][n]).astype(BF))

    def push_p(par, r):
        for m in range(2):
            pltpu.matmul_push_rhs(ps[2 * par + m][r], 1, m)

    def pv(it, r):
        g, h, _, kp = attn_split(it)
        at = pl.ds(pl.multiple_of(kp * 256, 256), 256)
        lhs = vt_ref[4 * g + r, h, :, at] * jnp.concatenate([mask_ref[:, at]] * 3, axis=0)
        for m in range(2):
            pltpu.matmul_acc_lhs(oacc[m][r], lhs, 1)

    def result(it):
        g, h, qp, _ = attn_split(it)
        for r in range(4):
            for m in range(2):
                o = pltpu.matmul_pop(oacc[m][r])
                d = o[32:33, :]
                at = pl.ds(pl.multiple_of(qp * 512 + m * 256, 256), 256)
                o_ref[4 * g + r, pl.ds(pl.multiple_of(h * 32, 32), 32), at] = o[0:32, :] * (1.0 / d)
                den_ref[h, r, pl.ds(g, 1), at] = d

    def step(it, par):
        g, h, qp, kp = attn_split(it)
        before = lax.max(it - 1, 0)
        for odd in range(2):
            for r in range(4):
                at = pl.ds(pl.multiple_of((2 * kp + odd) * 128, 128), 128)
                keep = jnp.concatenate([slot[lax.rem(h + r, 4)]] * 8, axis=0)
                lhs = jnp.concatenate([k_ref[4 * g + r, at, :] * keep, eye[...]], axis=1)
                if r >= 2:
                    pop_scores(1 - par if odd == 0 else par, 1 - odd, r, r)
                for m in range(2):
                    pltpu.matmul_acc_lhs(sacc[m][r], lhs, 0 if r == 0 else None)
                if r == 0:
                    if odd == 0:
                        push_qb(it, 1)
                    else:
                        push_qb(lax.min(it + 1, 63), 0)
                    push_p(1 - par, 2 * odd)
            pv(before, 2 * odd)
            push_p(1 - par, 2 * odd + 1)
            pv(before, 2 * odd + 1)
            for r in range(2):
                pop_scores(par, odd, r, r)

    def body(pair, _):
        step(2 * pair, 0)
        comm(pair + 1)

        @pl.when(lax.rem(pair, 2) == 0)
        def _():
            result(lax.max(2 * pair - 4, 0))

        step(2 * pair + 1, 1)
        return 0

    if first == 0:
        push_qb(0, 0)
    lax.fori_loop(first // 2, last // 2, body, 0)
    if last < 64:
        return
    par = (last - 1) % 2
    zero = jnp.zeros((128, 256), BF)
    for r in (2, 3):
        pop_scores(par, 1, r, r)
    for m in range(2):
        pltpu.matmul_acc_lhs(sacc[m][0], zero, 0)
        pltpu.matmul_pop(sacc[m][0])
    for r in range(4):
        push_p(par, r)
        pv(last - 1, r)
    result(last - 1)


def attn_kernel(piece_ref, q_hbm, k_hbm, vt_hbm, o_ref, den_ref, full_hbm, full, q_ref, k_ref, vt_ref, qs, eye, slot, ps0, ps1, ps2, ps3, mask_ref, send_sem, recv_sem, load_sem, out_sem):
    ps = (ps0, ps1, ps2, ps3)
    loads = [pltpu.make_async_copy(a, b, load_sem.at[n]) for n, (a, b) in enumerate(((q_hbm, q_ref), (k_hbm, k_ref), (vt_hbm, vt_ref)))]
    for c in loads:
        c.start()
    torus = Torus(piece_ref, full, send_sem, recv_sem)
    torus.barrier()
    torus.early()
    torus.late("outward", 0, True)
    torus.late("outward", 1)
    for c in loads:
        c.wait()
    attn_setup(q_ref, qs, eye, slot)
    torus.late("onward", 0, True)
    torus.late("outward", 2)
    torus.late("onward", 1)
    torus.late("outward", 3)
    torus.late("closing", 0, True)
    torus.early_shared()
    torus.late("shared", 0, True)
    b_ref = full.reshape(PLANES, 1024, 128)
    attn_mask(b_ref[EXTRA], mask_ref)

    out = pltpu.make_async_copy(full, full_hbm, out_sem)

    def comm(pair):
        @pl.when(pair == 16)
        def _():
            out.start()

        @pl.when(pair < 13)
        def _():
            @pl.when((pair == 1) | (pair == 3))
            def _():
                torus.late("onward", (pair + 3) // 2)

            @pl.when(lax.rem(pair, 4) == 2)
            def _():
                torus.late("closing", (pair + 2) // 4)

            @pl.when((pair > 0) & (lax.rem(pair, 4) == 0))
            def _():
                torus.late("shared", pair // 4)

    specs = []
    for m in range(2):
        specs += [pltpu.ACC(m)((128, 256), F32)] * 4 + [pltpu.ACC(m)((48, 256), F32)] * 4

    def run(*accs):
        sacc = [accs[8 * m:8 * m + 4] for m in range(2)]
        oacc = [accs[8 * m + 4:8 * m + 8] for m in range(2)]
        attn_loop(0, 64, comm, k_ref, vt_ref, b_ref, o_ref, den_ref, qs, eye, slot, ps, mask_ref, sacc, oacc)

    pl.run_scoped(run, *specs)
    torus.finish()
    out.wait()


def attention(piece, q, k, vt, collective_id):
    vmem = pl.BlockSpec(memory_space=pltpu.VMEM)
    hbm = pl.BlockSpec(memory_space=pl.ANY)
    shape = (PLANES, 2, 4, 2, 4, 2, 8, 128)
    o, den, full = pl.pallas_call(
        attn_kernel,
        in_specs=[vmem, hbm, hbm, hbm],
        out_specs=[vmem, vmem, hbm],
        out_shape=[
            jax.ShapeDtypeStruct((8, 128, 1024), F32),
            jax.ShapeDtypeStruct((4, 4, 2, 1024), F32),
            jax.ShapeDtypeStruct(shape, BF),
        ],
        scratch_shapes=[
            pltpu.VMEM(shape, BF),
            pltpu.VMEM((8, 1024, 128), BF),
            pltpu.VMEM((8, 1024, 128), BF),
            pltpu.VMEM((8, 4, 48, 1024), BF),
            pltpu.VMEM((8, 1024, 128), BF),
            pltpu.VMEM((128, 128), BF),
            pltpu.VMEM((4, 16, 128), BF),
            *[pltpu.VMEM((4, 256, 256), BF)] * 4,
            pltpu.VMEM((16, 1024), BF),
            pltpu.SemaphoreType.DMA((EARLY + 84,)),
            pltpu.SemaphoreType.DMA((EARLY + 84,)),
            pltpu.SemaphoreType.DMA((3,)),
            pltpu.SemaphoreType.DMA,
        ],
        compiler_params=pltpu.CompilerParams(collective_id=collective_id, has_side_effects=True, vmem_limit_bytes=44 * 2**20),
        name="tri_attn",
    )(piece, q, k, vt)
    return o, den, full.reshape(PLANES, 1024, 128)


def layer_norm(x, gain):
    mean = jnp.mean(x, axis=-1, keepdims=True)
    c = x - mean
    var = jnp.mean(c * c, axis=-1, keepdims=True)
    return (c * lax.rsqrt(var + 1e-05) * gain).astype(BF)


def pre_kernel(z_ref, gain_ref, wqk_ref, wvg_ref, bw_ref, gb_ref, mask_ref, q_ref, k_ref, vt_ref, gate_ref, b_ref, scr):
    i = pl.program_id(0)

    @pl.when(i == 0)
    def _():
        scr[...] = jnp.zeros((PLANES, 8, 128), F32)
        scr[EXTRA] = mask_ref[...]

    a = layer_norm(z_ref[0].astype(F32), gain_ref[...])
    qk = jnp.dot(a, wqk_ref[0], preferred_element_type=F32)
    q_ref[0] = (qk[:, :128] * (HEAD_DIM ** -0.5 * LOG2E)).astype(BF)
    k_ref[0] = qk[:, 128:].astype(BF)
    vg = jnp.dot(a, wvg_ref[...], preferred_element_type=F32)
    vt = jnp.transpose(vg[:, :128].astype(BF))
    tail = jnp.where(lax.broadcasted_iota(jnp.int32, (16, 1024), 0) == 0, 1.0, 0.0).astype(BF)
    for h in range(4):
        vt_ref[0, h, 0:32, :] = vt[32 * h:32 * h + 32, :]
        vt_ref[0, h, 32:48, :] = tail
    gate_ref[0] = jax.nn.sigmoid(vg[:, 128:] + gb_ref[...]).astype(BF)
    b = lax.dot_general(bw_ref[...], a, (((1,), (1,)), ((), ())), preferred_element_type=F32)
    b = b.astype(BF).astype(F32)
    m = jnp.max(b, axis=-1, keepdims=True)
    b = (b - m) * LOG2E
    for h in range(4):
        for kt in range(8):
            scr[plane(h, kt), pl.ds(i, 1), :] = b[h:h + 1, kt * 128:(kt + 1) * 128]
    lane = lax.broadcasted_iota(jnp.int32, (4, 128), 1)
    scr[EXTRA, 1:5, :] = jnp.where(lane == i, m[0:4], scr[EXTRA, 1:5, :])

    @pl.when(i == 7)
    def _():
        b_ref[...] = scr[...].astype(BF)


def pre(z, gain, proj, bias_w, gate_bias, mask_tile):
    wq, wk, wv, wg = [proj[:, 128 * n:128 * n + 128] for n in range(4)]

    def slots(w, i):
        return jnp.concatenate([w[:, 32 * ((s - i) % 4):32 * ((s - i) % 4) + 32] for s in range(4)], axis=1)

    wqk = jnp.stack([jnp.concatenate([slots(wq, i), slots(wk, i)], axis=1) for i in range(4)])
    wvg = jnp.concatenate([wv, wg], axis=1)
    bwt = jnp.pad(jnp.transpose(bias_w), ((0, 12), (0, 0)))
    row = lambda i: (i, 0, 0)
    return pl.pallas_call(
        pre_kernel,
        grid=(8,),
        in_specs=[
            pl.BlockSpec((1, 1024, 128), row),
            pl.BlockSpec((1, 128), lambda i: (0, 0)),
            pl.BlockSpec((1, 128, 256), lambda i: (lax.rem(i, 4), 0, 0)),
            pl.BlockSpec((128, 256), lambda i: (0, 0)),
            pl.BlockSpec((16, 128), lambda i: (0, 0)),
            pl.BlockSpec((1, 128), lambda i: (0, 0)),
            pl.BlockSpec((8, 128), lambda i: (0, 0)),
        ],
        out_specs=[
            pl.BlockSpec((1, 1024, 128), row),
            pl.BlockSpec((1, 1024, 128), row),
            pl.BlockSpec((1, 4, 48, 1024), lambda i: (i, 0, 0, 0)),
            pl.BlockSpec((1, 1024, 128), row),
            pl.BlockSpec((PLANES, 8, 128), lambda i: (0, 0, 0)),
        ],
        out_shape=[
            jax.ShapeDtypeStruct((8, 1024, 128), BF),
            jax.ShapeDtypeStruct((8, 1024, 128), BF),
            jax.ShapeDtypeStruct((8, 4, 48, 1024), BF),
            jax.ShapeDtypeStruct((8, 1024, 128), BF),
            jax.ShapeDtypeStruct((PLANES, 8, 128), BF),
        ],
        scratch_shapes=[pltpu.VMEM((PLANES, 8, 128), F32)],
        compiler_params=pltpu.CompilerParams(vmem_limit_bytes=48 * 2**20),
        name="tri_pre",
    )(z, gain.reshape(1, 128), wqk, wvg, bwt, gate_bias.reshape(1, 128), mask_tile)


def post_kernel(o_ref, gate_ref, z_ref, w_ref, out_ref, scr, outgoing, landed, send_sem, recv_sem, out_sem):
    gx, gy = lax.axis_index("gx"), lax.axis_index("gy")
    me = gx * 8 + gy
    barrier = pltpu.get_barrier_semaphore()

    def greet(n, _):
        peer = lax.rem(me + n, 128)
        pl.semaphore_signal(barrier, inc=1, device_id=(peer // 8, lax.rem(peer, 8)), device_id_type=MESH_ID)
        return 0

    lax.fori_loop(1, 128, greet, 0)

    def tile(s, _):
        t = lax.rem(s + gx // 2, 8)
        at = pl.ds(pl.multiple_of(t * 128, 128), 128)
        parts = []
        for i in range(8):
            o = jnp.transpose(o_ref[i, :, at])
            parts.append((o * gate_ref[i, at].astype(F32)).astype(BF))
        y = jnp.dot(jnp.concatenate(parts, axis=0), w_ref[...], preferred_element_type=F32)
        for i in range(8):
            scr[pl.ds(i, 128, stride=8), :] = z_ref[i, at].astype(F32) + y[128 * i:128 * i + 128]
        outgoing[pl.ds(pl.multiple_of(t * 16, 16), 16)] = scr[...].astype(BF).reshape(16, 8, 8, 128)

        @pl.when(s == 0)
        def _():
            pl.semaphore_wait(barrier, 127)

        def push(n, _):
            dest = t * 16 + lax.rem(me + n, 16)

            @pl.when(dest != me)
            def _():
                pltpu.make_async_remote_copy(
                    src_ref=outgoing.at[dest], dst_ref=landed.at[:, me], send_sem=send_sem, recv_sem=recv_sem,
                    device_id=(dest // 8, lax.rem(dest, 8)), device_id_type=MESH_ID).start()

            return 0

        lax.fori_loop(0, 16, push, 0)
        return 0

    lax.fori_loop(0, 8, tile, 0)
    landed[:, me] = outgoing[me]
    everything = landed.at[:, 0:127]
    arrived = pltpu.make_async_remote_copy(
        src_ref=outgoing.at[0:127], dst_ref=everything, send_sem=send_sem, recv_sem=recv_sem,
        device_id=(lax.rem(gx + 1, 16), gy), device_id_type=MESH_ID)
    arrived.wait_recv()
    out = pltpu.make_async_copy(landed, out_ref, out_sem)
    out.start()
    arrived.wait_send()
    out.wait()


def post(o, gate, z, w, collective_id):
    vmem = pl.BlockSpec(memory_space=pltpu.VMEM)
    out = pl.pallas_call(
        post_kernel,
        in_specs=[vmem] * 4,
        out_specs=pl.BlockSpec(memory_space=pl.ANY),
        out_shape=jax.ShapeDtypeStruct((8, 128, 8, 128), BF),
        scratch_shapes=[
            pltpu.VMEM((1024, 128), F32),
            pltpu.VMEM((128, 8, 8, 128), BF),
            pltpu.VMEM((8, 128, 8, 128), BF),
            pltpu.SemaphoreType.DMA,
            pltpu.SemaphoreType.DMA,
            pltpu.SemaphoreType.DMA,
        ],
        compiler_params=pltpu.CompilerParams(collective_id=collective_id, has_side_effects=True, vmem_limit_bytes=40 * 2**20),
        name="tri_post",
    )(o, gate, z, w)
    return out.reshape(8, 1024, 128)


def trans_kernel(z_ref, gain_ref, w1_ref, b1_ref, w2_ref, out_ref):
    z = z_ref[0].astype(F32)
    a = layer_norm(z, gain_ref[...])
    hid = jax.nn.relu(jnp.dot(a, w1_ref[...], preferred_element_type=F32) + b1_ref[...]).astype(BF)
    out_ref[0] = (z + jnp.dot(hid, w2_ref[...], preferred_element_type=F32)).astype(BF)


def trans(z, gain, w1, b1, w2):
    row = lambda i: (i, 0, 0)
    whole = lambda i: (0, 0)
    return pl.pallas_call(
        trans_kernel,
        grid=(8,),
        in_specs=[
            pl.BlockSpec((1, 1024, 128), row),
            pl.BlockSpec((1, 128), whole),
            pl.BlockSpec((128, 512), whole),
            pl.BlockSpec((1, 512), whole),
            pl.BlockSpec((512, 128), whole),
        ],
        out_specs=pl.BlockSpec((1, 1024, 128), row),
        out_shape=jax.ShapeDtypeStruct((8, 1024, 128), BF),
        compiler_params=pltpu.CompilerParams(vmem_limit_bytes=48 * 2**20),
        name="tri_trans",
    )(z, gain.reshape(1, 128), w1, b1.reshape(1, 512), w2)


def exact_attention(q, k, vt, full):
    extra = full[EXTRA].reshape(128, 8, 128)
    mask = jnp.sum(extra[:, 0].reshape(8, 16, 128).astype(F32), axis=1).reshape(1024)
    maxima = jnp.transpose(extra[:, 1:5, :8], (1, 0, 2)).reshape(4, 1024).astype(F32)
    key_bias = (mask - 1.0) * big_negative
    b = jnp.stack([jnp.stack([full[12 * (t // 3) + 3 * h + t % 3] for t in range(8)]) for h in range(4)])
    orders = jnp.array([[(h + i) % 4 for h in range(4)] for i in range(4)])

    def per_row(operands):
        i, q_row, k_row, vt_row = operands
        order = orders[lax.rem(i, 4)]
        qh = q_row.reshape(1024, 4, 32)[:, order]
        kh = k_row.reshape(1024, 4, 32)[:, order]

        def per_head(ops):
            qx, kx, vx, bx, mx = ops
            s = jnp.dot(qx, kx.T, preferred_element_type=F32)
            bias = jnp.swapaxes(bx, 0, 1).reshape(1024, 1024).astype(F32)
            s = (s + bias) * LN2 + mx[:, None] + key_bias
            w = jax.nn.softmax(s, axis=-1)
            return jnp.dot(vx[:32].astype(F32), w.T, preferred_element_type=F32)

        o = lax.map(per_head, (jnp.moveaxis(qh, 1, 0), jnp.moveaxis(kh, 1, 0), vt_row, b, maxima))
        return o.reshape(128, 1024)

    return lax.map(per_row, (jnp.arange(8), q, k, vt))


def phase(z, mask_tile, gain, proj, gate_bias, bias_w, out_w, collective_id):
    q, k, vt, gate, piece = pre(z, gain, proj, bias_w, gate_bias, mask_tile)
    o, den, full = attention(piece, q, k, vt, collective_id)
    fine = jnp.all((den > 2.0 ** -60) & (den < 2.0 ** 100))
    o = lax.cond(fine, lambda: o, lambda: exact_attention(q, k, vt, full))
    return post(o, gate, z, out_w, 2 + collective_id)


def local(
    pair_in,
    residue_mask,
    norm_start,
    proj_start,
    gate_bias_start,
    bias_w_start,
    out_w_start,
    norm_end,
    proj_end,
    gate_bias_end,
    bias_w_end,
    out_w_end,
    norm_trans,
    trans_in,
    trans_bias,
    trans_out,
):
    device = lax.axis_index("gx") * 8 + lax.axis_index("gy")
    lane = lax.broadcasted_iota(jnp.int32, (8, 128), 1)
    row = lax.broadcasted_iota(jnp.int32, (8, 128), 0)
    spread = jnp.tile(residue_mask.astype(F32), 16).reshape(1, 128)
    mask_tile = jnp.where((lane // 8 == lax.rem(device, 16)) & (row == 0), spread, 0.0)
    z = phase(pair_in, mask_tile, norm_start, proj_start, gate_bias_start, bias_w_start, out_w_start, 0)
    z = phase(z, mask_tile, norm_end, proj_end, gate_bias_end, bias_w_end, out_w_end, 1)
    return trans(z, norm_trans, trans_in, trans_bias, trans_out)


def solution(mesh):
    rows = P(AX, None, None)
    placed = (rows, P(AX)) + (P(),) * 14

    def whole(*args):
        with jax.sharding.use_abstract_mesh(mesh.abstract_mesh):
            return jax.shard_map(local, mesh=mesh, in_specs=placed, out_specs=rows, check_vma=False)(*args)

    return whole
```

```python
import jax
import jax.numpy as jnp
from jax import lax
from jax.experimental import pallas as pl
from jax.experimental.pallas import tpu as pltpu
from jax.sharding import PartitionSpec as P

F32 = jnp.float32
BF = jnp.bfloat16
AX = ("gx", "gy")
HEADS = 4
HEAD_DIM = 32
LOG2E = 1.4426950408889634
LN2 = 0.6931471805599453
big_negative = 1000000000.0


MESH_ID = pl.DeviceIdType.MESH
ORDERS = ((0, 1, 2), (1, 2, 0), (2, 0, 1))
EXTRA = 26
PLANES = 36
EARLY = 43


def plane(h, t):
    if isinstance(t, int):
        return 12 * (t // 3) + 3 * h + t % 3
    return 12 * (t // 3) + 3 * h + lax.rem(t, 3)


class Torus:
    def __init__(self, piece_ref, full, send_sem, recv_sem):
        gx, gy = lax.axis_index("gx"), lax.axis_index("gy")
        self.core = lax.rem(gx, 2)
        self.here = (lax.rem(gx // 2, 4), gy // 2, lax.rem(gy, 2) * 2 + gx // 8)
        self.piece, self.full, self.send_sem, self.recv_sem = piece_ref, full, send_sem, recv_sem
        self.partner = self.device(self.here, 1 - self.core)
        self.sent = []

    def device(self, pos, c):
        px, py, pz = pos
        return ((lax.rem(pz, 2) * 4 + px) * 2 + c, py * 2 + pz // 2)

    def moved(self, dim, step):
        pos = list(self.here)
        pos[dim] = lax.rem(pos[dim] + step, 4)
        return tuple(pos)

    def region(self, lo, n, pos, done, other=False):
        px, py, pz = pos
        zl = slice(None) if 2 in done else lax.rem(pz, 2)
        zh = slice(None) if 2 in done else pz // 2
        xi = slice(None) if 0 in done else px
        yi = slice(None) if 1 in done else py
        return self.full.at[pl.ds(lo, n), zl, xi, 1 - self.core if other else self.core, yi, zh]

    def send(self, slot, lo, n, pos, done, dev, first=False):
        spot = self.region(lo, n, pos, done)
        pltpu.make_async_remote_copy(
            src_ref=self.piece.at[pl.ds(lo, n)] if first else spot, dst_ref=spot, send_sem=self.send_sem.at[slot],
            recv_sem=self.recv_sem.at[slot], device_id=dev, device_id_type=MESH_ID).start()

    def wait(self, slot, lo, n, pos, done, other=False, sent=False):
        spot = self.region(lo, n, pos, done, other)
        c = pltpu.make_async_remote_copy(
            src_ref=spot, dst_ref=spot, send_sem=self.send_sem.at[slot], recv_sem=self.recv_sem.at[slot],
            device_id=self.partner, device_id_type=MESH_ID)
        c.wait_send() if sent else c.wait_recv()

    def barrier(self):
        barrier = pltpu.get_barrier_semaphore()
        peers = [self.device(self.moved(d, s), self.core) for d in range(3) for s in (1, 3)] + [self.partner]
        for peer in peers:
            pl.semaphore_signal(barrier, inc=1, device_id=peer, device_id_type=MESH_ID)
        px, py, pz = self.here
        self.full[:, lax.rem(pz, 2), px, self.core, py, pz // 2] = self.piece[...]
        pl.semaphore_wait(barrier, 7)

    def outward(self, base, o, stage, lo, n):
        dim, done = ORDERS[o][stage], ORDERS[o][:stage]
        self.send(base, lo, n, self.here, done, self.device(self.moved(dim, 1), self.core), stage == 0)
        self.send(base + 1, lo, n, self.here, done, self.device(self.moved(dim, 3), self.core), stage == 0)

    def onward(self, base, o, stage, lo, n, n1):
        dim, done = ORDERS[o][stage], ORDERS[o][:stage]
        left, right = self.moved(dim, 3), self.moved(dim, 1)
        self.wait(base, lo, n, left, done)
        self.send(base + 2, lo, n1, left, done, self.device(right, self.core))
        self.wait(base + 1, lo, n, right, done)
        self.send(base + 3, lo + n1, n - n1, right, done, self.device(left, self.core))
        self.send(base + 4, lo, n, left, done, self.partner)
        self.send(base + 5, lo, n, right, done, self.partner)

    def closing(self, base, o, stage, lo, n, n1):
        dim, done = ORDERS[o][stage], ORDERS[o][:stage]
        far = self.moved(dim, 2)
        self.wait(base + 2, lo, n1, far, done)
        self.wait(base + 3, lo + n1, n - n1, far, done)
        self.send(base + 6, lo, n, far, done, self.partner)

    def shared(self, base, o, stage, lo, n):
        dim, done = ORDERS[o][stage], ORDERS[o][:stage]
        for k, step in ((4, 3), (5, 1), (6, 2)):
            self.wait(base + k, lo, n, self.moved(dim, step), done, True)

    def settled(self, base, o, stage, lo, n, n1):
        done = ORDERS[o][:stage]
        for k, size in ((0, n), (1, n), (2, n1), (3, n - n1), (4, n), (5, n), (6, n)):
            self.wait(base + k, lo, size, self.here, done, False, True)

    def early(self):
        for stage in range(2):
            bases = [21 * stage + 7 * o for o in range(3)]
            for o in range(3):
                self.outward(bases[o], o, stage, 12 * o, 12)
            if stage == 0:
                self.send(42, 0, PLANES, self.here, (), self.partner, True)
            for o in range(3):
                self.onward(bases[o], o, stage, 12 * o, 12, 6)
            for o in range(3):
                self.closing(bases[o], o, stage, 12 * o, 12, 6)

    def sizes(self, first):
        return ((3, 2), (3, 1), (3, 1) if first else (2, 1))

    def late(self, action, h, first=False):
        for o, (n, n1) in enumerate(self.sizes(first)):
            base, lo = EARLY + 21 * h + 7 * o, 12 * o + 3 * h
            if action in ("outward", "shared"):
                getattr(self, action)(base, o, 2, lo, n)
            else:
                getattr(self, action)(base, o, 2, lo, n, n1)

    def early_shared(self):
        self.wait(42, 0, PLANES, self.here, (), True)
        for stage in range(2):
            for o in range(3):
                self.shared(21 * stage + 7 * o, o, stage, 12 * o, 12)

    def finish(self):
        self.wait(42, 0, PLANES, self.here, (), False, True)
        for stage in range(2):
            for o in range(3):
                self.settled(21 * stage + 7 * o, o, stage, 12 * o, 12, 6)
        for h in range(4):
            self.late("settled", h, h == 0)


def attn_setup(q_ref, qs, eye, slot):
    lane = lax.broadcasted_iota(jnp.int32, (16, 128), 1) // 32
    for s in range(4):
        slot[s] = jnp.where(lane == s, 1.0, 0.0).astype(BF)
    rowi = lax.broadcasted_iota(jnp.int32, (128, 128), 0)
    coli = lax.broadcasted_iota(jnp.int32, (128, 128), 1)
    eye[...] = jnp.where(rowi == coli, 1.0, 0.0).astype(BF)

    def stack(n, _):
        at = pl.ds(pl.multiple_of(n * 128, 128), 128)
        for g in range(2):
            rows = [q_ref[4 * g + r, at, :] for r in range(4)]
            for h in range(4):
                s = None
                for r in range(4):
                    t = rows[r] * jnp.concatenate([slot[(h + r) % 4]] * 8, axis=0)
                    s = t if s is None else s + t
                qs[2 * h + g, at, :] = s
        return 0

    lax.fori_loop(0, 8, stack, 0)


def attn_mask(extra, mask_ref):
    placed = jnp.sum(extra.astype(F32).reshape(8, 16, 8, 128), axis=1)
    for t in range(8):
        mask_ref[:, t * 128:(t + 1) * 128] = jnp.broadcast_to(placed[t, 0:1, :], (16, 128)).astype(BF)


def attn_split(it):
    group = it // 4
    return lax.rem(group, 2), lax.rem(group // 2, 4), group // 8, lax.rem(it, 4)


def attn_loop(first, last, comm, k_ref, vt_ref, b_ref, o_ref, qs, eye, slot, ps, mask_ref, sacc, oacc):
    def push_qb(it, odd):
        g, h, qp, kp = attn_split(it)
        at = [pl.ds(pl.multiple_of(qp * 512 + m * 256, 256), 256) for m in range(2)]
        for m in range(2):
            rhs = jnp.concatenate([qs[2 * h + g, at[m], :], b_ref[plane(h, 2 * kp + odd), at[m], :]], axis=1)
            pltpu.matmul_push_rhs(rhs, 0, m, transpose=True)

    def pop_scores(par, odd, r, n):
        for m in range(2):
            ps[2 * par + m][r, odd * 128:odd * 128 + 128, :] = jnp.exp2(pltpu.matmul_pop(sacc[m][n]).astype(BF))

    def push_p(par, r):
        for m in range(2):
            pltpu.matmul_push_rhs(ps[2 * par + m][r], 1, m)

    def pv(it, r):
        g, h, _, kp = attn_split(it)
        at = pl.ds(pl.multiple_of(kp * 256, 256), 256)
        lhs = vt_ref[4 * g + r, h, :, at] * jnp.concatenate([mask_ref[:, at]] * 3, axis=0)
        for m in range(2):
            pltpu.matmul_acc_lhs(oacc[m][r], lhs, 1)

    def result(it):
        g, h, qp, _ = attn_split(it)
        for r in range(4):
            for m in range(2):
                o = pltpu.matmul_pop(oacc[m][r])
                d = o[32:33, :]
                at = pl.ds(pl.multiple_of(qp * 512 + m * 256, 256), 256)
                fine = (d > 2.0 ** -60) & (d < 2.0 ** 100)
                o_ref[4 * g + r, pl.ds(pl.multiple_of(h * 32, 32), 32), at] = o[0:32, :] * jnp.where(fine, 1.0 / d, jnp.nan)

    def step(it, par):
        g, h, qp, kp = attn_split(it)
        before = lax.max(it - 1, 0)
        for odd in range(2):
            for r in range(4):
                at = pl.ds(pl.multiple_of((2 * kp + odd) * 128, 128), 128)
                keep = jnp.concatenate([slot[lax.rem(h + r, 4)]] * 8, axis=0)
                lhs = jnp.concatenate([k_ref[4 * g + r, at, :] * keep, eye[...]], axis=1)
                if r >= 2:
                    pop_scores(1 - par if odd == 0 else par, 1 - odd, r, r)
                for m in range(2):
                    pltpu.matmul_acc_lhs(sacc[m][r], lhs, 0 if r == 0 else None)
                if r == 0:
                    if odd == 0:
                        push_qb(it, 1)
                    else:
                        push_qb(lax.min(it + 1, 63), 0)
                    push_p(1 - par, 2 * odd)
            pv(before, 2 * odd)
            push_p(1 - par, 2 * odd + 1)
            pv(before, 2 * odd + 1)
            for r in range(2):
                pop_scores(par, odd, r, r)

    def body(pair, _):
        step(2 * pair, 0)
        comm(pair + 1)

        @pl.when(lax.rem(pair, 2) == 0)
        def _():
            result(lax.max(2 * pair - 4, 0))

        step(2 * pair + 1, 1)
        return 0

    if first == 0:
        push_qb(0, 0)
    lax.fori_loop(first // 2, last // 2, body, 0)
    if last < 64:
        return
    par = (last - 1) % 2
    zero = jnp.zeros((128, 256), BF)
    for r in (2, 3):
        pop_scores(par, 1, r, r)
    for m in range(2):
        pltpu.matmul_acc_lhs(sacc[m][0], zero, 0)
        pltpu.matmul_pop(sacc[m][0])
    for r in range(4):
        push_p(par, r)
        pv(last - 1, r)
    result(last - 1)


def attn_kernel(piece_ref, w_ref, q_hbm, k_hbm, vt_hbm, gate_hbm, z_hbm, out_hbm, full, q_ref, k_ref, vt_ref, gate_ref, z_ref, qs, eye, slot, ps0, ps1, ps2, ps3, mask_ref, o_ref, wide, scr, outgoing, landed, note, notes, bad, send_sem, recv_sem, load_sem, push_sem, land_sem, note_send, note_recv, out_sem):
    ps = (ps0, ps1, ps2, ps3)
    gx, gy = lax.axis_index("gx"), lax.axis_index("gy")
    me = gx * 8 + gy
    pairs = ((q_hbm, q_ref), (k_hbm, k_ref), (vt_hbm, vt_ref), (gate_hbm, gate_ref), (z_hbm, z_ref))
    loads = [pltpu.make_async_copy(a, b, load_sem.at[n]) for n, (a, b) in enumerate(pairs)]
    for c in loads:
        c.start()
    torus = Torus(piece_ref, full, send_sem, recv_sem)
    torus.barrier()
    torus.early()
    torus.late("outward", 0, True)
    torus.late("outward", 1)
    for c in loads:
        c.wait()
    attn_setup(q_ref, qs, eye, slot)
    wide[...] = jnp.zeros((256, 256), BF)
    wide[0:128, 0:128] = w_ref[...]
    wide[128:256, 128:256] = w_ref[...]
    bad[...] = jnp.zeros((8, 128), F32)
    torus.late("onward", 0, True)
    torus.late("outward", 2)
    torus.late("onward", 1)
    torus.late("outward", 3)
    torus.late("closing", 0, True)
    torus.early_shared()
    torus.late("shared", 0, True)
    b_ref = full.reshape(PLANES, 1024, 128)
    attn_mask(b_ref[EXTRA], mask_ref)

    def block(dest):
        return pltpu.make_async_remote_copy(
            src_ref=outgoing.at[dest], dst_ref=landed.at[:, me], send_sem=push_sem, recv_sem=land_sem,
            device_id=(dest // 8, lax.rem(dest, 8)), device_id_type=MESH_ID)

    def hand_over(t, sacc, final):
        at = pl.ds(pl.multiple_of(t * 128, 128), 128)
        for m in range(2):
            pltpu.matmul_push_rhs(wide[...], 1, m)
        for rp in range(4):
            parts = []
            for i in (2 * rp, 2 * rp + 1):
                parts.append((jnp.transpose(o_ref[i, :, at]) * gate_ref[i, at].astype(F32)).astype(BF))
            pltpu.matmul_acc_lhs(sacc[rp % 2][rp // 2], jnp.concatenate(parts, axis=1), 1 if rp < 2 else None)
        worst = bad[...]
        for rp in range(4):
            y = pltpu.matmul_pop(sacc[rp % 2][rp // 2])
            for u in range(2):
                i = 2 * rp + u
                v = z_ref[i, at].astype(F32) + y[:, 128 * u:128 * u + 128]
                scr[pl.ds(i, 128, stride=8), :] = v
                off = jnp.where(jnp.abs(v) < 1e30, 0.0, 1.0).reshape(16, 8, 128)
                worst = jnp.maximum(worst, jnp.max(off, axis=0))
        bad[...] = worst
        outgoing[pl.ds(pl.multiple_of(t * 16, 16), 16)] = scr[...].astype(BF).reshape(16, 8, 8, 128)

        def push(n, _):
            dest = t * 16 + lax.rem(me + n, 16)

            @pl.when(dest != me)
            def _():
                block(dest).start()

            return 0

        lax.fori_loop(0, 16, push, 0)

    specs = []
    for m in range(2):
        specs += [pltpu.ACC(m)((128, 256), F32)] * 4 + [pltpu.ACC(m)((48, 256), F32)] * 4

    def run(*accs):
        sacc = [accs[8 * m:8 * m + 4] for m in range(2)]
        oacc = [accs[8 * m + 4:8 * m + 8] for m in range(2)]

        def comm(pair):
            @pl.when(pair < 13)
            def _():
                @pl.when((pair == 1) | (pair == 3))
                def _():
                    torus.late("onward", (pair + 3) // 2)

                @pl.when(lax.rem(pair, 4) == 2)
                def _():
                    torus.late("closing", (pair + 2) // 4)

                @pl.when((pair > 0) & (lax.rem(pair, 4) == 0))
                def _():
                    torus.late("shared", pair // 4)

            @pl.when((pair >= 18) & (pair < 22))
            def _():
                hand_over(lax.rem(pair - 18 + gx // 2, 4), sacc, False)

        attn_loop(0, 64, comm, k_ref, vt_ref, b_ref, o_ref, qs, eye, slot, ps, mask_ref, sacc, oacc)

        def tail(t, _):
            hand_over(4 + lax.rem(t + gx // 2, 4), sacc, True)
            return 0

        lax.fori_loop(0, 4, tail, 0)

    pl.run_scoped(run, *specs)
    seen = jnp.max(bad[...], axis=(0, 1), keepdims=True)
    note[...] = jnp.broadcast_to(seen, (8, 128))
    landed[:, me] = outgoing[me]
    notes[me] = note[...]

    def tell(dest):
        return pltpu.make_async_remote_copy(
            src_ref=note, dst_ref=notes.at[me], send_sem=note_send, recv_sem=note_recv,
            device_id=(dest // 8, lax.rem(dest, 8)), device_id_type=MESH_ID)

    def spread(n, _):
        tell(lax.rem(me + n, 128)).start()
        return 0

    lax.fori_loop(1, 128, spread, 0)
    torus.finish()
    neighbour = dict(device_id=(lax.rem(gx + 1, 16), gy), device_id_type=MESH_ID)
    blocks = pltpu.make_async_remote_copy(
        src_ref=outgoing.at[0:127], dst_ref=landed.at[:, 0:127], send_sem=push_sem, recv_sem=land_sem, **neighbour)
    all_notes = pltpu.make_async_remote_copy(
        src_ref=notes.at[0:127], dst_ref=notes.at[0:127], send_sem=note_send, recv_sem=note_recv, **neighbour)
    blocks.wait_recv()
    all_notes.wait_recv()
    worst = jnp.max(notes[...], axis=0)
    landed[0, 0, 0:8] = jnp.where(worst > 0.0, jnp.nan, landed[0, 0, 0:8].astype(F32)).astype(BF)
    out = pltpu.make_async_copy(landed, out_hbm, out_sem)
    out.start()
    blocks.wait_send()
    all_notes.wait_send()
    out.wait()


def attention(piece, w, q, k, vt, gate, z, collective_id):
    vmem = pl.BlockSpec(memory_space=pltpu.VMEM)
    hbm = pl.BlockSpec(memory_space=pl.ANY)
    rows = pltpu.VMEM((8, 1024, 128), BF)
    out = pl.pallas_call(
        attn_kernel,
        in_specs=[vmem, vmem] + [hbm] * 5,
        out_specs=hbm,
        out_shape=jax.ShapeDtypeStruct((8, 128, 8, 128), BF),
        scratch_shapes=[
            pltpu.VMEM((PLANES, 2, 4, 2, 4, 2, 8, 128), BF),
            rows,
            rows,
            pltpu.VMEM((8, 4, 48, 1024), BF),
            rows,
            rows,
            rows,
            pltpu.VMEM((128, 128), BF),
            pltpu.VMEM((4, 16, 128), BF),
            *[pltpu.VMEM((4, 256, 256), BF)] * 4,
            pltpu.VMEM((16, 1024), BF),
            pltpu.VMEM((8, 128, 1024), F32),
            pltpu.VMEM((256, 256), BF),
            pltpu.VMEM((1024, 128), F32),
            pltpu.VMEM((128, 8, 8, 128), BF),
            pltpu.VMEM((8, 128, 8, 128), BF),
            pltpu.VMEM((8, 128), F32),
            pltpu.VMEM((128, 8, 128), F32),
            pltpu.VMEM((8, 128), F32),
            pltpu.SemaphoreType.DMA((EARLY + 84,)),
            pltpu.SemaphoreType.DMA((EARLY + 84,)),
            pltpu.SemaphoreType.DMA((5,)),
            *[pltpu.SemaphoreType.DMA] * 5,
        ],
        compiler_params=pltpu.CompilerParams(collective_id=collective_id, has_side_effects=True, vmem_limit_bytes=48 * 2**20),
        name="tri_attn",
    )(piece, w, q, k, vt, gate, z)
    return out.reshape(8, 1024, 128)


def layer_norm(x, gain):
    mean = jnp.mean(x, axis=-1, keepdims=True)
    c = x - mean
    var = jnp.mean(c * c, axis=-1, keepdims=True)
    return (c * lax.rsqrt(var + 1e-05) * gain).astype(BF)


def pre_kernel(z_ref, gain_ref, proj_ref, bw_ref, gb_ref, mask_ref, q_ref, k_ref, vt_ref, gate_ref, b_ref, scr):
    i = pl.program_id(0)

    @pl.when(i == 0)
    def _():
        scr[...] = jnp.zeros((PLANES, 8, 128), F32)
        scr[EXTRA] = mask_ref[...]

    a = layer_norm(z_ref[0].astype(F32), gain_ref[...])
    shift = 32 * lax.rem(i, 4)
    rolled = [pltpu.roll(proj_ref[:, 128 * n:128 * n + 128].astype(F32), shift, 1) for n in range(2)]
    qk = jnp.dot(a, jnp.concatenate(rolled, axis=1).astype(BF), preferred_element_type=F32)
    q_ref[0] = (qk[:, :128] * (HEAD_DIM ** -0.5 * LOG2E)).astype(BF)
    k_ref[0] = qk[:, 128:].astype(BF)
    vg = jnp.dot(a, proj_ref[:, 256:512], preferred_element_type=F32)
    vt = jnp.transpose(vg[:, :128].astype(BF))
    tail = jnp.where(lax.broadcasted_iota(jnp.int32, (16, 1024), 0) == 0, 1.0, 0.0).astype(BF)
    for h in range(4):
        vt_ref[0, h, 0:32, :] = vt[32 * h:32 * h + 32, :]
        vt_ref[0, h, 32:48, :] = tail
    gate_ref[0] = jax.nn.sigmoid(vg[:, 128:] + gb_ref[...]).astype(BF)
    b = lax.dot_general(bw_ref[...], a, (((1,), (1,)), ((), ())), preferred_element_type=F32)
    b = b.astype(BF).astype(F32)
    m = jnp.max(b, axis=-1, keepdims=True)
    b = (b - m) * LOG2E
    for h in range(4):
        for kt in range(8):
            scr[plane(h, kt), pl.ds(i, 1), :] = b[h:h + 1, kt * 128:(kt + 1) * 128]
    lane = lax.broadcasted_iota(jnp.int32, (4, 128), 1)
    scr[EXTRA, 1:5, :] = jnp.where(lane == i, m[0:4], scr[EXTRA, 1:5, :])

    @pl.when(i == 7)
    def _():
        b_ref[...] = scr[...].astype(BF)


def pre(z, gain, proj, bias_w, gate_bias, mask_tile):
    bwt = jnp.pad(jnp.transpose(bias_w), ((0, 12), (0, 0)))
    row = lambda i: (i, 0, 0)
    return pl.pallas_call(
        pre_kernel,
        grid=(8,),
        in_specs=[
            pl.BlockSpec((1, 1024, 128), row),
            pl.BlockSpec((1, 128), lambda i: (0, 0)),
            pl.BlockSpec((128, 512), lambda i: (0, 0)),
            pl.BlockSpec((16, 128), lambda i: (0, 0)),
            pl.BlockSpec((1, 128), lambda i: (0, 0)),
            pl.BlockSpec((8, 128), lambda i: (0, 0)),
        ],
        out_specs=[
            pl.BlockSpec((1, 1024, 128), row),
            pl.BlockSpec((1, 1024, 128), row),
            pl.BlockSpec((1, 4, 48, 1024), lambda i: (i, 0, 0, 0)),
            pl.BlockSpec((1, 1024, 128), row),
            pl.BlockSpec((PLANES, 8, 128), lambda i: (0, 0, 0)),
        ],
        out_shape=[
            jax.ShapeDtypeStruct((8, 1024, 128), BF),
            jax.ShapeDtypeStruct((8, 1024, 128), BF),
            jax.ShapeDtypeStruct((8, 4, 48, 1024), BF),
            jax.ShapeDtypeStruct((8, 1024, 128), BF),
            jax.ShapeDtypeStruct((PLANES, 8, 128), BF),
        ],
        scratch_shapes=[pltpu.VMEM((PLANES, 8, 128), F32)],
        compiler_params=pltpu.CompilerParams(vmem_limit_bytes=48 * 2**20),
        name="tri_pre",
    )(z, gain.reshape(1, 128), proj, bwt, gate_bias.reshape(1, 128), mask_tile)


def trans_kernel(z_ref, gain_ref, w1_ref, b1_ref, w2_ref, out_ref, flag_ref):
    z = z_ref[0].astype(F32)

    @pl.when(pl.program_id(0) == 0)
    def _():
        flag_ref[...] = jnp.zeros((8, 128), F32)

    off = jnp.where(jnp.abs(z[0:16]) < 1e30, 0.0, 1.0)
    flag_ref[...] = jnp.maximum(flag_ref[...], jnp.maximum(off[0:8], off[8:16]))
    a = layer_norm(z, gain_ref[...])
    hid = jax.nn.relu(jnp.dot(a, w1_ref[...], preferred_element_type=F32) + b1_ref[...]).astype(BF)
    out_ref[0] = (z + jnp.dot(hid, w2_ref[...], preferred_element_type=F32)).astype(BF)


def trans(z, gain, w1, b1, w2):
    row = lambda i: (i, 0, 0)
    whole = lambda i: (0, 0)
    return pl.pallas_call(
        trans_kernel,
        grid=(8,),
        in_specs=[
            pl.BlockSpec((1, 1024, 128), row),
            pl.BlockSpec((1, 128), whole),
            pl.BlockSpec((128, 512), whole),
            pl.BlockSpec((1, 512), whole),
            pl.BlockSpec((512, 128), whole),
        ],
        out_specs=[pl.BlockSpec((1, 1024, 128), row), pl.BlockSpec((8, 128), whole)],
        out_shape=[jax.ShapeDtypeStruct((8, 1024, 128), BF), jax.ShapeDtypeStruct((8, 128), F32)],
        compiler_params=pltpu.CompilerParams(vmem_limit_bytes=48 * 2**20),
        name="tri_trans",
    )(z, gain.reshape(1, 128), w1, b1.reshape(1, 512), w2)


def exact_phase(z, mask, gain, proj, gate_bias, bias_w, out_w):
    key_bias = (mask - 1.0) * big_negative
    a = layer_norm(z.astype(F32), gain)
    p = jnp.dot(a.reshape(8192, 128), proj, preferred_element_type=F32).reshape(8, 1024, 512)
    q, k, v = [jnp.moveaxis(p[..., 128 * n:128 * n + 128].astype(BF).reshape(8, 1024, 4, 32), 2, 0) for n in range(3)]
    b = jnp.dot(a.reshape(8192, 128), bias_w, preferred_element_type=F32).astype(BF).reshape(8, 1024, 4)
    b = lax.all_gather(jnp.transpose(b, (2, 0, 1)), AX, axis=1, tiled=True)

    def per_head(ops):
        qh, kh, vh, bh = ops

        def per_row(rows):
            qr, kr, vr = rows
            s = jnp.dot(qr, kr.T, preferred_element_type=F32) * HEAD_DIM ** -0.5 + bh.astype(F32) + key_bias
            return jnp.dot(jax.nn.softmax(s, axis=-1), vr.astype(F32), preferred_element_type=F32)

        return lax.map(per_row, (qh, kh, vh))

    o = jnp.moveaxis(lax.map(per_head, (q, k, v, b)), 0, 2).reshape(8, 1024, 128)
    gated = (o * jax.nn.sigmoid(p[..., 384:] + gate_bias)).astype(BF)
    y = jnp.dot(gated.reshape(8192, 128), out_w, preferred_element_type=F32).reshape(8, 1024, 128)
    z = (z.astype(F32) + y).astype(BF)
    z = lax.all_to_all(z, AX, split_axis=1, concat_axis=0, tiled=True)
    return jnp.swapaxes(z, 0, 1)


def exact(z, mask_local, phases, last):
    mask = lax.all_gather(mask_local.astype(F32), AX, axis=0, tiled=True)
    stacked = [jnp.stack(pair) for pair in zip(*phases)]
    z, _ = lax.scan(lambda z, ws: (exact_phase(z, mask, *ws), None), z, stacked)
    gain, w1, b1, w2 = last
    a = layer_norm(z.astype(F32), gain).reshape(8192, 128)
    hid = jax.nn.relu(jnp.dot(a, w1, preferred_element_type=F32) + b1).astype(BF)
    return (z.astype(F32) + jnp.dot(hid, w2, preferred_element_type=F32).reshape(8, 1024, 128)).astype(BF)


def phase(z, mask_tile, collective_id, gain, proj, gate_bias, bias_w, out_w):
    q, k, vt, gate, piece = pre(z, gain, proj, bias_w, gate_bias, mask_tile)
    return attention(piece, out_w, q, k, vt, gate, z, collective_id)


def local(
    pair_in,
    residue_mask,
    norm_start,
    proj_start,
    gate_bias_start,
    bias_w_start,
    out_w_start,
    norm_end,
    proj_end,
    gate_bias_end,
    bias_w_end,
    out_w_end,
    norm_trans,
    trans_in,
    trans_bias,
    trans_out,
):
    device = lax.axis_index("gx") * 8 + lax.axis_index("gy")
    lane = lax.broadcasted_iota(jnp.int32, (8, 128), 1)
    row = lax.broadcasted_iota(jnp.int32, (8, 128), 0)
    spread = jnp.tile(residue_mask.astype(F32), 16).reshape(1, 128)
    mask_tile = jnp.where((lane // 8 == lax.rem(device, 16)) & (row == 0), spread, 0.0)
    start = (norm_start, proj_start, gate_bias_start, bias_w_start, out_w_start)
    end = (norm_end, proj_end, gate_bias_end, bias_w_end, out_w_end)
    z = phase(pair_in, mask_tile, 0, *start)
    z = phase(z, mask_tile, 1, *end)
    last = (norm_trans, trans_in, trans_bias, trans_out)
    out, flag = trans(z, *last)
    return lax.cond(jnp.max(flag) == 0.0, lambda: out, lambda: exact(pair_in, residue_mask, (start, end), last))


def solution(mesh):
    rows = P(AX, None, None)
    placed = (rows, P(AX)) + (P(),) * 14

    def whole(*args):
        with jax.sharding.use_abstract_mesh(mesh.abstract_mesh):
            return jax.shard_map(local, mesh=mesh, in_specs=placed, out_specs=rows, check_vma=False)(*args)

    return whole
```

```python
import jax
import jax.numpy as jnp
from jax import lax
from jax.experimental import pallas as pl
from jax.experimental.pallas import tpu as pltpu
from jax.sharding import PartitionSpec as P

F32 = jnp.float32
BF = jnp.bfloat16
AX = ("gx", "gy")
HEADS = 4
HEAD_DIM = 32
LOG2E = 1.4426950408889634
LN2 = 0.6931471805599453
big_negative = 1000000000.0


MESH_ID = pl.DeviceIdType.MESH
ORDERS = ((0, 1, 2), (1, 2, 0), (2, 0, 1))
EXTRA = 26
PLANES = 36
EARLY = 43


def plane(h, t):
    if isinstance(t, int):
        return 12 * (t // 3) + 3 * h + t % 3
    return 12 * (t // 3) + 3 * h + lax.rem(t, 3)


class Torus:
    def __init__(self, piece_ref, full, send_sem, recv_sem):
        gx, gy = lax.axis_index("gx"), lax.axis_index("gy")
        self.core = lax.rem(gx, 2)
        self.here = (lax.rem(gx // 2, 4), gy // 2, lax.rem(gy, 2) * 2 + gx // 8)
        self.piece, self.full, self.send_sem, self.recv_sem = piece_ref, full, send_sem, recv_sem
        self.partner = self.device(self.here, 1 - self.core)
        self.sent = []

    def device(self, pos, c):
        px, py, pz = pos
        return ((lax.rem(pz, 2) * 4 + px) * 2 + c, py * 2 + pz // 2)

    def moved(self, dim, step):
        pos = list(self.here)
        pos[dim] = lax.rem(pos[dim] + step, 4)
        return tuple(pos)

    def region(self, lo, n, pos, done, other=False):
        px, py, pz = pos
        zl = slice(None) if 2 in done else lax.rem(pz, 2)
        zh = slice(None) if 2 in done else pz // 2
        xi = slice(None) if 0 in done else px
        yi = slice(None) if 1 in done else py
        return self.full.at[pl.ds(lo, n), zl, xi, 1 - self.core if other else self.core, yi, zh]

    def send(self, slot, lo, n, pos, done, dev, first=False):
        spot = self.region(lo, n, pos, done)
        pltpu.make_async_remote_copy(
            src_ref=self.piece.at[pl.ds(lo, n)] if first else spot, dst_ref=spot, send_sem=self.send_sem.at[slot],
            recv_sem=self.recv_sem.at[slot], device_id=dev, device_id_type=MESH_ID).start()

    def wait(self, slot, lo, n, pos, done, other=False, sent=False):
        spot = self.region(lo, n, pos, done, other)
        c = pltpu.make_async_remote_copy(
            src_ref=spot, dst_ref=spot, send_sem=self.send_sem.at[slot], recv_sem=self.recv_sem.at[slot],
            device_id=self.partner, device_id_type=MESH_ID)
        c.wait_send() if sent else c.wait_recv()

    def barrier(self):
        barrier = pltpu.get_barrier_semaphore()
        peers = [self.device(self.moved(d, s), self.core) for d in range(3) for s in (1, 3)] + [self.partner]
        for peer in peers:
            pl.semaphore_signal(barrier, inc=1, device_id=peer, device_id_type=MESH_ID)
        px, py, pz = self.here
        self.full[:, lax.rem(pz, 2), px, self.core, py, pz // 2] = self.piece[...]
        pl.semaphore_wait(barrier, 7)

    def outward(self, base, o, stage, lo, n):
        dim, done = ORDERS[o][stage], ORDERS[o][:stage]
        self.send(base, lo, n, self.here, done, self.device(self.moved(dim, 1), self.core), stage == 0)
        self.send(base + 1, lo, n, self.here, done, self.device(self.moved(dim, 3), self.core), stage == 0)

    def onward(self, base, o, stage, lo, n, n1):
        dim, done = ORDERS[o][stage], ORDERS[o][:stage]
        left, right = self.moved(dim, 3), self.moved(dim, 1)
        self.wait(base, lo, n, left, done)
        self.send(base + 2, lo, n1, left, done, self.device(right, self.core))
        self.wait(base + 1, lo, n, right, done)
        self.send(base + 3, lo + n1, n - n1, right, done, self.device(left, self.core))
        self.send(base + 4, lo, n, left, done, self.partner)
        self.send(base + 5, lo, n, right, done, self.partner)

    def closing(self, base, o, stage, lo, n, n1):
        dim, done = ORDERS[o][stage], ORDERS[o][:stage]
        far = self.moved(dim, 2)
        self.wait(base + 2, lo, n1, far, done)
        self.wait(base + 3, lo + n1, n - n1, far, done)
        self.send(base + 6, lo, n, far, done, self.partner)

    def shared(self, base, o, stage, lo, n):
        dim, done = ORDERS[o][stage], ORDERS[o][:stage]
        for k, step in ((4, 3), (5, 1), (6, 2)):
            self.wait(base + k, lo, n, self.moved(dim, step), done, True)

    def settled(self, base, o, stage, lo, n, n1):
        done = ORDERS[o][:stage]
        for k, size in ((0, n), (1, n), (2, n1), (3, n - n1), (4, n), (5, n), (6, n)):
            self.wait(base + k, lo, size, self.here, done, False, True)

    def early(self):
        for stage in range(2):
            bases = [21 * stage + 7 * o for o in range(3)]
            for o in range(3):
                self.outward(bases[o], o, stage, 12 * o, 12)
            if stage == 0:
                self.send(42, 0, PLANES, self.here, (), self.partner, True)
            for o in range(3):
                self.onward(bases[o], o, stage, 12 * o, 12, 6)
            for o in range(3):
                self.closing(bases[o], o, stage, 12 * o, 12, 6)

    def sizes(self, first):
        return ((3, 2), (3, 1), (3, 1) if first else (2, 1))

    def late(self, action, h, first=False):
        for o, (n, n1) in enumerate(self.sizes(first)):
            base, lo = EARLY + 21 * h + 7 * o, 12 * o + 3 * h
            if action in ("outward", "shared"):
                getattr(self, action)(base, o, 2, lo, n)
            else:
                getattr(self, action)(base, o, 2, lo, n, n1)

    def early_shared(self):
        self.wait(42, 0, PLANES, self.here, (), True)
        for stage in range(2):
            for o in range(3):
                self.shared(21 * stage + 7 * o, o, stage, 12 * o, 12)

    def finish(self):
        self.wait(42, 0, PLANES, self.here, (), False, True)
        for stage in range(2):
            for o in range(3):
                self.settled(21 * stage + 7 * o, o, stage, 12 * o, 12, 6)
        for h in range(4):
            self.late("settled", h, h == 0)


def attn_setup(q_ref, qs, eye, slot):
    lane = lax.broadcasted_iota(jnp.int32, (16, 128), 1) // 32
    for s in range(4):
        slot[s] = jnp.where(lane == s, 1.0, 0.0).astype(BF)
    rowi = lax.broadcasted_iota(jnp.int32, (128, 128), 0)
    coli = lax.broadcasted_iota(jnp.int32, (128, 128), 1)
    eye[...] = jnp.where(rowi == coli, 1.0, 0.0).astype(BF)

    def stack(n, _):
        at = pl.ds(pl.multiple_of(n * 128, 128), 128)
        for g in range(2):
            rows = [q_ref[4 * g + r, at, :] for r in range(4)]
            for h in range(4):
                s = None
                for r in range(4):
                    t = rows[r] * jnp.concatenate([slot[(h + r) % 4]] * 8, axis=0)
                    s = t if s is None else s + t
                qs[2 * h + g, at, :] = s
        return 0

    lax.fori_loop(0, 8, stack, 0)


def attn_mask(extra, mask_ref):
    placed = jnp.sum(extra.astype(F32).reshape(8, 16, 8, 128), axis=1)
    for t in range(8):
        mask_ref[:, t * 128:(t + 1) * 128] = jnp.broadcast_to(placed[t, 0:1, :], (16, 128)).astype(BF)


def attn_split(it):
    group = it // 4
    late = group >= 8
    head = jnp.where(late, lax.rem(group, 4), group // 2)
    quarter = jnp.where(late, group // 4, lax.rem(group, 2))
    return head, quarter, lax.rem(it, 4)


def attn_loop(first, last, comm, k_ref, vt_ref, b_ref, o_ref, qs, eye, slot, ps, mask_ref, sacc, oacc):
    def push_qb(it, odd):
        h, qp, kp = attn_split(it)
        at = pl.ds(pl.multiple_of(qp * 256, 256), 256)
        for m in range(2):
            rhs = jnp.concatenate([qs[2 * h + m, at, :], b_ref[plane(h, 2 * kp + odd), at, :]], axis=1)
            pltpu.matmul_push_rhs(rhs, 0, m, transpose=True)

    def pop_scores(par, odd, r, n):
        for m in range(2):
            ps[2 * par + m][r, odd * 128:odd * 128 + 128, :] = jnp.exp2(pltpu.matmul_pop(sacc[m][n]).astype(BF))

    def push_p(par, r):
        for m in range(2):
            pltpu.matmul_push_rhs(ps[2 * par + m][r], 1, m)

    def pv(it, r):
        h, _, kp = attn_split(it)
        at = pl.ds(pl.multiple_of(kp * 256, 256), 256)
        keep = jnp.concatenate([mask_ref[:, at]] * 3, axis=0)
        for m in range(2):
            pltpu.matmul_acc_lhs(oacc[m][r], vt_ref[4 * m + r, h, :, at] * keep, 1)

    def result(it):
        h, qp, _ = attn_split(it)
        at = pl.ds(pl.multiple_of(qp * 256, 256), 256)
        for r in range(4):
            for m in range(2):
                o = pltpu.matmul_pop(oacc[m][r])
                d = o[32:33, :]
                fine = (d > 2.0 ** -60) & (d < 2.0 ** 100)
                o_ref[4 * m + r, pl.ds(pl.multiple_of(h * 32, 32), 32), at] = o[0:32, :] * jnp.where(fine, 1.0 / d, jnp.nan)

    def step(it, par):
        h, _, kp = attn_split(it)
        before = lax.max(it - 1, 0)
        for odd in range(2):
            for r in range(4):
                at = pl.ds(pl.multiple_of((2 * kp + odd) * 128, 128), 128)
                keep = jnp.concatenate([slot[lax.rem(h + r, 4)]] * 8, axis=0)
                if r >= 2:
                    pop_scores(1 - par if odd == 0 else par, 1 - odd, r, r)
                for m in range(2):
                    lhs = jnp.concatenate([k_ref[4 * m + r, at, :] * keep, eye[...]], axis=1)
                    pltpu.matmul_acc_lhs(sacc[m][r], lhs, 0 if r == 0 else None)
                if r == 0:
                    if odd == 0:
                        push_qb(it, 1)
                    else:
                        push_qb(lax.min(it + 1, 63), 0)
                    push_p(1 - par, 2 * odd)
            pv(before, 2 * odd)
            push_p(1 - par, 2 * odd + 1)
            pv(before, 2 * odd + 1)
            for r in range(2):
                pop_scores(par, odd, r, r)

    def body(pair, _):
        step(2 * pair, 0)
        comm(pair + 1)

        @pl.when(lax.rem(pair, 2) == 0)
        def _():
            result(lax.max(2 * pair - 4, 0))

        step(2 * pair + 1, 1)
        return 0

    if first == 0:
        push_qb(0, 0)
    lax.fori_loop(first // 2, last // 2, body, 0)
    if last < 64:
        return
    par = (last - 1) % 2
    zero = jnp.zeros((128, 256), BF)
    for r in (2, 3):
        pop_scores(par, 1, r, r)
    for m in range(2):
        pltpu.matmul_acc_lhs(sacc[m][0], zero, 0)
        pltpu.matmul_pop(sacc[m][0])
    for r in range(4):
        push_p(par, r)
        pv(last - 1, r)
    result(last - 1)


def attn_kernel(piece_ref, w_ref, q_hbm, k_hbm, vt_hbm, gate_hbm, z_hbm, out_hbm, full, q_ref, k_ref, vt_ref, gate_ref, z_ref, qs, eye, slot, ps0, ps1, ps2, ps3, mask_ref, o_ref, wide, scr, outgoing, landed, note, notes, bad, send_sem, recv_sem, load_sem, push_sem, land_sem, note_send, note_recv, out_sem):
    ps = (ps0, ps1, ps2, ps3)
    gx, gy = lax.axis_index("gx"), lax.axis_index("gy")
    me = gx * 8 + gy
    pairs = ((q_hbm, q_ref), (k_hbm, k_ref), (vt_hbm, vt_ref), (gate_hbm, gate_ref), (z_hbm, z_ref))
    loads = [pltpu.make_async_copy(a, b, load_sem.at[n]) for n, (a, b) in enumerate(pairs)]
    for c in loads:
        c.start()
    torus = Torus(piece_ref, full, send_sem, recv_sem)
    torus.barrier()
    torus.early()
    torus.late("outward", 0, True)
    torus.late("outward", 1)
    for c in loads:
        c.wait()
    attn_setup(q_ref, qs, eye, slot)
    wide[...] = jnp.zeros((256, 256), BF)
    wide[0:128, 0:128] = w_ref[...]
    wide[128:256, 128:256] = w_ref[...]
    bad[...] = jnp.zeros((8, 128), F32)
    torus.late("onward", 0, True)
    torus.late("outward", 2)
    torus.late("onward", 1)
    torus.late("outward", 3)
    torus.late("closing", 0, True)
    torus.early_shared()
    torus.late("shared", 0, True)
    b_ref = full.reshape(PLANES, 1024, 128)
    attn_mask(b_ref[EXTRA], mask_ref)

    def block(dest):
        return pltpu.make_async_remote_copy(
            src_ref=outgoing.at[dest], dst_ref=landed.at[:, me], send_sem=push_sem, recv_sem=land_sem,
            device_id=(dest // 8, lax.rem(dest, 8)), device_id_type=MESH_ID)

    def hand_over(t, sacc):
        at = pl.ds(pl.multiple_of(t * 128, 128), 128)
        for m in range(2):
            pltpu.matmul_push_rhs(wide[...], 1, m)
        for rp in range(4):
            parts = []
            for i in (2 * rp, 2 * rp + 1):
                parts.append((jnp.transpose(o_ref[i, :, at]) * gate_ref[i, at].astype(F32)).astype(BF))
            pltpu.matmul_acc_lhs(sacc[rp % 2][rp // 2], jnp.concatenate(parts, axis=1), 1 if rp < 2 else None)
        worst = bad[...]
        for rp in range(4):
            y = pltpu.matmul_pop(sacc[rp % 2][rp // 2])
            for u in range(2):
                i = 2 * rp + u
                v = z_ref[i, at].astype(F32) + y[:, 128 * u:128 * u + 128]
                scr[pl.ds(i, 128, stride=8), :] = v
                off = jnp.where(jnp.abs(v) < 1e30, 0.0, 1.0).reshape(16, 8, 128)
                worst = jnp.maximum(worst, jnp.max(off, axis=0))
        bad[...] = worst
        outgoing[pl.ds(pl.multiple_of(t * 16, 16), 16)] = scr[...].astype(BF).reshape(16, 8, 8, 128)

        def push(n, _):
            dest = t * 16 + lax.rem(me + n, 16)

            @pl.when(dest != me)
            def _():
                block(dest).start()

            return 0

        lax.fori_loop(0, 16, push, 0)

    specs = []
    for m in range(2):
        specs += [pltpu.ACC(m)((128, 256), F32)] * 4 + [pltpu.ACC(m)((48, 256), F32)] * 4

    def run(*accs):
        sacc = [accs[8 * m:8 * m + 4] for m in range(2)]
        oacc = [accs[8 * m + 4:8 * m + 8] for m in range(2)]

        def comm(pair):
            @pl.when(pair < 13)
            def _():
                @pl.when((pair == 1) | (pair == 3))
                def _():
                    torus.late("onward", (pair + 3) // 2)

                @pl.when(lax.rem(pair, 4) == 2)
                def _():
                    torus.late("closing", (pair + 2) // 4)

                @pl.when((pair > 0) & (lax.rem(pair, 4) == 0))
                def _():
                    torus.late("shared", pair // 4)

            @pl.when((pair >= 18) & (pair < 22))
            def _():
                hand_over(lax.rem(pair - 18 + gx // 2, 4), sacc)

            @pl.when((pair >= 26) & (pair < 28))
            def _():
                hand_over(4 + lax.rem(pair + gx // 2, 2), sacc)

        attn_loop(0, 64, comm, k_ref, vt_ref, b_ref, o_ref, qs, eye, slot, ps, mask_ref, sacc, oacc)

        def tail(t, _):
            hand_over(6 + lax.rem(t + gx // 2, 2), sacc)
            return 0

        lax.fori_loop(0, 2, tail, 0)

    pl.run_scoped(run, *specs)
    seen = jnp.max(bad[...], axis=(0, 1), keepdims=True)
    note[...] = jnp.broadcast_to(seen, (8, 128))
    landed[:, me] = outgoing[me]
    notes[me] = note[...]

    def tell(dest):
        return pltpu.make_async_remote_copy(
            src_ref=note, dst_ref=notes.at[me], send_sem=note_send, recv_sem=note_recv,
            device_id=(dest // 8, lax.rem(dest, 8)), device_id_type=MESH_ID)

    def spread(n, _):
        tell(lax.rem(me + n, 128)).start()
        return 0

    lax.fori_loop(1, 128, spread, 0)
    torus.finish()
    neighbour = dict(device_id=(lax.rem(gx + 1, 16), gy), device_id_type=MESH_ID)
    blocks = pltpu.make_async_remote_copy(
        src_ref=outgoing.at[0:127], dst_ref=landed.at[:, 0:127], send_sem=push_sem, recv_sem=land_sem, **neighbour)
    all_notes = pltpu.make_async_remote_copy(
        src_ref=notes.at[0:127], dst_ref=notes.at[0:127], send_sem=note_send, recv_sem=note_recv, **neighbour)
    blocks.wait_recv()
    all_notes.wait_recv()
    worst = jnp.max(notes[...], axis=0)
    landed[0, 0, 0:8] = jnp.where(worst > 0.0, jnp.nan, landed[0, 0, 0:8].astype(F32)).astype(BF)
    out = pltpu.make_async_copy(landed, out_hbm, out_sem)
    out.start()
    blocks.wait_send()
    all_notes.wait_send()
    out.wait()


def attention(piece, w, q, k, vt, gate, z, collective_id):
    vmem = pl.BlockSpec(memory_space=pltpu.VMEM)
    hbm = pl.BlockSpec(memory_space=pl.ANY)
    rows = pltpu.VMEM((8, 1024, 128), BF)
    out = pl.pallas_call(
        attn_kernel,
        in_specs=[vmem, vmem] + [hbm] * 5,
        out_specs=hbm,
        out_shape=jax.ShapeDtypeStruct((8, 128, 8, 128), BF),
        scratch_shapes=[
            pltpu.VMEM((PLANES, 2, 4, 2, 4, 2, 8, 128), BF),
            rows,
            rows,
            pltpu.VMEM((8, 4, 48, 1024), BF),
            rows,
            rows,
            rows,
            pltpu.VMEM((128, 128), BF),
            pltpu.VMEM((4, 16, 128), BF),
            *[pltpu.VMEM((4, 256, 256), BF)] * 4,
            pltpu.VMEM((16, 1024), BF),
            pltpu.VMEM((8, 128, 1024), F32),
            pltpu.VMEM((256, 256), BF),
            pltpu.VMEM((1024, 128), F32),
            pltpu.VMEM((128, 8, 8, 128), BF),
            pltpu.VMEM((8, 128, 8, 128), BF),
            pltpu.VMEM((8, 128), F32),
            pltpu.VMEM((128, 8, 128), F32),
            pltpu.VMEM((8, 128), F32),
            pltpu.SemaphoreType.DMA((EARLY + 84,)),
            pltpu.SemaphoreType.DMA((EARLY + 84,)),
            pltpu.SemaphoreType.DMA((5,)),
            *[pltpu.SemaphoreType.DMA] * 5,
        ],
        compiler_params=pltpu.CompilerParams(collective_id=collective_id, has_side_effects=True, vmem_limit_bytes=48 * 2**20),
        name="tri_attn",
    )(piece, w, q, k, vt, gate, z)
    return out.reshape(8, 1024, 128)


def layer_norm(x, gain):
    mean = jnp.mean(x, axis=-1, keepdims=True)
    c = x - mean
    var = jnp.mean(c * c, axis=-1, keepdims=True)
    return (c * lax.rsqrt(var + 1e-05) * gain).astype(BF)


def pre_kernel(z_ref, gain_ref, proj_ref, bw_ref, gb_ref, mask_ref, q_ref, k_ref, vt_ref, gate_ref, b_ref, scr, wqk):
    i = pl.program_id(0)

    @pl.when(i == 0)
    def _():
        for s in range(4):
            for n in range(2):
                w = proj_ref[:, 128 * n:128 * n + 128].astype(F32)
                wqk[s, :, 128 * n:128 * n + 128] = (pltpu.roll(w, 32 * s, 1) if s else w).astype(BF)
        scr[...] = jnp.zeros((PLANES, 8, 128), F32)
        scr[EXTRA] = mask_ref[...]

    a = layer_norm(z_ref[0].astype(F32), gain_ref[...])
    qk = jnp.dot(a, wqk[lax.rem(i, 4)], preferred_element_type=F32)
    q_ref[0] = (qk[:, :128] * (HEAD_DIM ** -0.5 * LOG2E)).astype(BF)
    k_ref[0] = qk[:, 128:].astype(BF)
    vg = jnp.dot(a, proj_ref[:, 256:512], preferred_element_type=F32)
    vt = jnp.transpose(vg[:, :128].astype(BF))
    tail = jnp.where(lax.broadcasted_iota(jnp.int32, (16, 1024), 0) == 0, 1.0, 0.0).astype(BF)
    for h in range(4):
        vt_ref[0, h, 0:32, :] = vt[32 * h:32 * h + 32, :]
        vt_ref[0, h, 32:48, :] = tail
    gate_ref[0] = jax.nn.sigmoid(vg[:, 128:] + gb_ref[...]).astype(BF)
    b = lax.dot_general(bw_ref[...], a, (((1,), (1,)), ((), ())), preferred_element_type=F32)
    b = b.astype(BF).astype(F32)
    m = jnp.max(b, axis=-1, keepdims=True)
    b = (b - m) * LOG2E
    for h in range(4):
        for kt in range(8):
            scr[plane(h, kt), pl.ds(i, 1), :] = b[h:h + 1, kt * 128:(kt + 1) * 128]
    lane = lax.broadcasted_iota(jnp.int32, (4, 128), 1)
    scr[EXTRA, 1:5, :] = jnp.where(lane == i, m[0:4], scr[EXTRA, 1:5, :])

    @pl.when(i == 7)
    def _():
        b_ref[...] = scr[...].astype(BF)


def pre(z, gain, proj, bias_w, gate_bias, mask_tile):
    bwt = jnp.pad(jnp.transpose(bias_w), ((0, 12), (0, 0)))
    row = lambda i: (i, 0, 0)
    return pl.pallas_call(
        pre_kernel,
        grid=(8,),
        in_specs=[
            pl.BlockSpec((1, 1024, 128), row),
            pl.BlockSpec((1, 128), lambda i: (0, 0)),
            pl.BlockSpec((128, 512), lambda i: (0, 0)),
            pl.BlockSpec((16, 128), lambda i: (0, 0)),
            pl.BlockSpec((1, 128), lambda i: (0, 0)),
            pl.BlockSpec((8, 128), lambda i: (0, 0)),
        ],
        out_specs=[
            pl.BlockSpec((1, 1024, 128), row),
            pl.BlockSpec((1, 1024, 128), row),
            pl.BlockSpec((1, 4, 48, 1024), lambda i: (i, 0, 0, 0)),
            pl.BlockSpec((1, 1024, 128), row),
            pl.BlockSpec((PLANES, 8, 128), lambda i: (0, 0, 0)),
        ],
        out_shape=[
            jax.ShapeDtypeStruct((8, 1024, 128), BF),
            jax.ShapeDtypeStruct((8, 1024, 128), BF),
            jax.ShapeDtypeStruct((8, 4, 48, 1024), BF),
            jax.ShapeDtypeStruct((8, 1024, 128), BF),
            jax.ShapeDtypeStruct((PLANES, 8, 128), BF),
        ],
        scratch_shapes=[pltpu.VMEM((PLANES, 8, 128), F32), pltpu.VMEM((4, 128, 256), BF)],
        compiler_params=pltpu.CompilerParams(vmem_limit_bytes=48 * 2**20),
        name="tri_pre",
    )(z, gain.reshape(1, 128), proj, bwt, gate_bias.reshape(1, 128), mask_tile)


def trans_kernel(z_ref, gain_ref, w1_ref, b1_ref, w2_ref, out_ref, flag_ref):
    z = z_ref[0].astype(F32)

    @pl.when(pl.program_id(0) == 0)
    def _():
        flag_ref[...] = jnp.zeros((8, 128), F32)

    off = jnp.where(jnp.abs(z[0:16]) < 1e30, 0.0, 1.0)
    flag_ref[...] = jnp.maximum(flag_ref[...], jnp.maximum(off[0:8], off[8:16]))
    a = layer_norm(z, gain_ref[...])
    hid = jax.nn.relu(jnp.dot(a, w1_ref[...], preferred_element_type=F32) + b1_ref[...]).astype(BF)
    out_ref[0] = (z + jnp.dot(hid, w2_ref[...], preferred_element_type=F32)).astype(BF)


def trans(z, gain, w1, b1, w2):
    row = lambda i: (i, 0, 0)
    whole = lambda i: (0, 0)
    return pl.pallas_call(
        trans_kernel,
        grid=(8,),
        in_specs=[
            pl.BlockSpec((1, 1024, 128), row),
            pl.BlockSpec((1, 128), whole),
            pl.BlockSpec((128, 512), whole),
            pl.BlockSpec((1, 512), whole),
            pl.BlockSpec((512, 128), whole),
        ],
        out_specs=[pl.BlockSpec((1, 1024, 128), row), pl.BlockSpec((8, 128), whole)],
        out_shape=[jax.ShapeDtypeStruct((8, 1024, 128), BF), jax.ShapeDtypeStruct((8, 128), F32)],
        compiler_params=pltpu.CompilerParams(vmem_limit_bytes=48 * 2**20),
        name="tri_trans",
    )(z, gain.reshape(1, 128), w1, b1.reshape(1, 512), w2)


def exact_phase(z, mask, gain, proj, gate_bias, bias_w, out_w):
    key_bias = (mask - 1.0) * big_negative

    def before(row):
        a = layer_norm(row.astype(F32), gain)
        b = jnp.dot(a, bias_w, preferred_element_type=F32).astype(BF)
        return jnp.dot(a, proj, preferred_element_type=F32), jnp.transpose(b)

    p, b = lax.map(before, z)
    q, k, v = [jnp.moveaxis(p[..., 128 * n:128 * n + 128].astype(BF).reshape(8, 1024, 4, 32), 2, 0) for n in range(3)]

    def per_head(ops):
        qh, kh, vh, bh = ops
        eighths = jnp.swapaxes(bh.reshape(8, 8, 128), 0, 1)
        bias = lax.map(lambda c: lax.all_gather(c, AX, axis=0, tiled=True), eighths)
        bias = jnp.swapaxes(bias, 0, 1).reshape(1024, 1024).astype(F32)

        def per_row(rows):
            qr, kr, vr = rows
            s = jnp.dot(qr, kr.T, preferred_element_type=F32) * HEAD_DIM ** -0.5 + bias + key_bias
            return jnp.dot(jax.nn.softmax(s, axis=-1), vr.astype(F32), preferred_element_type=F32)

        return lax.map(per_row, (qh, kh, vh))

    o = jnp.moveaxis(lax.map(per_head, (q, k, v, jnp.swapaxes(b, 0, 1))), 0, 2).reshape(8, 1024, 128)

    def after(ops):
        row, mixed, logit = ops
        gated = (mixed * jax.nn.sigmoid(logit + gate_bias)).astype(BF)
        return (row.astype(F32) + jnp.dot(gated, out_w, preferred_element_type=F32)).astype(BF)

    z = lax.map(after, (z, o, p[..., 384:]))
    z = lax.all_to_all(z, AX, split_axis=1, concat_axis=0, tiled=True)
    return jnp.swapaxes(z, 0, 1)


def exact(z, mask_local, phases, last):
    mask = lax.all_gather(mask_local.astype(F32), AX, axis=0, tiled=True)
    stacked = [jnp.stack(pair) for pair in zip(*phases)]
    z, _ = lax.scan(lambda z, ws: (exact_phase(z, mask, *ws), None), z, stacked)
    return trans(z, *last)[0]


def phase(z, mask_tile, collective_id, gain, proj, gate_bias, bias_w, out_w):
    q, k, vt, gate, piece = pre(z, gain, proj, bias_w, gate_bias, mask_tile)
    return attention(piece, out_w, q, k, vt, gate, z, collective_id)


def local(
    pair_in,
    residue_mask,
    norm_start,
    proj_start,
    gate_bias_start,
    bias_w_start,
    out_w_start,
    norm_end,
    proj_end,
    gate_bias_end,
    bias_w_end,
    out_w_end,
    norm_trans,
    trans_in,
    trans_bias,
    trans_out,
):
    device = lax.axis_index("gx") * 8 + lax.axis_index("gy")
    lane = lax.broadcasted_iota(jnp.int32, (8, 128), 1)
    row = lax.broadcasted_iota(jnp.int32, (8, 128), 0)
    spread = jnp.tile(residue_mask.astype(F32), 16).reshape(1, 128)
    mask_tile = jnp.where((lane // 8 == lax.rem(device, 16)) & (row == 0), spread, 0.0)
    start = (norm_start, proj_start, gate_bias_start, bias_w_start, out_w_start)
    end = (norm_end, proj_end, gate_bias_end, bias_w_end, out_w_end)
    z = phase(pair_in, mask_tile, 0, *start)
    z = phase(z, mask_tile, 1, *end)
    last = (norm_trans, trans_in, trans_bias, trans_out)
    out, flag = trans(z, *last)
    return lax.cond(jnp.max(flag) == 0.0, lambda: out, lambda: exact(pair_in, residue_mask, (start, end), last))


def solution(mesh):
    rows = P(AX, None, None)
    placed = (rows, P(AX)) + (P(),) * 14

    def whole(*args):
        with jax.sharding.use_abstract_mesh(mesh.abstract_mesh):
            return jax.shard_map(local, mesh=mesh, in_specs=placed, out_specs=rows, check_vma=False)(*args)

    return whole
```

```python
import jax
import jax.numpy as jnp
from jax import lax
from jax.experimental import pallas as pl
from jax.experimental.pallas import tpu as pltpu
from jax.sharding import PartitionSpec as P

F32 = jnp.float32
BF = jnp.bfloat16
AX = ("gx", "gy")
HEADS = 4
HEAD_DIM = 32
LOG2E = 1.4426950408889634
LN2 = 0.6931471805599453
big_negative = 1000000000.0


MESH_ID = pl.DeviceIdType.MESH
ORDERS = ((0, 1, 2), (1, 2, 0), (2, 0, 1))
EXTRA = 26
PLANES = 36
EARLY = 43


def plane(h, t):
    if isinstance(t, int):
        return 12 * (t // 3) + 3 * h + t % 3
    return 12 * (t // 3) + 3 * h + lax.rem(t, 3)


class Torus:
    def __init__(self, piece_ref, full, send_sem, recv_sem):
        gx, gy = lax.axis_index("gx"), lax.axis_index("gy")
        self.core = lax.rem(gx, 2)
        self.here = (lax.rem(gx // 2, 4), gy // 2, lax.rem(gy, 2) * 2 + gx // 8)
        self.piece, self.full, self.send_sem, self.recv_sem = piece_ref, full, send_sem, recv_sem
        self.partner = self.device(self.here, 1 - self.core)
        self.sent = []

    def device(self, pos, c):
        px, py, pz = pos
        return ((lax.rem(pz, 2) * 4 + px) * 2 + c, py * 2 + pz // 2)

    def moved(self, dim, step):
        pos = list(self.here)
        pos[dim] = lax.rem(pos[dim] + step, 4)
        return tuple(pos)

    def region(self, lo, n, pos, done, other=False):
        px, py, pz = pos
        zl = slice(None) if 2 in done else lax.rem(pz, 2)
        zh = slice(None) if 2 in done else pz // 2
        xi = slice(None) if 0 in done else px
        yi = slice(None) if 1 in done else py
        return self.full.at[pl.ds(lo, n), zl, xi, 1 - self.core if other else self.core, yi, zh]

    def send(self, slot, lo, n, pos, done, dev, first=False):
        spot = self.region(lo, n, pos, done)
        pltpu.make_async_remote_copy(
            src_ref=self.piece.at[pl.ds(lo, n)] if first else spot, dst_ref=spot, send_sem=self.send_sem.at[slot],
            recv_sem=self.recv_sem.at[slot], device_id=dev, device_id_type=MESH_ID).start()

    def wait(self, slot, lo, n, pos, done, other=False, sent=False):
        spot = self.region(lo, n, pos, done, other)
        c = pltpu.make_async_remote_copy(
            src_ref=spot, dst_ref=spot, send_sem=self.send_sem.at[slot], recv_sem=self.recv_sem.at[slot],
            device_id=self.partner, device_id_type=MESH_ID)
        c.wait_send() if sent else c.wait_recv()

    def barrier(self):
        barrier = pltpu.get_barrier_semaphore()
        peers = [self.device(self.moved(d, s), self.core) for d in range(3) for s in (1, 3)] + [self.partner]
        for peer in peers:
            pl.semaphore_signal(barrier, inc=1, device_id=peer, device_id_type=MESH_ID)
        px, py, pz = self.here
        self.full[:, lax.rem(pz, 2), px, self.core, py, pz // 2] = self.piece[...]
        pl.semaphore_wait(barrier, 7)

    def outward(self, base, o, stage, lo, n):
        dim, done = ORDERS[o][stage], ORDERS[o][:stage]
        self.send(base, lo, n, self.here, done, self.device(self.moved(dim, 1), self.core), stage == 0)
        self.send(base + 1, lo, n, self.here, done, self.device(self.moved(dim, 3), self.core), stage == 0)

    def onward(self, base, o, stage, lo, n, n1):
        dim, done = ORDERS[o][stage], ORDERS[o][:stage]
        left, right = self.moved(dim, 3), self.moved(dim, 1)
        self.wait(base, lo, n, left, done)
        self.send(base + 2, lo, n1, left, done, self.device(right, self.core))
        self.wait(base + 1, lo, n, right, done)
        self.send(base + 3, lo + n1, n - n1, right, done, self.device(left, self.core))
        self.send(base + 4, lo, n, left, done, self.partner)
        self.send(base + 5, lo, n, right, done, self.partner)

    def closing(self, base, o, stage, lo, n, n1):
        dim, done = ORDERS[o][stage], ORDERS[o][:stage]
        far = self.moved(dim, 2)
        self.wait(base + 2, lo, n1, far, done)
        self.wait(base + 3, lo + n1, n - n1, far, done)
        self.send(base + 6, lo, n, far, done, self.partner)

    def shared(self, base, o, stage, lo, n):
        dim, done = ORDERS[o][stage], ORDERS[o][:stage]
        for k, step in ((4, 3), (5, 1), (6, 2)):
            self.wait(base + k, lo, n, self.moved(dim, step), done, True)

    def settled(self, base, o, stage, lo, n, n1):
        done = ORDERS[o][:stage]
        for k, size in ((0, n), (1, n), (2, n1), (3, n - n1), (4, n), (5, n), (6, n)):
            self.wait(base + k, lo, size, self.here, done, False, True)

    def early(self):
        for stage in range(2):
            bases = [21 * stage + 7 * o for o in range(3)]
            for o in range(3):
                self.outward(bases[o], o, stage, 12 * o, 12)
            if stage == 0:
                self.send(42, 0, PLANES, self.here, (), self.partner, True)
            for o in range(3):
                self.onward(bases[o], o, stage, 12 * o, 12, 6)
            for o in range(3):
                self.closing(bases[o], o, stage, 12 * o, 12, 6)

    def sizes(self, first):
        return ((3, 2), (3, 1), (3, 1) if first else (2, 1))

    def late(self, action, h, first=False):
        for o, (n, n1) in enumerate(self.sizes(first)):
            base, lo = EARLY + 21 * h + 7 * o, 12 * o + 3 * h
            if action in ("outward", "shared"):
                getattr(self, action)(base, o, 2, lo, n)
            else:
                getattr(self, action)(base, o, 2, lo, n, n1)

    def early_shared(self):
        self.wait(42, 0, PLANES, self.here, (), True)
        for stage in range(2):
            for o in range(3):
                self.shared(21 * stage + 7 * o, o, stage, 12 * o, 12)

    def finish(self):
        self.wait(42, 0, PLANES, self.here, (), False, True)
        for stage in range(2):
            for o in range(3):
                self.settled(21 * stage + 7 * o, o, stage, 12 * o, 12, 6)
        for h in range(4):
            self.late("settled", h, h == 0)


def attn_setup(q_ref, qs, eye, slot):
    lane = lax.broadcasted_iota(jnp.int32, (16, 128), 1) // 32
    for s in range(4):
        slot[s] = jnp.where(lane == s, 1.0, 0.0).astype(BF)
    rowi = lax.broadcasted_iota(jnp.int32, (128, 128), 0)
    coli = lax.broadcasted_iota(jnp.int32, (128, 128), 1)
    eye[...] = jnp.where(rowi == coli, 1.0, 0.0).astype(BF)

    def stack(n, _):
        at = pl.ds(pl.multiple_of(n * 128, 128), 128)
        for g in range(2):
            rows = [q_ref[4 * g + r, at, :] for r in range(4)]
            for h in range(4):
                s = None
                for r in range(4):
                    t = rows[r] * jnp.concatenate([slot[(h + r) % 4]] * 8, axis=0)
                    s = t if s is None else s + t
                qs[2 * h + g, at, :] = s
        return 0

    lax.fori_loop(0, 8, stack, 0)


def attn_mask(extra, mask_ref):
    placed = jnp.sum(extra.astype(F32).reshape(8, 16, 8, 128), axis=1)
    for t in range(8):
        mask_ref[:, t * 128:(t + 1) * 128] = jnp.broadcast_to(placed[t, 0:1, :], (16, 128)).astype(BF)


def attn_split(it):
    group = it // 4
    late = group >= 8
    head = jnp.where(late, lax.rem(group, 4), group // 2)
    quarter = jnp.where(late, group // 4, lax.rem(group, 2))
    return head, quarter, lax.rem(it, 4)


def attn_loop(first, last, comm, k_ref, vt_ref, b_ref, o_ref, qs, eye, slot, ps, mask_ref, sacc, oacc):
    def push_qb(it, odd):
        h, qp, kp = attn_split(it)
        core, zl = qp // 2, lax.rem(qp, 2)
        bias = b_ref[plane(h, 2 * kp + odd), zl, :, core].reshape(256, 128)
        for m in range(2):
            rhs = jnp.concatenate([qs[2 * h + m, zl, :, core].reshape(256, 128), bias], axis=1)
            pltpu.matmul_push_rhs(rhs, 0, m, transpose=True)

    def pop_scores(par, odd, r, n):
        for m in range(2):
            ps[2 * par + m][r, odd * 128:odd * 128 + 128, :] = jnp.exp2(pltpu.matmul_pop(sacc[m][n]).astype(BF))

    def push_p(par, r):
        for m in range(2):
            pltpu.matmul_push_rhs(ps[2 * par + m][r], 1, m)

    def pv(it, r):
        h, _, kp = attn_split(it)
        at = pl.ds(pl.multiple_of(kp * 256, 256), 256)
        keep = jnp.concatenate([mask_ref[:, at]] * 3, axis=0)
        for m in range(2):
            pltpu.matmul_acc_lhs(oacc[m][r], vt_ref[4 * m + r, h, :, at] * keep, 1)

    def result(it):
        h, qp, _ = attn_split(it)
        at = pl.ds(pl.multiple_of(qp * 256, 256), 256)
        for r in range(4):
            for m in range(2):
                o = pltpu.matmul_pop(oacc[m][r])
                d = o[32:33, :]
                fine = (d > 2.0 ** -60) & (d < 2.0 ** 100)
                o_ref[4 * m + r, pl.ds(pl.multiple_of(h * 32, 32), 32), at] = o[0:32, :] * jnp.where(fine, 1.0 / d, jnp.nan)

    def step(it, par):
        h, _, kp = attn_split(it)
        before = lax.max(it - 1, 0)
        for odd in range(2):
            for r in range(4):
                at = pl.ds(pl.multiple_of((2 * kp + odd) * 128, 128), 128)
                keep = jnp.concatenate([slot[lax.rem(h + r, 4)]] * 8, axis=0)
                if r >= 2:
                    pop_scores(1 - par if odd == 0 else par, 1 - odd, r, r)
                for m in range(2):
                    lhs = jnp.concatenate([k_ref[4 * m + r, at, :] * keep, eye[...]], axis=1)
                    pltpu.matmul_acc_lhs(sacc[m][r], lhs, 0 if r == 0 else None)
                if r == 0:
                    if odd == 0:
                        push_qb(it, 1)
                    else:
                        push_qb(lax.min(it + 1, 63), 0)
                    push_p(1 - par, 2 * odd)
            pv(before, 2 * odd)
            push_p(1 - par, 2 * odd + 1)
            pv(before, 2 * odd + 1)
            for r in range(2):
                pop_scores(par, odd, r, r)

    def body(pair, _):
        step(2 * pair, 0)
        comm(pair + 1)

        @pl.when(lax.rem(pair, 2) == 0)
        def _():
            result(lax.max(2 * pair - 4, 0))

        step(2 * pair + 1, 1)
        return 0

    if first == 0:
        push_qb(0, 0)
    lax.fori_loop(first // 2, last // 2, body, 0)
    if last < 64:
        return
    par = (last - 1) % 2
    zero = jnp.zeros((128, 256), BF)
    for r in (2, 3):
        pop_scores(par, 1, r, r)
    for m in range(2):
        pltpu.matmul_acc_lhs(sacc[m][0], zero, 0)
        pltpu.matmul_pop(sacc[m][0])
    for r in range(4):
        push_p(par, r)
        pv(last - 1, r)
    result(last - 1)


def attn_kernel(piece_ref, w_ref, q_hbm, k_hbm, vt_hbm, gate_hbm, z_hbm, out_hbm, full, q_ref, k_ref, vt_ref, gate_ref, z_ref, qs, eye, slot, ps0, ps1, ps2, ps3, mask_ref, o_ref, wide, scr, outgoing, landed, note, notes, bad, send_sem, recv_sem, load_sem, push_sem, land_sem, note_send, note_recv, out_sem):
    ps = (ps0, ps1, ps2, ps3)
    gx, gy = lax.axis_index("gx"), lax.axis_index("gy")
    me = gx * 8 + gy
    pairs = ((q_hbm, q_ref), (k_hbm, k_ref), (vt_hbm, vt_ref), (gate_hbm, gate_ref), (z_hbm, z_ref))
    loads = [pltpu.make_async_copy(a, b, load_sem.at[n]) for n, (a, b) in enumerate(pairs)]
    for c in loads:
        c.start()
    torus = Torus(piece_ref, full, send_sem, recv_sem)
    torus.barrier()
    torus.early()
    torus.late("outward", 0, True)
    torus.late("outward", 1)
    for c in loads:
        c.wait()
    attn_setup(q_ref, qs, eye, slot)
    wide[...] = jnp.zeros((256, 256), BF)
    wide[0:128, 0:128] = w_ref[...]
    wide[128:256, 128:256] = w_ref[...]
    bad[...] = jnp.zeros((8, 128), F32)
    torus.late("onward", 0, True)
    torus.late("outward", 2)
    torus.late("onward", 1)
    torus.late("outward", 3)
    torus.late("closing", 0, True)
    torus.early_shared()
    torus.late("shared", 0, True)
    attn_mask(full.reshape(PLANES, 1024, 128)[EXTRA], mask_ref)
    b_ref = full.reshape(PLANES, 2, 4, 2, 64, 128)
    qs_by = qs.reshape(8, 2, 4, 2, 64, 128)
    gate_by = gate_ref.reshape(8, 2, 4, 2, 64, 128)
    z_by = z_ref.reshape(8, 2, 4, 2, 64, 128)

    def owner(n):
        quarter, x, low = n // 32, lax.rem(n // 8, 4), lax.rem(n, 8)
        return (lax.rem(quarter, 2) * 8 + x * 2 + quarter // 2) * 8 + low

    my_block = (lax.rem(gx, 2) * 2 + gx // 8) * 32 + lax.rem(gx // 2, 4) * 8 + gy

    def block(n):
        dest = owner(n)
        return pltpu.make_async_remote_copy(
            src_ref=outgoing.at[n], dst_ref=landed.at[:, me], send_sem=push_sem, recv_sem=land_sem,
            device_id=(dest // 8, lax.rem(dest, 8)), device_id_type=MESH_ID)

    def hand_over(t, sacc):
        at = pl.ds(pl.multiple_of(t * 128, 128), 128)
        core, zl, half = t // 4, lax.rem(t // 2, 2), pl.ds(2 * lax.rem(t, 2), 2)
        for m in range(2):
            pltpu.matmul_push_rhs(wide[...], 1, m)
        for rp in range(4):
            parts = []
            for i in (2 * rp, 2 * rp + 1):
                parts.append((jnp.transpose(o_ref[i, :, at]) * gate_by[i, zl, half, core].reshape(128, 128).astype(F32)).astype(BF))
            pltpu.matmul_acc_lhs(sacc[rp % 2][rp // 2], jnp.concatenate(parts, axis=1), 1 if rp < 2 else None)
        worst = bad[...]
        for rp in range(4):
            y = pltpu.matmul_pop(sacc[rp % 2][rp // 2])
            for u in range(2):
                i = 2 * rp + u
                v = z_by[i, zl, half, core].reshape(128, 128).astype(F32) + y[:, 128 * u:128 * u + 128]
                scr[pl.ds(i, 128, stride=8), :] = v
                off = jnp.where(jnp.abs(v) < 1e30, 0.0, 1.0).reshape(16, 8, 128)
                worst = jnp.maximum(worst, jnp.max(off, axis=0))
        bad[...] = worst
        outgoing[pl.ds(pl.multiple_of(t * 16, 16), 16)] = scr[...].astype(BF).reshape(16, 8, 8, 128)

        def push(n, _):
            spot = t * 16 + lax.rem(me + n, 16)

            @pl.when(spot != my_block)
            def _():
                block(spot).start()

            return 0

        lax.fori_loop(0, 16, push, 0)

    specs = []
    for m in range(2):
        specs += [pltpu.ACC(m)((128, 256), F32)] * 4 + [pltpu.ACC(m)((48, 256), F32)] * 4

    def run(*accs):
        sacc = [accs[8 * m:8 * m + 4] for m in range(2)]
        oacc = [accs[8 * m + 4:8 * m + 8] for m in range(2)]

        def comm(pair):
            @pl.when(pair < 13)
            def _():
                @pl.when((pair == 1) | (pair == 3))
                def _():
                    torus.late("onward", (pair + 3) // 2)

                @pl.when(lax.rem(pair, 4) == 2)
                def _():
                    torus.late("closing", (pair + 2) // 4)

                @pl.when((pair > 0) & (lax.rem(pair, 4) == 0))
                def _():
                    torus.late("shared", pair // 4)

            @pl.when((pair >= 18) & (pair < 22))
            def _():
                hand_over(lax.rem(pair - 18 + gx // 2, 4), sacc)

            @pl.when((pair >= 26) & (pair < 28))
            def _():
                hand_over(4 + lax.rem(pair + gx // 2, 2), sacc)

        attn_loop(0, 64, comm, k_ref, vt_ref, b_ref, o_ref, qs_by, eye, slot, ps, mask_ref, sacc, oacc)

        def tail(t, _):
            hand_over(6 + lax.rem(t + gx // 2, 2), sacc)
            return 0

        lax.fori_loop(0, 2, tail, 0)

    pl.run_scoped(run, *specs)
    seen = jnp.max(bad[...], axis=(0, 1), keepdims=True)
    note[...] = jnp.broadcast_to(seen, (8, 128))
    landed[:, me] = outgoing[my_block]
    notes[me] = note[...]

    def tell(dest):
        return pltpu.make_async_remote_copy(
            src_ref=note, dst_ref=notes.at[me], send_sem=note_send, recv_sem=note_recv,
            device_id=(dest // 8, lax.rem(dest, 8)), device_id_type=MESH_ID)

    def spread(n, _):
        tell(lax.rem(me + n, 128)).start()
        return 0

    lax.fori_loop(1, 128, spread, 0)
    torus.finish()
    neighbour = dict(device_id=(lax.rem(gx + 1, 16), gy), device_id_type=MESH_ID)
    blocks = pltpu.make_async_remote_copy(
        src_ref=outgoing.at[0:127], dst_ref=landed.at[:, 0:127], send_sem=push_sem, recv_sem=land_sem, **neighbour)
    all_notes = pltpu.make_async_remote_copy(
        src_ref=notes.at[0:127], dst_ref=notes.at[0:127], send_sem=note_send, recv_sem=note_recv, **neighbour)
    blocks.wait_recv()
    all_notes.wait_recv()
    worst = jnp.max(notes[...], axis=0)
    landed[0, 0, 0:8] = jnp.where(worst > 0.0, jnp.nan, landed[0, 0, 0:8].astype(F32)).astype(BF)
    out = pltpu.make_async_copy(landed, out_hbm, out_sem)
    out.start()
    blocks.wait_send()
    all_notes.wait_send()
    out.wait()


def attention(piece, w, q, k, vt, gate, z, collective_id):
    vmem = pl.BlockSpec(memory_space=pltpu.VMEM)
    hbm = pl.BlockSpec(memory_space=pl.ANY)
    rows = pltpu.VMEM((8, 1024, 128), BF)
    out = pl.pallas_call(
        attn_kernel,
        in_specs=[vmem, vmem] + [hbm] * 5,
        out_specs=hbm,
        out_shape=jax.ShapeDtypeStruct((8, 128, 8, 128), BF),
        scratch_shapes=[
            pltpu.VMEM((PLANES, 2, 4, 2, 4, 2, 8, 128), BF),
            rows,
            rows,
            pltpu.VMEM((8, 4, 48, 1024), BF),
            rows,
            rows,
            rows,
            pltpu.VMEM((128, 128), BF),
            pltpu.VMEM((4, 16, 128), BF),
            *[pltpu.VMEM((4, 256, 256), BF)] * 4,
            pltpu.VMEM((16, 1024), BF),
            pltpu.VMEM((8, 128, 1024), F32),
            pltpu.VMEM((256, 256), BF),
            pltpu.VMEM((1024, 128), F32),
            pltpu.VMEM((128, 8, 8, 128), BF),
            pltpu.VMEM((8, 128, 8, 128), BF),
            pltpu.VMEM((8, 128), F32),
            pltpu.VMEM((128, 8, 128), F32),
            pltpu.VMEM((8, 128), F32),
            pltpu.SemaphoreType.DMA((EARLY + 84,)),
            pltpu.SemaphoreType.DMA((EARLY + 84,)),
            pltpu.SemaphoreType.DMA((5,)),
            *[pltpu.SemaphoreType.DMA] * 5,
        ],
        compiler_params=pltpu.CompilerParams(collective_id=collective_id, has_side_effects=True, vmem_limit_bytes=48 * 2**20),
        name="tri_attn",
    )(piece, w, q, k, vt, gate, z)
    return out.reshape(8, 1024, 128)


def layer_norm(x, gain):
    mean = jnp.mean(x, axis=-1, keepdims=True)
    c = x - mean
    var = jnp.mean(c * c, axis=-1, keepdims=True)
    return (c * lax.rsqrt(var + 1e-05) * gain).astype(BF)


def pre_kernel(z_ref, gain_ref, proj_ref, bw_ref, gb_ref, mask_ref, q_ref, k_ref, vt_ref, gate_ref, b_ref, scr, wqk):
    i = pl.program_id(0)

    @pl.when(i == 0)
    def _():
        for s in range(4):
            for n in range(2):
                w = proj_ref[:, 128 * n:128 * n + 128].astype(F32)
                wqk[s, :, 128 * n:128 * n + 128] = (pltpu.roll(w, 32 * s, 1) if s else w).astype(BF)
        scr[...] = jnp.zeros((PLANES, 8, 128), F32)
        scr[EXTRA] = mask_ref[...]

    a = layer_norm(z_ref[0].astype(F32), gain_ref[...])
    qk = jnp.dot(a, wqk[lax.rem(i, 4)], preferred_element_type=F32)
    q_ref[0] = (qk[:, :128] * (HEAD_DIM ** -0.5 * LOG2E)).astype(BF)
    k_ref[0] = qk[:, 128:].astype(BF)
    vg = jnp.dot(a, proj_ref[:, 256:512], preferred_element_type=F32)
    vt = jnp.transpose(vg[:, :128].astype(BF))
    tail = jnp.where(lax.broadcasted_iota(jnp.int32, (16, 1024), 0) == 0, 1.0, 0.0).astype(BF)
    for h in range(4):
        vt_ref[0, h, 0:32, :] = vt[32 * h:32 * h + 32, :]
        vt_ref[0, h, 32:48, :] = tail
    gate_ref[0] = jax.nn.sigmoid(vg[:, 128:] + gb_ref[...]).astype(BF)
    b = lax.dot_general(bw_ref[...], a, (((1,), (1,)), ((), ())), preferred_element_type=F32)
    b = b.astype(BF).astype(F32)
    m = jnp.max(b, axis=-1, keepdims=True)
    b = (b - m) * LOG2E
    for h in range(4):
        for kt in range(8):
            scr[plane(h, kt), pl.ds(i, 1), :] = b[h:h + 1, kt * 128:(kt + 1) * 128]
    lane = lax.broadcasted_iota(jnp.int32, (4, 128), 1)
    scr[EXTRA, 1:5, :] = jnp.where(lane == i, m[0:4], scr[EXTRA, 1:5, :])

    @pl.when(i == 7)
    def _():
        b_ref[...] = scr[...].astype(BF)


def pre(z, gain, proj, bias_w, gate_bias, mask_tile):
    bwt = jnp.pad(jnp.transpose(bias_w), ((0, 12), (0, 0)))
    row = lambda i: (i, 0, 0)
    return pl.pallas_call(
        pre_kernel,
        grid=(8,),
        in_specs=[
            pl.BlockSpec((1, 1024, 128), row),
            pl.BlockSpec((1, 128), lambda i: (0, 0)),
            pl.BlockSpec((128, 512), lambda i: (0, 0)),
            pl.BlockSpec((16, 128), lambda i: (0, 0)),
            pl.BlockSpec((1, 128), lambda i: (0, 0)),
            pl.BlockSpec((8, 128), lambda i: (0, 0)),
        ],
        out_specs=[
            pl.BlockSpec((1, 1024, 128), row),
            pl.BlockSpec((1, 1024, 128), row),
            pl.BlockSpec((1, 4, 48, 1024), lambda i: (i, 0, 0, 0)),
            pl.BlockSpec((1, 1024, 128), row),
            pl.BlockSpec((PLANES, 8, 128), lambda i: (0, 0, 0)),
        ],
        out_shape=[
            jax.ShapeDtypeStruct((8, 1024, 128), BF),
            jax.ShapeDtypeStruct((8, 1024, 128), BF),
            jax.ShapeDtypeStruct((8, 4, 48, 1024), BF),
            jax.ShapeDtypeStruct((8, 1024, 128), BF),
            jax.ShapeDtypeStruct((PLANES, 8, 128), BF),
        ],
        scratch_shapes=[pltpu.VMEM((PLANES, 8, 128), F32), pltpu.VMEM((4, 128, 256), BF)],
        compiler_params=pltpu.CompilerParams(vmem_limit_bytes=48 * 2**20),
        name="tri_pre",
    )(z, gain.reshape(1, 128), proj, bwt, gate_bias.reshape(1, 128), mask_tile)


def trans_kernel(z_ref, gain_ref, w1_ref, b1_ref, w2_ref, out_ref, flag_ref):
    z = z_ref[0].astype(F32)

    @pl.when(pl.program_id(0) == 0)
    def _():
        flag_ref[...] = jnp.zeros((8, 128), F32)

    off = jnp.where(jnp.abs(z[0:16]) < 1e30, 0.0, 1.0)
    flag_ref[...] = jnp.maximum(flag_ref[...], jnp.maximum(off[0:8], off[8:16]))
    a = layer_norm(z, gain_ref[...])
    hid = jax.nn.relu(jnp.dot(a, w1_ref[...], preferred_element_type=F32) + b1_ref[...]).astype(BF)
    out_ref[0] = (z + jnp.dot(hid, w2_ref[...], preferred_element_type=F32)).astype(BF)


def trans(z, gain, w1, b1, w2):
    row = lambda i: (i, 0, 0)
    whole = lambda i: (0, 0)
    return pl.pallas_call(
        trans_kernel,
        grid=(8,),
        in_specs=[
            pl.BlockSpec((1, 1024, 128), row),
            pl.BlockSpec((1, 128), whole),
            pl.BlockSpec((128, 512), whole),
            pl.BlockSpec((1, 512), whole),
            pl.BlockSpec((512, 128), whole),
        ],
        out_specs=[pl.BlockSpec((1, 1024, 128), row), pl.BlockSpec((8, 128), whole)],
        out_shape=[jax.ShapeDtypeStruct((8, 1024, 128), BF), jax.ShapeDtypeStruct((8, 128), F32)],
        compiler_params=pltpu.CompilerParams(vmem_limit_bytes=48 * 2**20),
        name="tri_trans",
    )(z, gain.reshape(1, 128), w1, b1.reshape(1, 512), w2)


def exact_phase(z, mask, gain, proj, gate_bias, bias_w, out_w):
    key_bias = (mask - 1.0) * big_negative

    def before(row):
        a = layer_norm(row.astype(F32), gain)
        b = jnp.dot(a, bias_w, preferred_element_type=F32).astype(BF)
        return jnp.dot(a, proj, preferred_element_type=F32), jnp.transpose(b)

    p, b = lax.map(before, z)
    q, k, v = [jnp.moveaxis(p[..., 128 * n:128 * n + 128].astype(BF).reshape(8, 1024, 4, 32), 2, 0) for n in range(3)]

    def per_head(ops):
        qh, kh, vh, bh = ops
        eighths = jnp.swapaxes(bh.reshape(8, 8, 128), 0, 1)
        bias = lax.map(lambda c: lax.all_gather(c, AX, axis=0, tiled=True), eighths)
        bias = jnp.swapaxes(bias, 0, 1).reshape(1024, 1024).astype(F32)

        def per_row(rows):
            qr, kr, vr = rows
            s = jnp.dot(qr, kr.T, preferred_element_type=F32) * HEAD_DIM ** -0.5 + bias + key_bias
            return jnp.dot(jax.nn.softmax(s, axis=-1), vr.astype(F32), preferred_element_type=F32)

        return lax.map(per_row, (qh, kh, vh))

    o = jnp.moveaxis(lax.map(per_head, (q, k, v, jnp.swapaxes(b, 0, 1))), 0, 2).reshape(8, 1024, 128)

    def after(ops):
        row, mixed, logit = ops
        gated = (mixed * jax.nn.sigmoid(logit + gate_bias)).astype(BF)
        return (row.astype(F32) + jnp.dot(gated, out_w, preferred_element_type=F32)).astype(BF)

    z = lax.map(after, (z, o, p[..., 384:]))
    z = lax.all_to_all(z, AX, split_axis=1, concat_axis=0, tiled=True)
    return jnp.swapaxes(z, 0, 1)


def exact(z, mask_local, phases, last):
    mask = lax.all_gather(mask_local.astype(F32), AX, axis=0, tiled=True)
    stacked = [jnp.stack(pair) for pair in zip(*phases)]
    z, _ = lax.scan(lambda z, ws: (exact_phase(z, mask, *ws), None), z, stacked)
    return trans(z, *last)[0]


def phase(z, mask_tile, collective_id, gain, proj, gate_bias, bias_w, out_w):
    q, k, vt, gate, piece = pre(z, gain, proj, bias_w, gate_bias, mask_tile)
    return attention(piece, out_w, q, k, vt, gate, z, collective_id)


def local(
    pair_in,
    residue_mask,
    norm_start,
    proj_start,
    gate_bias_start,
    bias_w_start,
    out_w_start,
    norm_end,
    proj_end,
    gate_bias_end,
    bias_w_end,
    out_w_end,
    norm_trans,
    trans_in,
    trans_bias,
    trans_out,
):
    device = lax.axis_index("gx") * 8 + lax.axis_index("gy")
    lane = lax.broadcasted_iota(jnp.int32, (8, 128), 1)
    row = lax.broadcasted_iota(jnp.int32, (8, 128), 0)
    spread = jnp.tile(residue_mask.astype(F32), 16).reshape(1, 128)
    mask_tile = jnp.where((lane // 8 == lax.rem(device, 16)) & (row == 0), spread, 0.0)
    start = (norm_start, proj_start, gate_bias_start, bias_w_start, out_w_start)
    end = (norm_end, proj_end, gate_bias_end, bias_w_end, out_w_end)
    z = phase(pair_in, mask_tile, 0, *start)
    z = phase(z, mask_tile, 1, *end)
    last = (norm_trans, trans_in, trans_bias, trans_out)
    out, flag = trans(z, *last)
    return lax.cond(jnp.max(flag) == 0.0, lambda: out, lambda: exact(pair_in, residue_mask, (start, end), last))


def solution(mesh):
    rows = P(AX, None, None)
    placed = (rows, P(AX)) + (P(),) * 14

    def whole(*args):
        with jax.sharding.use_abstract_mesh(mesh.abstract_mesh):
            return jax.shard_map(local, mesh=mesh, in_specs=placed, out_specs=rows, check_vma=False)(*args)

    return whole
```

```python
import jax
import jax.numpy as jnp
from jax import lax
from jax.experimental import pallas as pl
from jax.experimental.pallas import tpu as pltpu
from jax.sharding import PartitionSpec as P

F32 = jnp.float32
BF = jnp.bfloat16
AX = ("gx", "gy")
HEADS = 4
HEAD_DIM = 32
LOG2E = 1.4426950408889634
LN2 = 0.6931471805599453
big_negative = 1000000000.0


MESH_ID = pl.DeviceIdType.MESH
ORDERS = ((0, 1, 2), (1, 2, 0), (2, 0, 1))
EXTRA = 26
PLANES = 36
EARLY = 43


def plane(h, t):
    if isinstance(t, int):
        return 12 * (t // 3) + 3 * h + t % 3
    return 12 * (t // 3) + 3 * h + lax.rem(t, 3)


class Torus:
    def __init__(self, piece_ref, full, send_sem, recv_sem):
        gx, gy = lax.axis_index("gx"), lax.axis_index("gy")
        self.core = lax.rem(gx, 2)
        self.here = (lax.rem(gx // 2, 4), gy // 2, lax.rem(gy, 2) * 2 + gx // 8)
        self.piece, self.full, self.send_sem, self.recv_sem = piece_ref, full, send_sem, recv_sem
        self.partner = self.device(self.here, 1 - self.core)
        self.sent = []

    def device(self, pos, c):
        px, py, pz = pos
        return ((lax.rem(pz, 2) * 4 + px) * 2 + c, py * 2 + pz // 2)

    def moved(self, dim, step):
        pos = list(self.here)
        pos[dim] = lax.rem(pos[dim] + step, 4)
        return tuple(pos)

    def region(self, lo, n, pos, done, other=False):
        px, py, pz = pos
        zl = slice(None) if 2 in done else lax.rem(pz, 2)
        zh = slice(None) if 2 in done else pz // 2
        xi = slice(None) if 0 in done else px
        yi = slice(None) if 1 in done else py
        return self.full.at[pl.ds(lo, n), zl, xi, 1 - self.core if other else self.core, yi, zh]

    def send(self, slot, lo, n, pos, done, dev, first=False):
        spot = self.region(lo, n, pos, done)
        pltpu.make_async_remote_copy(
            src_ref=self.piece.at[pl.ds(lo, n)] if first else spot, dst_ref=spot, send_sem=self.send_sem.at[slot],
            recv_sem=self.recv_sem.at[slot], device_id=dev, device_id_type=MESH_ID).start()

    def wait(self, slot, lo, n, pos, done, other=False, sent=False):
        spot = self.region(lo, n, pos, done, other)
        c = pltpu.make_async_remote_copy(
            src_ref=spot, dst_ref=spot, send_sem=self.send_sem.at[slot], recv_sem=self.recv_sem.at[slot],
            device_id=self.partner, device_id_type=MESH_ID)
        c.wait_send() if sent else c.wait_recv()

    def barrier(self):
        barrier = pltpu.get_barrier_semaphore()
        peers = [self.device(self.moved(d, s), self.core) for d in range(3) for s in (1, 3)] + [self.partner]
        for peer in peers:
            pl.semaphore_signal(barrier, inc=1, device_id=peer, device_id_type=MESH_ID)
        px, py, pz = self.here
        self.full[:, lax.rem(pz, 2), px, self.core, py, pz // 2] = self.piece[...]
        pl.semaphore_wait(barrier, 7)

    def outward(self, base, o, stage, lo, n):
        dim, done = ORDERS[o][stage], ORDERS[o][:stage]
        self.send(base, lo, n, self.here, done, self.device(self.moved(dim, 1), self.core), stage == 0)
        self.send(base + 1, lo, n, self.here, done, self.device(self.moved(dim, 3), self.core), stage == 0)

    def onward(self, base, o, stage, lo, n, n1):
        dim, done = ORDERS[o][stage], ORDERS[o][:stage]
        left, right = self.moved(dim, 3), self.moved(dim, 1)
        self.wait(base, lo, n, left, done)
        self.send(base + 2, lo, n1, left, done, self.device(right, self.core))
        self.wait(base + 1, lo, n, right, done)
        self.send(base + 3, lo + n1, n - n1, right, done, self.device(left, self.core))
        self.send(base + 4, lo, n, left, done, self.partner)
        self.send(base + 5, lo, n, right, done, self.partner)

    def closing(self, base, o, stage, lo, n, n1):
        dim, done = ORDERS[o][stage], ORDERS[o][:stage]
        far = self.moved(dim, 2)
        self.wait(base + 2, lo, n1, far, done)
        self.wait(base + 3, lo + n1, n - n1, far, done)
        self.send(base + 6, lo, n, far, done, self.partner)

    def shared(self, base, o, stage, lo, n):
        dim, done = ORDERS[o][stage], ORDERS[o][:stage]
        for k, step in ((4, 3), (5, 1), (6, 2)):
            self.wait(base + k, lo, n, self.moved(dim, step), done, True)

    def settled(self, base, o, stage, lo, n, n1):
        done = ORDERS[o][:stage]
        for k, size in ((0, n), (1, n), (2, n1), (3, n - n1), (4, n), (5, n), (6, n)):
            self.wait(base + k, lo, size, self.here, done, False, True)

    def early(self):
        for stage in range(2):
            bases = [21 * stage + 7 * o for o in range(3)]
            for o in range(3):
                self.outward(bases[o], o, stage, 12 * o, 12)
            if stage == 0:
                self.send(42, 0, PLANES, self.here, (), self.partner, True)
            for o in range(3):
                self.onward(bases[o], o, stage, 12 * o, 12, 6)
            for o in range(3):
                self.closing(bases[o], o, stage, 12 * o, 12, 6)

    def sizes(self, first):
        return ((3, 2), (3, 1), (3, 1) if first else (2, 1))

    def late(self, action, h, first=False):
        for o, (n, n1) in enumerate(self.sizes(first)):
            base, lo = EARLY + 21 * h + 7 * o, 12 * o + 3 * h
            if action in ("outward", "shared"):
                getattr(self, action)(base, o, 2, lo, n)
            else:
                getattr(self, action)(base, o, 2, lo, n, n1)

    def early_shared(self):
        self.wait(42, 0, PLANES, self.here, (), True)
        for stage in range(2):
            for o in range(3):
                self.shared(21 * stage + 7 * o, o, stage, 12 * o, 12)

    def finish(self):
        self.wait(42, 0, PLANES, self.here, (), False, True)
        for stage in range(2):
            for o in range(3):
                self.settled(21 * stage + 7 * o, o, stage, 12 * o, 12, 6)
        for h in range(4):
            self.late("settled", h, h == 0)


def attn_setup(q_ref, qs, eye, slot):
    lane = lax.broadcasted_iota(jnp.int32, (16, 128), 1) // 32
    for s in range(4):
        slot[s] = jnp.where(lane == s, 1.0, 0.0).astype(BF)
    rowi = lax.broadcasted_iota(jnp.int32, (128, 128), 0)
    coli = lax.broadcasted_iota(jnp.int32, (128, 128), 1)
    eye[...] = jnp.where(rowi == coli, 1.0, 0.0).astype(BF)

    def stack(n, _):
        at = pl.ds(pl.multiple_of(n * 128, 128), 128)
        for g in range(2):
            rows = [q_ref[4 * g + r, at, :] for r in range(4)]
            for h in range(4):
                s = None
                for r in range(4):
                    t = rows[r] * jnp.concatenate([slot[(h + r) % 4]] * 8, axis=0)
                    s = t if s is None else s + t
                qs[2 * h + g, at, :] = s
        return 0

    lax.fori_loop(0, 8, stack, 0)


def attn_mask(extra, mask_ref):
    placed = jnp.sum(extra.astype(F32).reshape(8, 16, 8, 128), axis=1)
    for t in range(8):
        mask_ref[:, t * 128:(t + 1) * 128] = jnp.broadcast_to(placed[t, 0:1, :], (16, 128)).astype(BF)


def attn_split(it):
    group = it // 4
    late = group >= 8
    head = jnp.where(late, lax.rem(group, 4), group // 2)
    quarter = jnp.where(late, group // 4, lax.rem(group, 2))
    return head, quarter, lax.rem(it, 4)


def attn_loop(first, last, comm, k_ref, vt_ref, b_ref, o_ref, qs, eye, slot, ps, mask_ref, sacc, oacc):
    def push_qb(it, odd):
        h, qp, kp = attn_split(it)
        core, zl = qp // 2, lax.rem(qp, 2)
        bias = b_ref[plane(h, 2 * kp + odd), zl, :, core].reshape(256, 128)
        for m in range(2):
            rhs = jnp.concatenate([qs[2 * h + m, zl, :, core].reshape(256, 128), bias], axis=1)
            pltpu.matmul_push_rhs(rhs, 0, m, transpose=True)

    def pop_scores(par, odd, r, n):
        for m in range(2):
            ps[2 * par + m][r, odd * 128:odd * 128 + 128, :] = jnp.exp2(pltpu.matmul_pop(sacc[m][n]).astype(BF))

    def push_p(par, r):
        for m in range(2):
            pltpu.matmul_push_rhs(ps[2 * par + m][r], 1, m)

    def pv(it, r):
        h, _, kp = attn_split(it)
        at = pl.ds(pl.multiple_of(kp * 256, 256), 256)
        keep = jnp.concatenate([mask_ref[:, at]] * 3, axis=0)
        for m in range(2):
            pltpu.matmul_acc_lhs(oacc[m][r], vt_ref[4 * m + r, h, :, at] * keep, 1)

    def result(it):
        h, qp, _ = attn_split(it)
        at = pl.ds(pl.multiple_of(qp * 256, 256), 256)
        for r in range(4):
            for m in range(2):
                o = pltpu.matmul_pop(oacc[m][r])
                d = o[32:33, :]
                fine = (d > 2.0 ** -60) & (d < 2.0 ** 100)
                o_ref[4 * m + r, pl.ds(pl.multiple_of(h * 32, 32), 32), at] = o[0:32, :] * jnp.where(fine, 1.0 / d, jnp.nan)

    def step(it, par):
        h, _, kp = attn_split(it)
        before = lax.max(it - 1, 0)
        for odd in range(2):
            for r in range(4):
                at = pl.ds(pl.multiple_of((2 * kp + odd) * 128, 128), 128)
                keep = jnp.concatenate([slot[lax.rem(h + r, 4)]] * 8, axis=0)
                if r >= 2:
                    pop_scores(1 - par if odd == 0 else par, 1 - odd, r, r)
                for m in range(2):
                    lhs = jnp.concatenate([k_ref[4 * m + r, at, :] * keep, eye[...]], axis=1)
                    pltpu.matmul_acc_lhs(sacc[m][r], lhs, 0 if r == 0 else None)
                if r == 0:
                    if odd == 0:
                        push_qb(it, 1)
                    else:
                        push_qb(lax.min(it + 1, 63), 0)
                    push_p(1 - par, 2 * odd)
            pv(before, 2 * odd)
            push_p(1 - par, 2 * odd + 1)
            pv(before, 2 * odd + 1)
            for r in range(2):
                pop_scores(par, odd, r, r)

    def body(pair, _):
        step(2 * pair, 0)
        comm(pair + 1)

        @pl.when(lax.rem(pair, 2) == 0)
        def _():
            result(lax.max(2 * pair - 4, 0))

        step(2 * pair + 1, 1)
        return 0

    if first == 0:
        push_qb(0, 0)
    lax.fori_loop(first // 2, last // 2, body, 0)
    if last < 64:
        return
    par = (last - 1) % 2
    zero = jnp.zeros((128, 256), BF)
    for r in (2, 3):
        pop_scores(par, 1, r, r)
    for m in range(2):
        pltpu.matmul_acc_lhs(sacc[m][0], zero, 0)
        pltpu.matmul_pop(sacc[m][0])
    for r in range(4):
        push_p(par, r)
        pv(last - 1, r)
    result(last - 1)


def attn_kernel(piece_ref, w_ref, q_hbm, k_hbm, vt_hbm, gate_hbm, z_hbm, out_hbm, full, q_ref, k_ref, vt_ref, gate_ref, z_ref, qs, eye, slot, ps0, ps1, ps2, ps3, mask_ref, o_ref, wide, scr, outgoing, landed, note, notes, bad, send_sem, recv_sem, load_sem, push_sem, land_sem, note_send, note_recv, out_sem):
    ps = (ps0, ps1, ps2, ps3)
    gx, gy = lax.axis_index("gx"), lax.axis_index("gy")
    me = gx * 8 + gy
    pairs = ((q_hbm, q_ref), (k_hbm, k_ref), (vt_hbm, vt_ref), (gate_hbm, gate_ref), (z_hbm, z_ref))
    loads = [pltpu.make_async_copy(a, b, load_sem.at[n]) for n, (a, b) in enumerate(pairs)]
    for c in loads:
        c.start()
    torus = Torus(piece_ref, full, send_sem, recv_sem)
    torus.barrier()
    torus.early()
    torus.late("outward", 0, True)
    torus.late("outward", 1)
    for c in loads:
        c.wait()
    attn_setup(q_ref, qs, eye, slot)
    wide[...] = jnp.zeros((256, 256), BF)
    wide[0:128, 0:128] = w_ref[...]
    wide[128:256, 128:256] = w_ref[...]
    bad[...] = jnp.zeros((8, 128), F32)
    torus.late("onward", 0, True)
    torus.late("outward", 2)
    torus.late("onward", 1)
    torus.late("outward", 3)
    torus.late("closing", 0, True)
    torus.early_shared()
    torus.late("shared", 0, True)
    attn_mask(full.reshape(PLANES, 1024, 128)[EXTRA], mask_ref)
    b_ref = full.reshape(PLANES, 2, 4, 2, 64, 128)
    qs_by = qs.reshape(8, 2, 4, 2, 64, 128)
    gate_by = gate_ref.reshape(8, 2, 4, 2, 64, 128)
    z_by = z_ref.reshape(8, 2, 4, 2, 64, 128)

    def owner(n):
        quarter, x, low = n // 32, lax.rem(n // 8, 4), lax.rem(n, 8)
        return (lax.rem(quarter, 2) * 8 + x * 2 + quarter // 2) * 8 + low

    my_block = (lax.rem(gx, 2) * 2 + gx // 8) * 32 + lax.rem(gx // 2, 4) * 8 + gy

    def block(n):
        dest = owner(n)
        return pltpu.make_async_remote_copy(
            src_ref=outgoing.at[n], dst_ref=landed.at[:, me], send_sem=push_sem, recv_sem=land_sem,
            device_id=(dest // 8, lax.rem(dest, 8)), device_id_type=MESH_ID)

    def hand_over(t, sacc):
        at = pl.ds(pl.multiple_of(t * 128, 128), 128)
        core, zl, half = t // 4, lax.rem(t // 2, 2), pl.ds(2 * lax.rem(t, 2), 2)
        for m in range(2):
            pltpu.matmul_push_rhs(wide[...], 1, m)
        for rp in range(4):
            parts = []
            for i in (2 * rp, 2 * rp + 1):
                parts.append((jnp.transpose(o_ref[i, :, at]) * gate_by[i, zl, half, core].reshape(128, 128).astype(F32)).astype(BF))
            pltpu.matmul_acc_lhs(sacc[rp % 2][rp // 2], jnp.concatenate(parts, axis=1), 1 if rp < 2 else None)
        worst = bad[...]
        for rp in range(4):
            y = pltpu.matmul_pop(sacc[rp % 2][rp // 2])
            for u in range(2):
                i = 2 * rp + u
                v = z_by[i, zl, half, core].reshape(128, 128).astype(F32) + y[:, 128 * u:128 * u + 128]
                scr[pl.ds(i, 128, stride=8), :] = v
                off = jnp.where(jnp.abs(v) < 1e30, 0.0, 1.0).reshape(16, 8, 128)
                worst = jnp.maximum(worst, jnp.max(off, axis=0))
        bad[...] = worst
        outgoing[pl.ds(pl.multiple_of(t * 16, 16), 16)] = scr[...].astype(BF).reshape(16, 8, 8, 128)

        def push(n, _):
            spot = t * 16 + lax.rem(me + n, 16)

            @pl.when(spot != my_block)
            def _():
                block(spot).start()

            return 0

        lax.fori_loop(0, 16, push, 0)

    specs = []
    for m in range(2):
        specs += [pltpu.ACC(m)((128, 256), F32)] * 4 + [pltpu.ACC(m)((48, 256), F32)] * 4

    def run(*accs):
        sacc = [accs[8 * m:8 * m + 4] for m in range(2)]
        oacc = [accs[8 * m + 4:8 * m + 8] for m in range(2)]

        def comm(pair):
            @pl.when(pair < 13)
            def _():
                @pl.when((pair == 1) | (pair == 3))
                def _():
                    torus.late("onward", (pair + 3) // 2)

                @pl.when(lax.rem(pair, 4) == 2)
                def _():
                    torus.late("closing", (pair + 2) // 4)

                @pl.when((pair > 0) & (lax.rem(pair, 4) == 0))
                def _():
                    torus.late("shared", pair // 4)

            @pl.when((pair >= 18) & (pair < 22))
            def _():
                hand_over(lax.rem(pair - 18 + gx // 2, 4), sacc)

            @pl.when((pair >= 26) & (pair < 28))
            def _():
                hand_over(4 + lax.rem(pair + gx // 2, 2), sacc)

        attn_loop(0, 64, comm, k_ref, vt_ref, b_ref, o_ref, qs_by, eye, slot, ps, mask_ref, sacc, oacc)

        def tail(t, _):
            hand_over(6 + lax.rem(t + gx // 2, 2), sacc)
            return 0

        lax.fori_loop(0, 2, tail, 0)

    pl.run_scoped(run, *specs)
    seen = jnp.max(bad[...], axis=(0, 1), keepdims=True)
    note[...] = jnp.broadcast_to(seen, (8, 128))
    landed[:, me] = outgoing[my_block]
    notes[me] = note[...]

    def tell(dest):
        return pltpu.make_async_remote_copy(
            src_ref=note, dst_ref=notes.at[me], send_sem=note_send, recv_sem=note_recv,
            device_id=(dest // 8, lax.rem(dest, 8)), device_id_type=MESH_ID)

    def spread(n, _):
        tell(lax.rem(me + n, 128)).start()
        return 0

    lax.fori_loop(1, 128, spread, 0)
    torus.finish()
    neighbour = dict(device_id=(lax.rem(gx + 1, 16), gy), device_id_type=MESH_ID)
    blocks = pltpu.make_async_remote_copy(
        src_ref=outgoing.at[0:127], dst_ref=landed.at[:, 0:127], send_sem=push_sem, recv_sem=land_sem, **neighbour)
    all_notes = pltpu.make_async_remote_copy(
        src_ref=notes.at[0:127], dst_ref=notes.at[0:127], send_sem=note_send, recv_sem=note_recv, **neighbour)
    blocks.wait_recv()
    all_notes.wait_recv()
    worst = jnp.max(notes[...], axis=0)
    landed[0, 0, 0:8] = jnp.where(worst > 0.0, jnp.nan, landed[0, 0, 0:8].astype(F32)).astype(BF)
    out = pltpu.make_async_copy(landed, out_hbm, out_sem)
    out.start()
    blocks.wait_send()
    all_notes.wait_send()
    out.wait()


def attention(piece, w, q, k, vt, gate, z, collective_id):
    vmem = pl.BlockSpec(memory_space=pltpu.VMEM)
    hbm = pl.BlockSpec(memory_space=pl.ANY)
    rows = pltpu.VMEM((8, 1024, 128), BF)
    out = pl.pallas_call(
        attn_kernel,
        in_specs=[vmem, vmem] + [hbm] * 5,
        out_specs=hbm,
        out_shape=jax.ShapeDtypeStruct((8, 128, 8, 128), BF),
        scratch_shapes=[
            pltpu.VMEM((PLANES, 2, 4, 2, 4, 2, 8, 128), BF),
            rows,
            rows,
            pltpu.VMEM((8, 4, 48, 1024), BF),
            rows,
            rows,
            rows,
            pltpu.VMEM((128, 128), BF),
            pltpu.VMEM((4, 16, 128), BF),
            *[pltpu.VMEM((4, 256, 256), BF)] * 4,
            pltpu.VMEM((16, 1024), BF),
            pltpu.VMEM((8, 128, 1024), F32),
            pltpu.VMEM((256, 256), BF),
            pltpu.VMEM((1024, 128), F32),
            pltpu.VMEM((128, 8, 8, 128), BF),
            pltpu.VMEM((8, 128, 8, 128), BF),
            pltpu.VMEM((8, 128), F32),
            pltpu.VMEM((128, 8, 128), F32),
            pltpu.VMEM((8, 128), F32),
            pltpu.SemaphoreType.DMA((EARLY + 84,)),
            pltpu.SemaphoreType.DMA((EARLY + 84,)),
            pltpu.SemaphoreType.DMA((5,)),
            *[pltpu.SemaphoreType.DMA] * 5,
        ],
        compiler_params=pltpu.CompilerParams(collective_id=collective_id, has_side_effects=True, vmem_limit_bytes=60 * 2**20),
        name="tri_attn",
    )(piece, w, q, k, vt, gate, z)
    return out.reshape(8, 1024, 128)


def layer_norm(x, gain):
    mean = jnp.mean(x, axis=-1, keepdims=True)
    c = x - mean
    var = jnp.mean(c * c, axis=-1, keepdims=True)
    return (c * lax.rsqrt(var + 1e-05) * gain).astype(BF)


def pre_kernel(z_ref, gain_ref, proj_ref, bw_ref, gb_ref, mask_ref, q_ref, k_ref, vt_ref, gate_ref, b_ref, scr, wqk):
    i = pl.program_id(0)

    @pl.when(i == 0)
    def _():
        for s in range(4):
            for n in range(2):
                w = proj_ref[:, 128 * n:128 * n + 128].astype(F32)
                wqk[s, :, 128 * n:128 * n + 128] = (pltpu.roll(w, 32 * s, 1) if s else w).astype(BF)
        scr[...] = jnp.zeros((PLANES, 8, 128), F32)
        scr[EXTRA] = mask_ref[...]

    a = layer_norm(z_ref[0].astype(F32), gain_ref[...])
    qk = jnp.dot(a, wqk[lax.rem(i, 4)], preferred_element_type=F32)
    q_ref[0] = (qk[:, :128] * (HEAD_DIM ** -0.5 * LOG2E)).astype(BF)
    k_ref[0] = qk[:, 128:].astype(BF)
    vg = jnp.dot(a, proj_ref[:, 256:512], preferred_element_type=F32)
    vt = jnp.transpose(vg[:, :128].astype(BF))
    tail = jnp.where(lax.broadcasted_iota(jnp.int32, (16, 1024), 0) == 0, 1.0, 0.0).astype(BF)
    for h in range(4):
        vt_ref[0, h, 0:32, :] = vt[32 * h:32 * h + 32, :]
        vt_ref[0, h, 32:48, :] = tail
    gate_ref[0] = jax.nn.sigmoid(vg[:, 128:] + gb_ref[...]).astype(BF)
    b = lax.dot_general(bw_ref[...], a, (((1,), (1,)), ((), ())), preferred_element_type=F32)
    b = b.astype(BF).astype(F32)
    m = jnp.max(b, axis=-1, keepdims=True)
    b = (b - m) * LOG2E
    for h in range(4):
        for kt in range(8):
            scr[plane(h, kt), pl.ds(i, 1), :] = b[h:h + 1, kt * 128:(kt + 1) * 128]
    lane = lax.broadcasted_iota(jnp.int32, (4, 128), 1)
    scr[EXTRA, 1:5, :] = jnp.where(lane == i, m[0:4], scr[EXTRA, 1:5, :])

    @pl.when(i == 7)
    def _():
        b_ref[...] = scr[...].astype(BF)


def pre(z, gain, proj, bias_w, gate_bias, mask_tile):
    bwt = jnp.pad(jnp.transpose(bias_w), ((0, 12), (0, 0)))
    row = lambda i: (i, 0, 0)
    return pl.pallas_call(
        pre_kernel,
        grid=(8,),
        in_specs=[
            pl.BlockSpec((1, 1024, 128), row),
            pl.BlockSpec((1, 128), lambda i: (0, 0)),
            pl.BlockSpec((128, 512), lambda i: (0, 0)),
            pl.BlockSpec((16, 128), lambda i: (0, 0)),
            pl.BlockSpec((1, 128), lambda i: (0, 0)),
            pl.BlockSpec((8, 128), lambda i: (0, 0)),
        ],
        out_specs=[
            pl.BlockSpec((1, 1024, 128), row),
            pl.BlockSpec((1, 1024, 128), row),
            pl.BlockSpec((1, 4, 48, 1024), lambda i: (i, 0, 0, 0)),
            pl.BlockSpec((1, 1024, 128), row),
            pl.BlockSpec((PLANES, 8, 128), lambda i: (0, 0, 0)),
        ],
        out_shape=[
            jax.ShapeDtypeStruct((8, 1024, 128), BF),
            jax.ShapeDtypeStruct((8, 1024, 128), BF),
            jax.ShapeDtypeStruct((8, 4, 48, 1024), BF),
            jax.ShapeDtypeStruct((8, 1024, 128), BF),
            jax.ShapeDtypeStruct((PLANES, 8, 128), BF),
        ],
        scratch_shapes=[pltpu.VMEM((PLANES, 8, 128), F32), pltpu.VMEM((4, 128, 256), BF)],
        compiler_params=pltpu.CompilerParams(vmem_limit_bytes=48 * 2**20),
        name="tri_pre",
    )(z, gain.reshape(1, 128), proj, bwt, gate_bias.reshape(1, 128), mask_tile)


def trans_kernel(z_ref, gain_ref, w1_ref, b1_ref, w2_ref, out_ref, flag_ref):
    z = z_ref[0].astype(F32)

    @pl.when(pl.program_id(0) == 0)
    def _():
        flag_ref[...] = jnp.zeros((8, 128), F32)

    off = jnp.where(jnp.abs(z[0:16]) < 1e30, 0.0, 1.0)
    flag_ref[...] = jnp.maximum(flag_ref[...], jnp.maximum(off[0:8], off[8:16]))
    a = layer_norm(z, gain_ref[...])
    hid = jax.nn.relu(jnp.dot(a, w1_ref[...], preferred_element_type=F32) + b1_ref[...]).astype(BF)
    out_ref[0] = (z + jnp.dot(hid, w2_ref[...], preferred_element_type=F32)).astype(BF)


def trans(z, gain, w1, b1, w2):
    row = lambda i: (i, 0, 0)
    whole = lambda i: (0, 0)
    return pl.pallas_call(
        trans_kernel,
        grid=(8,),
        in_specs=[
            pl.BlockSpec((1, 1024, 128), row),
            pl.BlockSpec((1, 128), whole),
            pl.BlockSpec((128, 512), whole),
            pl.BlockSpec((1, 512), whole),
            pl.BlockSpec((512, 128), whole),
        ],
        out_specs=[pl.BlockSpec((1, 1024, 128), row), pl.BlockSpec((8, 128), whole)],
        out_shape=[jax.ShapeDtypeStruct((8, 1024, 128), BF), jax.ShapeDtypeStruct((8, 128), F32)],
        compiler_params=pltpu.CompilerParams(vmem_limit_bytes=48 * 2**20),
        name="tri_trans",
    )(z, gain.reshape(1, 128), w1, b1.reshape(1, 512), w2)


def exact_phase(z, mask, gain, proj, gate_bias, bias_w, out_w):
    key_bias = (mask - 1.0) * big_negative

    def before(row):
        a = layer_norm(row.astype(F32), gain)
        b = jnp.dot(a, bias_w, preferred_element_type=F32).astype(BF)
        return jnp.dot(a, proj, preferred_element_type=F32), jnp.transpose(b)

    p, b = lax.map(before, z)
    q, k, v = [jnp.moveaxis(p[..., 128 * n:128 * n + 128].astype(BF).reshape(8, 1024, 4, 32), 2, 0) for n in range(3)]

    def per_head(ops):
        qh, kh, vh, bh = ops
        eighths = jnp.swapaxes(bh.reshape(8, 8, 128), 0, 1)
        bias = lax.map(lambda c: lax.all_gather(c, AX, axis=0, tiled=True), eighths)
        bias = jnp.swapaxes(bias, 0, 1).reshape(1024, 1024).astype(F32)

        def per_row(rows):
            qr, kr, vr = rows
            s = jnp.dot(qr, kr.T, preferred_element_type=F32) * HEAD_DIM ** -0.5 + bias + key_bias
            return jnp.dot(jax.nn.softmax(s, axis=-1), vr.astype(F32), preferred_element_type=F32)

        return lax.map(per_row, (qh, kh, vh))

    o = jnp.moveaxis(lax.map(per_head, (q, k, v, jnp.swapaxes(b, 0, 1))), 0, 2).reshape(8, 1024, 128)

    def after(ops):
        row, mixed, logit = ops
        gated = (mixed * jax.nn.sigmoid(logit + gate_bias)).astype(BF)
        return (row.astype(F32) + jnp.dot(gated, out_w, preferred_element_type=F32)).astype(BF)

    z = lax.map(after, (z, o, p[..., 384:]))
    z = lax.all_to_all(z, AX, split_axis=1, concat_axis=0, tiled=True)
    return jnp.swapaxes(z, 0, 1)


def exact(z, mask_local, phases, last):
    mask = lax.all_gather(mask_local.astype(F32), AX, axis=0, tiled=True)
    stacked = [jnp.stack(pair) for pair in zip(*phases)]
    z, _ = lax.scan(lambda z, ws: (exact_phase(z, mask, *ws), None), z, stacked)
    return trans(z, *last)[0]


def phase(z, mask_tile, collective_id, gain, proj, gate_bias, bias_w, out_w):
    q, k, vt, gate, piece = pre(z, gain, proj, bias_w, gate_bias, mask_tile)
    return attention(piece, out_w, q, k, vt, gate, z, collective_id)


def local(
    pair_in,
    residue_mask,
    norm_start,
    proj_start,
    gate_bias_start,
    bias_w_start,
    out_w_start,
    norm_end,
    proj_end,
    gate_bias_end,
    bias_w_end,
    out_w_end,
    norm_trans,
    trans_in,
    trans_bias,
    trans_out,
):
    device = lax.axis_index("gx") * 8 + lax.axis_index("gy")
    lane = lax.broadcasted_iota(jnp.int32, (8, 128), 1)
    row = lax.broadcasted_iota(jnp.int32, (8, 128), 0)
    spread = jnp.tile(residue_mask.astype(F32), 16).reshape(1, 128)
    mask_tile = jnp.where((lane // 8 == lax.rem(device, 16)) & (row == 0), spread, 0.0)
    start = (norm_start, proj_start, gate_bias_start, bias_w_start, out_w_start)
    end = (norm_end, proj_end, gate_bias_end, bias_w_end, out_w_end)
    z = phase(pair_in, mask_tile, 0, *start)
    z = phase(z, mask_tile, 1, *end)
    last = (norm_trans, trans_in, trans_bias, trans_out)
    out, flag = trans(z, *last)
    return lax.cond(jnp.max(flag) == 0.0, lambda: out, lambda: exact(pair_in, residue_mask, (start, end), last))


def solution(mesh):
    rows = P(AX, None, None)
    placed = (rows, P(AX)) + (P(),) * 14

    def whole(*args):
        with jax.sharding.use_abstract_mesh(mesh.abstract_mesh):
            return jax.shard_map(local, mesh=mesh, in_specs=placed, out_specs=rows, check_vma=False)(*args)

    return whole
```
